256 devices in a mesh: col: 32 (over z, y), row: 8 (over x, core).
Axes of the slice: x: 4, y: 4, z: 8, core: 2. Of those that a mesh axis runs over, the one named last changes fastest.
Arguments:
- psi_init: float32 [4096, 2, 4096], P('row', None, 'col')
- left_env: float32 [4096, 3, 4096], P('row')
- mpo_tensor: float32 [3, 3, 2, 2], replicated
- right_env: float32 [4096, 3, 4096], P('col')
Outputs:
- output 1: float32 [4], replicated
- output 2: float32 [4], replicated
- output 3: float32 [4096, 2, 4096], P('row', None, 'col')
All inputs are finite; a program needn't handle non-finite values.
Results may differ from the reference program's by a relative error of at most 0.001.
Values sent between devices are 32-bit elements.
A program may use at most 768 MiB of HBM per device.

```python
import jax
import jax.numpy as jnp
from jax import lax

BOND_DIM = 4096
PHYS_DIM = 2
MPO_DIM = 3
LANCZOS_STEPS = 4
REF_BLOCK = min(BOND_DIM, 128)
EXACT_PREC = lax.Precision.HIGHEST


def make_env(key_dense, key_shift):
    dense_part = jax.random.normal(key_dense, (BOND_DIM, MPO_DIM, BOND_DIM), jnp.float32)
    dense_part = (dense_part + jnp.transpose(dense_part, (2, 1, 0))) * (0.5 / BOND_DIM) ** 0.5
    shifts = 1.0 + 0.5 * jax.random.normal(key_shift, (MPO_DIM,), jnp.float32)
    eye_mat = jnp.eye(BOND_DIM, dtype=jnp.float32)
    return dense_part + eye_mat[:, None, :] * shifts[None, :, None]


def setup_inputs(seed: int = 0) -> dict:
    key_list = jax.random.split(jax.random.key(seed), 6)
    psi_init = jax.random.normal(key_list[0], (BOND_DIM, PHYS_DIM, BOND_DIM), jnp.float32)
    left_env = make_env(key_list[1], key_list[2])
    mpo_raw = jax.random.normal(key_list[3], (MPO_DIM, MPO_DIM, PHYS_DIM, PHYS_DIM), jnp.float32)
    mpo_tensor = (mpo_raw + jnp.transpose(mpo_raw, (0, 1, 3, 2))) * (0.5 ** 0.5 / (MPO_DIM * PHYS_DIM ** 0.5))
    mpo_tensor = mpo_tensor + jnp.eye(PHYS_DIM, dtype=jnp.float32) / MPO_DIM ** 2
    right_env = make_env(key_list[4], key_list[5])
    return {"psi_init": psi_init, "left_env": left_env, "mpo_tensor": mpo_tensor, "right_env": right_env}


def apply_ham(vec_in, left_blocks, mpo_tensor, right_env):
    def one_block(left_blk):
        t_one = jnp.einsum("alc,asb->lcsb", left_blk, vec_in, precision=EXACT_PREC)
        t_two = jnp.einsum("lcsb,lrst->cbrt", t_one, mpo_tensor, precision=EXACT_PREC)
        return jnp.einsum("cbrt,brd->ctd", t_two, right_env, precision=EXACT_PREC)
    out_blocks = lax.map(one_block, left_blocks)
    return out_blocks.reshape(BOND_DIM, PHYS_DIM, BOND_DIM)


def reference(psi_init, left_env, mpo_tensor, right_env):
    block_count = BOND_DIM // REF_BLOCK
    left_blocks = jnp.transpose(left_env.reshape(BOND_DIM, MPO_DIM, block_count, REF_BLOCK), (2, 0, 1, 3))
    vec_init = psi_init / jnp.sqrt(jnp.sum(psi_init * psi_init))

    def lanczos_step(loop_state, step_input):
        vec_prev, vec_cur, beta_prev = loop_state
        work_vec = apply_ham(vec_cur, left_blocks, mpo_tensor, right_env)
        alpha_val = jnp.sum(vec_cur * work_vec)
        work_vec = work_vec - alpha_val * vec_cur - beta_prev * vec_prev
        beta_val = jnp.sqrt(jnp.sum(work_vec * work_vec))
        return (vec_cur, work_vec / beta_val, beta_val), (alpha_val, beta_val)

    state_init = (jnp.zeros_like(vec_init), vec_init, jnp.zeros((), vec_init.dtype))
    final_state, scalar_lists = lax.scan(lanczos_step, state_init, None, length=LANCZOS_STEPS)
    return scalar_lists[0], scalar_lists[1], final_state[1]
```

```python
import functools

import jax
import jax.numpy as jnp
from jax import lax
from jax.experimental import pallas as pl
from jax.experimental.pallas import tpu as pltpu
from jax.sharding import PartitionSpec as P

LANCZOS_STEPS = 4
EXACT_PREC = lax.Precision.HIGHEST
MESH = pl.DeviceIdType.MESH
ROWS = 8
PAIR = range(2)
TRIPLE = range(3)
WAYS = (1, -1)
GONE, HERE = True, False


def fold(body, count, unroll=4):
    while count % unroll:
        unroll //= 2

    def trip(i, carry):
        for u in range(unroll):
            body(i * unroll + u)
        return carry

    lax.fori_loop(0, count // unroll, trip, 0)


def lanczos_kernel(
    nz, nx, wa, wb, n0,
    psi_ref, l_hbm, w_ref, r_hbm,
    scal_ref, vout_ref,
    vbuf, lbuf, rbuf, ubuf, tbuf, vv, rd, ps, po, hx, fx, yx, red, sc,
    ag_s, ag_r, rd_s, rd_r, hx_s, hx_r, fx_s, fx_r, yx_s, yx_r,
    ar_s, ar_r, rr_s, rr_r, io_s, io_r, ld_s, credit,
):
    hops = nz // 2
    half = wb // 2
    quart = half // 4
    col, row = lax.axis_index("col"), lax.axis_index("row")
    z, y, x, c = col // 4, col % 4, row // 2, row % 2
    yh, yl, sub = y // 2, ((y + 1) // 2) % 2, y % 2
    own = z * 2 + yh

    def dev(zz=None, yy=None, xx=None, cc=None):
        zz = z if zz is None else zz
        yy = y if yy is None else yy
        xx = x if xx is None else xx
        cc = c if cc is None else cc
        return {"col": zz * 4 + yy, "row": xx * 2 + cc}

    def zat(off):
        return (z + off + 2 * nz) % nz

    sibling = dev(cc=1 - c)
    yl_partner = dev(yy=y + 1 - 2 * sub)
    yh_partner = dev(yy=3 - y)
    x_mate = dev(xx=x + 1 - 2 * (x % 2))
    z_next = {1: dev(zz=zat(1)), -1: dev(zz=zat(-1))}
    x_next = {1: dev(xx=(x + 1) % nx), -1: dev(xx=(x + nx - 1) % nx)}

    def remote(src, dst, send, recv, to):
        return pltpu.make_async_remote_copy(
            src_ref=src, dst_ref=dst, send_sem=send, recv_sem=recv, device_id=to, device_id_type=MESH
        )

    def rows_of(kind, d=0, h=0):
        start, count = (0, n0) if kind == 0 else (n0, wb - n0)
        if h == hops:
            count //= 2
            if d < 0:
                start += count
        return start, count

    def piece(p, s, k, kind, d, h, mid, to):
        start, count = rows_of(kind, d, h)
        at = vbuf.at[p, s, pl.ds(pl.multiple_of(k * wb + start, ROWS), count), :]
        return remote(at, at, ag_s.at[s, mid], ag_r.at[p, s, mid], to)

    def z_id(d, line, h):
        return ((0 if d > 0 else 1) * 3 + line) * hops + h - 1

    def z_copy(p, s, d, line, h, gone):
        k = zat(-d * (h - 1 if gone else h)) * 2 + (1 - yh if line == 2 else yh)
        return piece(p, s, k, min(line, 1), d, h, z_id(d, line, h), z_next[d])

    pair_last = 6 * hops

    def pair_copy(p, s, kind, d, h, gone):
        if kind == 1:
            mid = pair_last
        elif h == 0:
            mid = pair_last + 1
        else:
            mid = pair_last + 2 + (0 if d > 0 else 1) * hops + h - 1
        k = zat(-d * h) * 2 + (yh if gone else 1 - yh)
        return piece(p, s, k, kind, d, h, mid, yh_partner)

    def own_sends(p, s):
        pair_copy(p, s, 1, 0, 0, GONE).start()
        for line in PAIR:
            for d in WAYS:
                z_copy(p, s, d, line, 1, GONE).start()
        pair_copy(p, s, 0, 0, 0, GONE).start()

    def take_pair(p, s):
        pair_copy(p, s, 1, 0, 0, HERE).wait_recv()
        for d in WAYS:
            z_copy(p, s, d, 2, 1, GONE).start()

    def take_hop(p, s, line, h):
        for d in WAYS:
            z_copy(p, s, d, line, h, HERE).wait_recv()
            if h < hops:
                z_copy(p, s, d, line, h + 1, GONE).start()
            if line == 0:
                pair_copy(p, s, 0, d, h, GONE).start()

    def take_cross(p, s, h):
        for d in WAYS if h else (0,):
            pair_copy(p, s, 0, d, h, HERE).wait_recv()

    def drain_sends(p, s):
        pair_copy(p, s, 1, 0, 0, GONE).wait_send()
        pair_copy(p, s, 0, 0, 0, GONE).wait_send()
        for d in WAYS:
            for h in range(1, hops + 1):
                for line in TRIPLE:
                    z_copy(p, s, d, line, h, GONE).wait_send()
                pair_copy(p, s, 0, d, h, GONE).wait_send()

    def events(p, s):
        out = [lambda: take_pair(p, s)]
        for h in range(1, hops + 1):
            for line in TRIPLE:
                out.append(functools.partial(take_hop, p, s, line, h))
        return out

    groups = (
        (0, nx * 2, row, lambda d: {"col": col, "row": (row + d) % (nx * 2)}),
        (nx * 2, 4, y, lambda d: dev(yy=(y + d) % 4)),
        (nx * 2 + 4, nz, z, lambda d: dev(zz=(z + d) % nz)),
    )

    def sum_send(which, stage, tile):
        base, count, me, peer = groups[stage]
        red[which, base + me] = tile
        at = red.at[which, base + me]
        for d in range(1, count):
            remote(at, at, ar_s.at[which, stage], ar_r.at[which, stage], peer(d)).start()

    def sum_take(which, stage):
        base, count, _, _ = groups[stage]
        at = red.at[which, pl.ds(base, count - 1)]
        pltpu.make_async_copy(at, at, ar_r.at[which, stage]).wait()
        pltpu.make_async_copy(at, at, ar_s.at[which, stage]).wait()
        total = red[which, base]
        for i in range(1, count):
            total = total + red[which, base + i]
        return total

    lanes = red.shape[-1]

    def narrow(tile):
        out = tile[:, :lanes]
        for i in range(1, wa // lanes):
            out = out + tile[:, i * lanes : (i + 1) * lanes]
        return out

    def block(i):
        return pl.ds(pl.multiple_of(i * ROWS, ROWS), ROWS)

    def own_block(i):
        return pl.ds(pl.multiple_of(own * wb + i * ROWS, ROWS), ROWS)

    def accumulate(term):
        def trip(i, acc):
            for s in PAIR:
                acc = acc + term(s, i)
            return acc

        return lax.fori_loop(0, wb // ROWS, trip, jnp.zeros((ROWS, wa), jnp.float32), unroll=4)

    def alpha_open(p):
        acc = accumulate(lambda s, i: vv[p, s, block(i), :] * vbuf[p, s, own_block(i), :])
        sum_send(0, 0, narrow(acc))

    def alpha_close(tile, slot):
        value = jnp.full((ROWS, wa), jnp.sum(tile), jnp.float32)
        sc[0] = value
        scal_ref[slot] = value[:, :lanes]

    def beta_open(p):
        alpha, beta = sc[0], sc[2]

        def term(s, i):
            u = vbuf[p, s, own_block(i), :] - alpha * vv[p, s, block(i), :] - beta * vv[1 - p, s, block(i), :]
            vv[1 - p, s, block(i), :] = u
            return u * u

        sum_send(1, 0, narrow(accumulate(term)))

    def beta_close(p, tile, slot):
        value = jnp.sqrt(jnp.full((ROWS, wa), jnp.sum(tile), jnp.float32))
        sc[1] = value
        scal_ref[LANCZOS_STEPS + slot] = value[:, :lanes]

        def scale(i):
            for s in PAIR:
                vv[1 - p, s, block(i), :] = vv[1 - p, s, block(i), :] / value

        fold(scale, wb // ROWS)

    def r_rows(r, of_sub, q):
        return rbuf.at[pl.ds(pl.multiple_of(r * wb + of_sub * half + q * quart, ROWS), quart), :]

    q_own, q_mate = (x % 2) * 2 + c, (1 - x % 2) * 2 + c
    q_sib, q_sib_mate = (x % 2) * 2 + 1 - c, (1 - x % 2) * 2 + 1 - c

    def r_copy(way, r, gone):
        if way == 0:
            src = r_hbm.at[r, pl.ds(pl.multiple_of(q_own * quart, ROWS), quart), :]
            dst = r_rows(r, sub if gone else 1 - sub, q_own)
            return remote(src, dst, rr_s.at[0, r], rr_r.at[0, r], yl_partner)
        if way == 1:
            at = r_rows(r, 1 - sub, q_own if gone else q_mate)
            return remote(at, at, rr_s.at[1, r], rr_r.at[1, r], x_mate)
        if way == 2:
            at = r_rows(r, 1 - sub, q_own if gone else q_sib)
        else:
            at = r_rows(r, 1 - sub, q_mate if gone else q_sib_mate)
        return remote(at, at, rr_s.at[way, r], rr_r.at[way, r], sibling)

    def r_first(r):
        r_copy(0, r, HERE).wait_recv()
        r_copy(1, r, GONE).start()
        r_copy(2, r, GONE).start()

    def r_second(r):
        r_copy(1, r, HERE).wait_recv()
        r_copy(3, r, GONE).start()

    def r_last():
        for r in TRIPLE:
            r_copy(2, r, HERE).wait_recv()
            r_copy(3, r, HERE).wait_recv()
            for way in range(4):
                r_copy(way, r, GONE).wait_send()

    def right_group(p, s, h):
        def one(i, carry):
            off = 0 if h == 0 else h * (1 - 2 * (i // 2))
            start = pl.multiple_of((zat(off) * 2 + i % 2) * wb, wb)
            ubuf[s] = ubuf[s] + jnp.dot(
                rbuf[:, pl.ds(start, wb)],
                vbuf[p, s, pl.ds(start, wb), :],
                precision=EXACT_PREC,
                preferred_element_type=jnp.float32,
            )
            return carry

        lax.fori_loop(0, 2 if h in (0, hops) else 4, one, 0)

    def clear_products():
        def trip(i):
            for s in PAIR:
                ubuf[s, block(i), :] = jnp.zeros((ROWS, wa), jnp.float32)

        fold(trip, 3 * wb // ROWS)

    def mix():
        def trip(i):
            tiles = [[ubuf[s, pl.ds(pl.multiple_of(r * wb + i * ROWS, ROWS), ROWS), :] for s in PAIR] for r in TRIPLE]
            for t in PAIR:
                for l in TRIPLE:
                    acc = None
                    for r in TRIPLE:
                        for s in PAIR:
                            term = w_ref[((l * 3 + r) * 2 + s) * 2 + t] * tiles[r][s]
                            acc = term if acc is None else acc + term
                    tbuf[t, block(i), l * wa : (l + 1) * wa] = acc

        fold(trip, wb // ROWS, 1)
        clear_products()

    def left_product(t, xx, cc):
        start = pl.multiple_of((xx * 2 + cc) * 2 * wa, 2 * wa)
        return jnp.dot(
            tbuf[t], lbuf[:, pl.ds(start, 2 * wa)], precision=EXACT_PREC, preferred_element_type=jnp.float32
        )

    def sib_copy(t, i):
        return remote(ps.at[i % 2], rd.at[t, i], rd_s.at[i % 2], rd_r.at[t, i], sibling)

    def lane(theirs):
        return pl.ds(pl.multiple_of((1 - yl if theirs else yl) * wa, wa), wa)

    def half_copy(p, t, d, theirs):
        at = pl.ds(0 if d > 0 else half, half)
        slot, side = 0 if d > 0 else 1, 0 if theirs else 1
        src = rd.at[t, 0, at, lane(theirs)]
        return remote(src, hx.at[p, t, slot, side], hx_s.at[t, slot, side], hx_r.at[p, t, slot, side], x_next[d])

    def full_copy(p, t, d, theirs):
        slot, side = 0 if d > 0 else 1, 0 if theirs else 1
        src = rd.at[t, 1 + slot, :, lane(theirs)]
        return remote(src, fx.at[p, t, slot, side], fx_s.at[t, slot, side], fx_r.at[p, t, slot, side], x_next[d])

    def cross_copy(p, t):
        return remote(rd.at[t, 3, :, lane(True)], yx.at[p, t], yx_s.at[t], yx_r.at[p, t], yl_partner)

    def left_stage(p, t, i):
        xx = (x + (2, 1, nx - 1, 0)[i]) % nx
        if i >= 2:
            sib_copy(t, i - 2).wait_send()
        elif t:
            sib_copy(0, i + 2).wait_send()
        ps[i % 2] = left_product(t, xx, 1 - c)
        sib_copy(t, i).start()
        po[...] = left_product(t, xx, c)
        sib_copy(t, i).wait_recv()
        for theirs in (GONE, HERE):
            lanes_at = lane(theirs)
            side = 0 if theirs else 1
            if i in (1, 2):
                half_copy(p, t, 1 if i == 1 else -1, theirs).wait_recv()
                base = 0 if i == 1 else half

                def add_half(k):
                    rows = pl.ds(pl.multiple_of(k * ROWS + base, ROWS), ROWS)
                    rd[t, i, rows, lanes_at] = rd[t, i, rows, lanes_at] + hx[p, t, i - 1, side, block(k), :]

                fold(add_half, half // ROWS)

            def add(k):
                rows = block(k)
                rd[t, i, rows, lanes_at] = rd[t, i, rows, lanes_at] + po[rows, lanes_at]

            fold(add, wb // ROWS)
            if i == 0:
                half_copy(p, t, 1, theirs).start()
                half_copy(p, t, -1, theirs).start()
            elif i < 3:
                full_copy(p, t, 1 if i == 1 else -1, theirs).start()

    def close_half(p, t):
        for theirs in (GONE, HERE):
            lanes_at = lane(theirs)
            side = 0 if theirs else 1
            for d in WAYS:
                full_copy(p, t, d, theirs).wait_recv()

            def add(k):
                rows = block(k)
                rd[t, 3, rows, lanes_at] = rd[t, 3, rows, lanes_at] + fx[p, t, 0, side, rows, :] + fx[p, t, 1, side, rows, :]

            fold(add, wb // ROWS)
            if theirs:
                cross_copy(p, t).start()
        cross_copy(p, t).wait_recv()
        alpha, beta, old = sc[0], sc[1], sc[2]
        mine = lane(False)

        def step(k):
            rows = block(k)
            g = rd[t, 3, rows, mine] + yx[p, t, rows, :]
            w_now, w_old = vbuf[p, t, own_block(k), :], vbuf[1 - p, t, own_block(k), :]
            vbuf[1 - p, t, own_block(k), :] = (g - alpha * w_now - old * w_old) / beta

        fold(step, wb // ROWS)

    def drain_sums(p, t):
        for theirs in (GONE, HERE):
            for d in WAYS:
                half_copy(p, t, d, theirs).wait_send()
                full_copy(p, t, d, theirs).wait_send()
        cross_copy(p, t).wait_send()

    def l_load(l):
        return pltpu.make_async_copy(
            l_hbm.at[l, pl.ds(pl.multiple_of(yl * wa, ROWS), wa), :], lbuf.at[pl.ds(l * wa, wa), :], ld_s.at[l]
        )

    def r_load(r):
        return pltpu.make_async_copy(
            r_hbm.at[r], rbuf.at[pl.ds(pl.multiple_of(r * wb + sub * half, ROWS), half), :], ld_s.at[3 + r]
        )

    def psi_at(s, of_sub):
        return vbuf.at[0, s, pl.ds(pl.multiple_of(own * wb + of_sub * half, ROWS), half), :]

    def psi_load(s):
        return pltpu.make_async_copy(psi_ref.at[yl, s], psi_at(s, sub), ld_s.at[6 + s])

    def psi_copy(s, gone):
        return remote(psi_ref.at[1 - yl, s], psi_at(s, sub if gone else 1 - sub), io_s.at[s], io_r.at[s], yl_partner)

    for s in PAIR:
        psi_load(s).start()
        psi_copy(s, GONE).start()
    for r in TRIPLE:
        r_copy(0, r, GONE).start()
        r_load(r).start()
    for l in TRIPLE:
        l_load(l).start()
    for t in PAIR:
        pl.semaphore_signal(credit.at[t], inc=1, device_id=sibling, device_id_type=MESH)

    def clear(i):
        for s in PAIR:
            vbuf[1, s, own_block(i), :] = jnp.zeros((ROWS, wa), jnp.float32)
            for p in PAIR:
                vv[p, s, block(i), :] = jnp.zeros((ROWS, wa), jnp.float32)

    fold(clear, wb // ROWS)
    clear_products()
    sc[2] = jnp.zeros((ROWS, wa), jnp.float32)
    for s in PAIR:
        psi_load(s).wait()
        psi_copy(s, HERE).wait_recv()
        own_sends(0, s)

    early = 1 + 3 * min(2, hops - 1) + (1 if hops > 2 else 0)
    for n, event in enumerate(events(0, 0)[:early]):
        event()
        if n in (3, 6):
            r_first((n - 3) // 3)
    for r in range(3 if early <= 3 else (2 if early <= 6 else 1)):
        r_first((2 if early > 6 else 1 if early > 3 else 0) + r)
    for r in TRIPLE:
        r_load(r).wait()
        l_load(r).wait()
    for s in PAIR:
        psi_copy(s, GONE).wait_send()

    def lanczos_step(j, carry):
        p = j % 2
        slot = (j + LANCZOS_STEPS - 1) % LANCZOS_STEPS
        more = j < LANCZOS_STEPS - 1
        late0 = events(p, 0)[early:]
        all1 = events(p, 1)

        all1.pop(0)()
        alpha_open(p)
        while late0:
            late0.pop(0)()
            if len(all1) > 3 * (hops - 1) and len(late0) % 2 == 0:
                all1.pop(0)()
        sum_send(0, 1, sum_take(0, 0))
        for h in range(hops + 1):
            take_cross(p, 0, h)

        @pl.when(j == 0)
        def _():
            for r in TRIPLE:
                r_second(r)
            r_last()

        marks = [
            ((0, 1), lambda: sum_send(0, 2, sum_take(0, 1))),
            ((0, hops), lambda: (alpha_close(sum_take(0, 2), slot), beta_open(p))),
            ((1, hops - 1), lambda: sum_send(1, 1, sum_take(1, 0))),
        ]
        for s in PAIR:
            for h in range(hops + 1):
                if s:
                    while len(all1) > 3 * (hops - h):
                        all1.pop(0)()
                    take_cross(p, 1, h)
                right_group(p, s, h)
                if all1:
                    all1.pop(0)()
                for where, mark in marks:
                    if where == (s, h):
                        mark()
        sum_send(1, 2, sum_take(1, 1))
        mix()
        for s in PAIR:
            drain_sends(p, s)

        ahead = events(1 - p, 0)[:early]

        def serve(count):
            @pl.when(more)
            def _():
                for _ in range(min(count, len(ahead))):
                    ahead.pop(0)()

        for t in PAIR:
            pl.semaphore_wait(credit.at[t], 1)
        for i in range(4):
            left_stage(p, 0, i)
            if i == 1:
                beta_close(p, sum_take(1, 2), slot)
        left_stage(p, 1, 0)
        close_half(p, 0)

        @pl.when(more)
        def _():
            own_sends(1 - p, 0)

        for i in range(1, 4):
            left_stage(p, 1, i)
            serve(2)
        serve(early)
        close_half(p, 1)

        @pl.when(more)
        def _():
            own_sends(1 - p, 1)

        for i in (2, 3):
            sib_copy(1, i).wait_send()
        for t in PAIR:
            drain_sums(p, t)

        @pl.when(more)
        def _():
            for t in PAIR:
                pl.semaphore_signal(credit.at[t], inc=1, device_id=sibling, device_id_type=MESH)

        sc[2] = jnp.where(j > 0, sc[1], jnp.zeros((ROWS, wa), jnp.float32))
        return carry

    lax.fori_loop(0, LANCZOS_STEPS, lanczos_step, 0)

    p = LANCZOS_STEPS % 2
    alpha_open(p)
    for stage in (1, 2):
        sum_send(0, stage, sum_take(0, stage - 1))
    alpha_close(sum_take(0, 2), LANCZOS_STEPS - 1)
    beta_open(p)
    for stage in (1, 2):
        sum_send(1, stage, sum_take(1, stage - 1))
    beta_close(p, sum_take(1, 2), LANCZOS_STEPS - 1)

    def out_store(s):
        src = vv.at[1 - p, s, pl.ds(pl.multiple_of(sub * half, ROWS), half), :]
        return pltpu.make_async_copy(src, vout_ref.at[yl, s], ld_s.at[6 + s])

    def out_copy(s, gone):
        src = vv.at[1 - p, s, pl.ds(pl.multiple_of((1 - sub) * half, ROWS), half), :]
        return remote(src, vout_ref.at[yl if gone else 1 - yl, s], io_s.at[2 + s], io_r.at[2 + s], yl_partner)

    for s in PAIR:
        out_copy(s, GONE).start()
        out_store(s).start()
    for s in PAIR:
        out_store(s).wait()
        out_copy(s, GONE).wait_send()
        out_copy(s, HERE).wait_recv()


def solution(mesh):
    nz, nx = mesh.shape["col"] // 4, mesh.shape["row"] // 2

    def local_steps(psi_blk, left_blk, mpo_tensor, right_blk):
        wa, wb = psi_blk.shape[0] // 2, psi_blk.shape[2] * 2
        da, db = left_blk.shape[2], right_blk.shape[2]
        half = wb // 2
        hops = nz // 2
        n0 = wb * 9 // 16 // 16 * 16
        lanes = 128 if wa % 128 == 0 else wa
        f32 = jnp.float32
        psi_t = jnp.transpose(psi_blk.reshape(2, wa, 2, half), (0, 2, 3, 1))
        kernel = functools.partial(lanczos_kernel, nz, nx, wa, wb, n0)
        vmem, dma = pltpu.VMEM, pltpu.SemaphoreType.DMA
        ids = 8 * hops + 2
        scalars, v_out = pl.pallas_call(
            kernel,
            out_shape=(
                jax.ShapeDtypeStruct((2 * LANCZOS_STEPS, ROWS, lanes), f32),
                jax.ShapeDtypeStruct((2, 2, half, wa), f32),
            ),
            in_specs=[
                pl.BlockSpec(memory_space=pl.ANY),
                pl.BlockSpec(memory_space=pl.ANY),
                pl.BlockSpec(memory_space=pltpu.SMEM),
                pl.BlockSpec(memory_space=pl.ANY),
            ],
            out_specs=(pl.BlockSpec(memory_space=pltpu.VMEM), pl.BlockSpec(memory_space=pl.ANY)),
            scratch_shapes=[
                vmem((2, 2, db, wa), f32),
                vmem((3 * wa, da), f32),
                vmem((3 * wb, db), f32),
                vmem((2, 3 * wb, wa), f32),
                vmem((2, wb, 3 * wa), f32),
                vmem((2, 2, wb, wa), f32),
                vmem((2, 4, wb, 2 * wa), f32),
                vmem((2, wb, 2 * wa), f32),
                vmem((wb, 2 * wa), f32),
                vmem((2, 2, 2, 2, half, wa), f32),
                vmem((2, 2, 2, 2, wb, wa), f32),
                vmem((2, 2, wb, wa), f32),
                vmem((2, nx * 2 + 4 + nz, ROWS, lanes), f32),
                vmem((3, ROWS, wa), f32),
                dma((2, ids)),
                dma((2, 2, ids)),
                dma((2,)),
                dma((2, 4)),
                dma((2, 2, 2)),
                dma((2, 2, 2, 2)),
                dma((2, 2, 2)),
                dma((2, 2, 2, 2)),
                dma((2,)),
                dma((2, 2)),
                dma((2, 3)),
                dma((2, 3)),
                dma((4, 3)),
                dma((4, 3)),
                dma((4,)),
                dma((4,)),
                dma((8,)),
                pltpu.SemaphoreType.REGULAR((2,)),
            ],
            compiler_params=pltpu.CompilerParams(has_side_effects=True, vmem_limit_bytes=66 * 1000 * 1000),
            name="lanczos",
        )(psi_t, jnp.transpose(left_blk, (1, 0, 2)), mpo_tensor.reshape(-1), jnp.transpose(right_blk, (1, 0, 2)))
        v_next = jnp.transpose(v_out, (0, 3, 1, 2)).reshape(psi_blk.shape)
        return scalars[:LANCZOS_STEPS, 0, 0], scalars[LANCZOS_STEPS:, 0, 0], v_next

    return jax.shard_map(
        local_steps,
        mesh=mesh,
        in_specs=(P("row", None, "col"), P("row", None, None), P(), P("col", None, None)),
        out_specs=(P(), P(), P("row", None, "col")),
        check_vma=False,
    )
```

```python
import functools

import jax
import jax.numpy as jnp
from jax import lax
from jax.experimental import pallas as pl
from jax.experimental.pallas import tpu as pltpu
from jax.sharding import PartitionSpec as P

LANCZOS_STEPS = 4
EXACT_PREC = lax.Precision.HIGHEST
MESH = pl.DeviceIdType.MESH
ROWS = 8
SPLIT = 2
PIECES = 4
GATHER_ORDER = (
    "h201,a0,h211,h122,a1,p3,h103,h113,h221,m00*,h301,m01+,h311",
    "a2,m01-,h202,m02+,h212,h123,m02-,h321,h104,m03+,h114,h222",
    "m03-,h302,m10*,h312,m11+,h203,b0,h213,h124,m04*,h322,m11-",
    "h223,b1,m12+,h303,m12-,h313,h204,b2,h214,h323,h224,m13+,h304",
    "h314,h324,m13-,m14*",
)
REDUCE_ORDER = (
    "l00,f000,l01,l02,f030,f010,f020,d0,f011,f021,b3,l10,f100,l11",
    "o0,l12,f130,l20,c0,f110,f120,f111,f121,f200,l21,l22,h001,p0",
    "h011,f230,o1,l30,f300,h002,l31,h021,f210,c1,f220,l32,h012",
    "h003,f211,f221,f330,f310,f320,f311,f321,h022,p1,h101,o2,h111",
    "h013,h004,h023,c2,h121,o3,h102,h112,h014,p2,h024,c3",
)
PAIR = range(2)
TRIPLE = range(3)
WAYS = (1, -1)
GONE, HERE = True, False


def fold(body, count, unroll=4):
    while count % unroll:
        unroll //= 2

    def trip(i, carry):
        for u in range(unroll):
            body(i * unroll + u)
        return carry

    lax.fori_loop(0, count // unroll, trip, 0)


def lanczos_kernel(
    nz, nx, wa, wb,
    psi_ref, l_hbm, w_ref, r_hbm,
    scal_ref, vout_ref,
    vbuf, lbuf, rbuf, ubuf, tbuf, vv, rd, yb, hx, fx, yx, ob, red, sc,
    ag_s, ag_r, rd_s, rd_r, hx_s, hx_r, fx_s, fx_r, yx_s, yx_r,
    ar_s, ar_r, rr_s, rr_r, io_s, io_r, ld_s, credit,
):
    hops = nz // 2
    half, mb = wb // 2, wb // SPLIT
    quart = half // 4
    bit = quart // PIECES
    chunks = range(2 * SPLIT)
    col, row = lax.axis_index("col"), lax.axis_index("row")
    z, y, x, c = col // 4, col % 4, row // 2, row % 2
    yh, yl, sub = y // 2, ((y + 1) // 2) % 2, y % 2
    own = z * 2 + yh

    def dev(zz=None, yy=None, xx=None, cc=None):
        zz = z if zz is None else zz
        yy = y if yy is None else yy
        xx = x if xx is None else xx
        cc = c if cc is None else cc
        return {"col": zz * 4 + yy, "row": xx * 2 + cc}

    def zat(off):
        return (z + off + 2 * nz) % nz

    sibling = dev(cc=1 - c)
    yl_partner = dev(yy=y + 1 - 2 * sub)
    yh_partner = dev(yy=3 - y)
    x_mate = dev(xx=x + 1 - 2 * (x % 2))
    z_next = {1: dev(zz=zat(1)), -1: dev(zz=zat(-1))}
    x_next = {1: dev(xx=(x + 1) % nx), -1: dev(xx=(x + nx - 1) % nx)}

    def remote(src, dst, send, recv, to):
        return pltpu.make_async_remote_copy(
            src_ref=src, dst_ref=dst, send_sem=send, recv_sem=recv, device_id=to, device_id_type=MESH
        )

    def span(start, count):
        return pl.ds(pl.multiple_of(start, ROWS), count)

    def block(i):
        return span(i * ROWS, ROWS)

    def piece(p, q, k, kind, d, h, mid, to):
        cut = mb // 2 + (q % SPLIT) * mb // 8
        start, count = (0, cut) if kind == 0 else (cut, mb - cut)
        if h == hops:
            count //= 2
            start += count if d < 0 else 0
        at = vbuf.at[p, q // SPLIT, span(k * wb + (q % SPLIT) * mb + start, count), :]
        return remote(at, at, ag_s.at[q, mid], ag_r.at[p, q, mid], to)

    def z_copy(p, q, d, line, h, gone):
        k = zat(-d * (h - 1 if gone else h)) * 2 + (1 - yh if line == 2 else yh)
        mid = ((0 if d > 0 else 3) + line) * hops + h - 1
        return piece(p, q, k, min(line, 1), d, h, mid, z_next[d])

    def pair_copy(p, q, kind, d, h, gone):
        mid = 6 * hops + (2 * h + max(d, 0) if h else 0 if kind else 1)
        return piece(p, q, zat(-d * h) * 2 + (yh if gone else 1 - yh), kind, d, h, mid, yh_partner)

    def own_sends(p, q):
        pair_copy(p, q, 1, 0, 0, GONE).start()
        for line in PAIR:
            for d in WAYS:
                z_copy(p, q, d, line, 1, GONE).start()
        pair_copy(p, q, 0, 0, 0, GONE).start()

    def take_pair(p, q):
        pair_copy(p, q, 1, 0, 0, HERE).wait_recv()
        for d in WAYS:
            z_copy(p, q, d, 2, 1, GONE).start()

    def take_hop(p, q, line, h):
        for d in WAYS:
            z_copy(p, q, d, line, h, HERE).wait_recv()
            if h < hops:
                z_copy(p, q, d, line, h + 1, GONE).start()
            if line == 0:
                pair_copy(p, q, 0, d, h, GONE).start()

    def drain_gather(p):
        for q in chunks:
            for kind in PAIR:
                pair_copy(p, q, kind, 0, 0, GONE).wait_send()
            for d in WAYS:
                for h in range(1, hops + 1):
                    for line in TRIPLE:
                        z_copy(p, q, d, line, h, GONE).wait_send()
                    pair_copy(p, q, 0, d, h, GONE).wait_send()

    groups = (
        (0, nx * 2, row, lambda d: {"col": col, "row": (row + d) % (nx * 2)}),
        (nx * 2, 4, y, lambda d: dev(yy=(y + d) % 4)),
        (nx * 2 + 4, nz, z, lambda d: dev(zz=(z + d) % nz)),
    )

    def sum_send(which, stage, tile):
        base, count, me, peer = groups[stage]
        red[which, base + me] = tile
        at = red.at[which, base + me]
        for d in range(1, count):
            remote(at, at, ar_s.at[which, stage], ar_r.at[which, stage], peer(d)).start()

    def sum_take(which, stage):
        base, count, _, _ = groups[stage]
        at = red.at[which, pl.ds(base, count - 1)]
        pltpu.make_async_copy(at, at, ar_r.at[which, stage]).wait()
        pltpu.make_async_copy(at, at, ar_s.at[which, stage]).wait()
        total = red[which, base]
        for i in range(1, count):
            total = total + red[which, base + i]
        return total

    def sum_pass(which, stage):
        sum_send(which, stage, sum_take(which, stage - 1))

    lanes = red.shape[-1]

    def narrow(tile):
        out = tile[:, :lanes]
        for i in range(1, wa // lanes):
            out = out + tile[:, i * lanes : (i + 1) * lanes]
        return out

    def own_block(i):
        return span(own * wb + i * ROWS, ROWS)

    def accumulate(term):
        def trip(i, acc):
            for s in PAIR:
                acc = acc + term(s, i)
            return acc

        return lax.fori_loop(0, wb // ROWS, trip, jnp.zeros((ROWS, wa), jnp.float32), unroll=4)

    def alpha_open(p):
        acc = accumulate(lambda s, i: vv[p, s, block(i), :] * vbuf[p, s, own_block(i), :])
        sum_send(0, 0, narrow(acc))

    def alpha_close(slot):
        value = jnp.full((ROWS, wa), jnp.sum(sum_take(0, 2)), jnp.float32)
        sc[0] = value
        scal_ref[slot] = value[:, :lanes]

    def beta_open(p):
        alpha, beta = sc[0], sc[2]

        def term(s, i):
            u = vbuf[p, s, own_block(i), :] - alpha * vv[p, s, block(i), :] - beta * vv[1 - p, s, block(i), :]
            vv[1 - p, s, block(i), :] = u
            return u * u

        sum_send(1, 0, narrow(accumulate(term)))

    def beta_close(slot):
        value = jnp.sqrt(jnp.full((ROWS, wa), jnp.sum(sum_take(1, 2)), jnp.float32))
        sc[1] = value
        scal_ref[LANCZOS_STEPS + slot] = value[:, :lanes]

    def scale(p):
        def trip(i):
            for s in PAIR:
                vv[1 - p, s, block(i), :] = vv[1 - p, s, block(i), :] / sc[1]

        fold(trip, wb // ROWS)

    def r_rows(e, of_sub, q):
        return rbuf.at[span((e // PIECES) * wb + of_sub * half + q * quart + (e % PIECES) * bit, bit), :]

    q_own, q_mate = (x % 2) * 2 + c, (1 - x % 2) * 2 + c
    q_sib, q_sib_mate = (x % 2) * 2 + 1 - c, (1 - x % 2) * 2 + 1 - c

    def r_copy(way, e, gone):
        sems = rr_s.at[way, e], rr_r.at[way, e]
        if way == 0:
            src = r_hbm.at[e // PIECES, span(q_own * quart + (e % PIECES) * bit, bit), :]
            return remote(src, r_rows(e, sub if gone else 1 - sub, q_own), *sems, yl_partner)
        here, there = (q_mate, q_sib_mate) if way == 3 else (q_own, q_mate if way == 1 else q_sib)
        at = r_rows(e, 1 - sub, here if gone else there)
        return remote(at, at, *sems, x_mate if way == 1 else sibling)

    def r_first(e):
        r_copy(0, e, HERE).wait_recv()
        r_copy(1, e, GONE).start()
        r_copy(2, e, GONE).start()

    def r_second(e):
        r_copy(1, e, HERE).wait_recv()
        r_copy(3, e, GONE).start()

    def r_last():
        for e in range(3 * PIECES):
            r_copy(2, e, HERE).wait_recv()
            r_copy(3, e, HERE).wait_recv()
            for way in range(4):
                r_copy(way, e, GONE).wait_send()

    def right_group(p, s, h, way):
        d = 1 if way == "+" else -1
        for q in range(s * SPLIT, s * SPLIT + SPLIT):
            for e in (d,) if way != "*" else WAYS if h else (0,):
                pair_copy(p, q, 0, e, h, HERE).wait_recv()

        def one(i, carry):
            start = pl.multiple_of((zat(-d * h) * 2 + i) * wb, wb)
            ubuf[s] = ubuf[s] + jnp.dot(
                rbuf[:, pl.ds(start, wb)],
                vbuf[p, s, pl.ds(start, wb), :],
                precision=EXACT_PREC,
                preferred_element_type=jnp.float32,
            )
            return carry

        lax.fori_loop(0, 2, one, 0)

    def clear_products():
        def trip(i):
            for s in PAIR:
                ubuf[s, block(i), :] = jnp.zeros((ROWS, wa), jnp.float32)

        fold(trip, 3 * wb // ROWS)

    def mix():
        def trip(i):
            tiles = [[ubuf[s, span(r * wb + i * ROWS, ROWS), :] for s in PAIR] for r in TRIPLE]
            for t in PAIR:
                for l in TRIPLE:
                    acc = None
                    for r in TRIPLE:
                        for s in PAIR:
                            term = w_ref[((l * 3 + r) * 2 + s) * 2 + t] * tiles[r][s]
                            acc = term if acc is None else acc + term
                    tbuf[t, block(i), l * wa : (l + 1) * wa] = acc

        fold(trip, wb // ROWS, 1)
        clear_products()

    def sib_copy(q, i):
        return remote(yb.at[i], rd.at[q, i], rd_s.at[i], rd_r.at[q, i], sibling)

    def left_products(q, part):
        def one(n, carry):
            theirs = n < (2, 2, 0)[part]
            i = n % 2 if part == 0 else n + 3 - part
            away = jnp.where(i < 2, i + 2, 3 - i)
            start = (((x + away) % nx) * 2 + jnp.where(theirs, 1 - c, c)) * 2 * wa
            yb[jnp.where(theirs, i, i + 4)] = jnp.dot(
                tbuf[q // SPLIT, (q % SPLIT) * mb : (q % SPLIT + 1) * mb, :],
                lbuf[:, pl.ds(pl.multiple_of(start, 2 * wa), 2 * wa)],
                precision=EXACT_PREC,
                preferred_element_type=jnp.float32,
            )

            @pl.when(theirs)
            def _():
                sib_copy(q, i).start()

            return carry

        for i in ((0, 1), (2, 3), ())[part] if q else ():
            sib_copy(q - 1, i).wait_send()
        lax.fori_loop(0, (3, 2, 3)[part], one, 0)

    def lane(theirs):
        return pl.ds(pl.multiple_of((1 - yl if theirs else yl) * wa, wa), wa)

    def half_copy(p, q, d, theirs):
        slot, side = 0 if d > 0 else 1, 0 if theirs else 1
        src = rd.at[q, 0, pl.ds(slot * mb // 2, mb // 2), lane(theirs)]
        return remote(src, hx.at[p, q, slot, side], hx_s.at[q, slot, side], hx_r.at[p, q, slot, side], x_next[d])

    def full_copy(p, q, d, theirs):
        slot, side = 0 if d > 0 else 1, 0 if theirs else 1
        src = rd.at[q, 2 - slot, :, lane(theirs)]
        return remote(src, fx.at[p, q, slot, side], fx_s.at[q, slot, side], fx_r.at[p, q, slot, side], x_next[d])

    def cross_copy(p, q):
        return remote(rd.at[q, 3, :, lane(GONE)], yx.at[p, q], yx_s.at[q], yx_r.at[p, q], yl_partner)

    def left_sum(p, q, i, side):
        if side == 0:
            sib_copy(q, i).wait_recv()

            def add(k):
                rows = block(k)
                rd[q, i, rows, :] = rd[q, i, rows, :] + yb[i + 4, rows, :]

            fold(add, mb // ROWS)
        if i == 0:
            for theirs in (GONE, HERE):
                for d in WAYS:
                    half_copy(p, q, d, theirs).start()
        elif i < 3:
            d, theirs = 2 * i - 3, side == 0
            lanes_at = lane(theirs)
            half_copy(p, q, d, theirs).wait_recv()

            def add_half(k):
                rows = span(k * ROWS + (0 if d > 0 else mb // 2), ROWS)
                rd[q, i, rows, lanes_at] = rd[q, i, rows, lanes_at] + hx[p, q, i % 2, side, block(k), :]

            fold(add_half, mb // 2 // ROWS)
            full_copy(p, q, d, theirs).start()

    def chip_sum(p, q, theirs):
        lanes_at, side = lane(theirs), 0 if theirs else 1
        for d in WAYS:
            full_copy(p, q, d, theirs).wait_recv()

        def add(k):
            rows = block(k)
            rd[q, 3, rows, lanes_at] = rd[q, 3, rows, lanes_at] + fx[p, q, 0, side, rows, :] + fx[p, q, 1, side, rows, :]

        fold(add, mb // ROWS)

    def open_cross(p, q):
        chip_sum(p, q, GONE)
        cross_copy(p, q).start()

    def close_chunk(p, q, more):
        chip_sum(p, q, HERE)
        cross_copy(p, q).wait_recv()
        alpha, beta, old = sc[0], sc[1], sc[2]
        s, mine = q // SPLIT, lane(HERE)

        def step(k):
            rows, at = block(k), own_block(k + (q % SPLIT) * mb // ROWS)
            g = rd[q, 3, rows, mine] + yx[p, q, rows, :]
            vbuf[1 - p, s, at, :] = (g - alpha * vbuf[p, s, at, :] - old * vbuf[1 - p, s, at, :]) / beta

        fold(step, mb // ROWS)

        @pl.when(more)
        def _():
            own_sends(1 - p, q)

    def drain_sums(p, q):
        for theirs in (GONE, HERE):
            for d in WAYS:
                half_copy(p, q, d, theirs).wait_send()
                full_copy(p, q, d, theirs).wait_send()
        cross_copy(p, q).wait_send()

    def l_load(l):
        return pltpu.make_async_copy(l_hbm.at[l, span(yl * wa, wa), :], lbuf.at[pl.ds(l * wa, wa), :], ld_s.at[l])

    def r_load(r):
        return pltpu.make_async_copy(r_hbm.at[r], rbuf.at[span(r * wb + sub * half, half), :], ld_s.at[3 + r])

    def psi_at(s, of_sub):
        return vbuf.at[0, s, span(own * wb + of_sub * half, half), :]

    def psi_load(s):
        return pltpu.make_async_copy(psi_ref.at[yl, s], psi_at(s, sub), ld_s.at[6 + s])

    def psi_copy(s, gone):
        return remote(psi_ref.at[1 - yl, s], psi_at(s, sub if gone else 1 - sub), io_s.at[s], io_r.at[s], yl_partner)

    for s in PAIR:
        psi_load(s).start()
        psi_copy(s, GONE).start()
    for e in range(3 * PIECES):
        r_copy(0, e, GONE).start()
    for r in TRIPLE:
        r_load(r).start()
    for l in TRIPLE:
        l_load(l).start()
    pl.semaphore_signal(credit, inc=1, device_id=sibling, device_id_type=MESH)

    def clear(i):
        for s in PAIR:
            vbuf[1, s, own_block(i), :] = jnp.zeros((ROWS, wa), jnp.float32)
            for p in PAIR:
                vv[p, s, block(i), :] = jnp.zeros((ROWS, wa), jnp.float32)

    fold(clear, wb // ROWS)
    clear_products()
    sc[2] = jnp.zeros((ROWS, wa), jnp.float32)
    def work(name, p, more, slot):
        kind, tail = name[0], name[1:]
        if kind == "m":
            return functools.partial(right_group, p, int(tail[0]), int(tail[1]), tail[2])
        args = [int(digit) for digit in tail]
        if kind in "ab":
            calls = {
                "a0": lambda: alpha_open(p),
                "b0": lambda: (alpha_close(slot), beta_open(p)),
                "b3": lambda: (beta_close(slot), scale(p)),
            }
            return calls.get(name, functools.partial(sum_pass, "ab".index(kind), args[0]))
        if kind == "c":
            return functools.partial(close_chunk, p, *args, more)
        if kind == "d":
            return functools.partial(drain_gather, p)
        if kind == "l":
            return functools.partial(left_products, *args)
        return functools.partial({"p": take_pair, "h": take_hop, "f": left_sum, "o": open_cross}[kind], p, *args)

    gather_order = ",".join(GATHER_ORDER).split(",")
    reduce_order = ",".join(REDUCE_ORDER).split(",")
    r_plan = []
    for e in range(3 * PIECES + 2):
        if e < 3 * PIECES:
            r_plan.append(functools.partial(r_first, e))
        if e > 1:
            r_plan.append(functools.partial(r_second, e - 2))

    for s in PAIR:
        psi_load(s).wait()
        psi_copy(s, HERE).wait_recv()
        own_sends(0, s * SPLIT)
    served = [name for name in reduce_order if name[0] in "phc"]
    for n, name in enumerate(served):
        if name[0] != "c":
            work(name, 0, None, None)()
        elif int(name[1]) % SPLIT:
            own_sends(0, int(name[1]))
        if n % 3 > 0 and n * 3 > len(served):
            r_plan.pop(0)()
    for r in TRIPLE:
        r_load(r).wait()
        l_load(r).wait()
    for s in PAIR:
        psi_copy(s, GONE).wait_send()

    def lanczos_step(j, carry):
        p = j % 2
        slot = (j + LANCZOS_STEPS - 1) % LANCZOS_STEPS
        more = j < LANCZOS_STEPS - 1

        rest = list(r_plan)
        for name in gather_order:
            if name[0] == "m" and rest is not None or name[0] in "ph" and rest:
                now = len(rest) if name[0] == "m" else 2

                @pl.when(j == 0)
                def _():
                    for _ in range(min(now, len(rest))):
                        rest.pop(0)()
                    if name[0] == "m":
                        r_last()

                rest = None if name[0] == "m" else rest
            work(name, p, more, slot)()
        mix()

        pl.semaphore_wait(credit, 1)
        for name in reduce_order:
            if name[0] in "ph":
                pl.when(more)(work(name, 1 - p, more, slot))
            else:
                work(name, p, more, slot)()
        for i in range(4):
            sib_copy(chunks[-1], i).wait_send()
        for q in chunks:
            drain_sums(p, q)

        @pl.when(more)
        def _():
            pl.semaphore_signal(credit, inc=1, device_id=sibling, device_id_type=MESH)

        sc[2] = jnp.where(j > 0, sc[1], jnp.zeros((ROWS, wa), jnp.float32))
        return carry

    lax.fori_loop(0, LANCZOS_STEPS, lanczos_step, 0)

    p = LANCZOS_STEPS % 2

    def out_copy(s):
        src = vv.at[1 - p, s, span((1 - sub) * half, half), :]
        return remote(src, ob.at[s], io_s.at[2 + s], io_r.at[2 + s], yl_partner)

    alpha_open(p)
    sum_pass(0, 1)
    sum_pass(0, 2)
    alpha_close(LANCZOS_STEPS - 1)
    beta_open(p)
    for s in PAIR:
        out_copy(s).start()
    sum_pass(1, 1)
    sum_pass(1, 2)
    beta_close(LANCZOS_STEPS - 1)
    for s in PAIR:
        out_copy(s).wait_recv()

        def put(i):
            vout_ref[yl, s, block(i), :] = vv[1 - p, s, span(sub * half + i * ROWS, ROWS), :] / sc[1]
            vout_ref[1 - yl, s, block(i), :] = ob[s, block(i), :] / sc[1]

        fold(put, half // ROWS)
        out_copy(s).wait_send()


def solution(mesh):
    nz, nx = mesh.shape["col"] // 4, mesh.shape["row"] // 2

    def local_steps(psi_blk, left_blk, mpo_tensor, right_blk):
        wa, wb = psi_blk.shape[0] // 2, psi_blk.shape[2] * 2
        da, db = left_blk.shape[2], right_blk.shape[2]
        half = wb // 2
        hops = nz // 2
        mb = wb // SPLIT
        parts = 2 * SPLIT
        lanes = 128 if wa % 128 == 0 else wa
        f32 = jnp.float32
        psi_t = jnp.transpose(psi_blk.reshape(2, wa, 2, half), (0, 2, 3, 1))
        kernel = functools.partial(lanczos_kernel, nz, nx, wa, wb)
        vmem, dma = pltpu.VMEM, pltpu.SemaphoreType.DMA
        ids = 8 * hops + 2
        scalars, v_out = pl.pallas_call(
            kernel,
            out_shape=(
                jax.ShapeDtypeStruct((2 * LANCZOS_STEPS, ROWS, lanes), f32),
                jax.ShapeDtypeStruct((2, 2, half, wa), f32),
            ),
            in_specs=[
                pl.BlockSpec(memory_space=pl.ANY),
                pl.BlockSpec(memory_space=pl.ANY),
                pl.BlockSpec(memory_space=pltpu.SMEM),
                pl.BlockSpec(memory_space=pl.ANY),
            ],
            out_specs=(pl.BlockSpec(memory_space=pltpu.VMEM),) * 2,
            scratch_shapes=[
                vmem((2, 2, db, wa), f32),
                vmem((3 * wa, da), f32),
                vmem((3 * wb, db), f32),
                vmem((2, 3 * wb, wa), f32),
                vmem((2, wb, 3 * wa), f32),
                vmem((2, 2, wb, wa), f32),
                vmem((parts, 4, mb, 2 * wa), f32),
                vmem((8, mb, 2 * wa), f32),
                vmem((2, parts, 2, 2, mb // 2, wa), f32),
                vmem((2, parts, 2, 2, mb, wa), f32),
                vmem((2, parts, mb, wa), f32),
                vmem((2, half, wa), f32),
                vmem((2, nx * 2 + 4 + nz, ROWS, lanes), f32),
                vmem((3, ROWS, wa), f32),
                dma((parts, ids)),
                dma((2, parts, ids)),
                dma((4,)),
                dma((parts, 4)),
                dma((parts, 2, 2)),
                dma((2, parts, 2, 2)),
                dma((parts, 2, 2)),
                dma((2, parts, 2, 2)),
                dma((parts,)),
                dma((2, parts)),
                dma((2, 3)),
                dma((2, 3)),
                dma((4, 3 * PIECES)),
                dma((4, 3 * PIECES)),
                dma((4,)),
                dma((4,)),
                dma((8,)),
                pltpu.SemaphoreType.REGULAR,
            ],
            compiler_params=pltpu.CompilerParams(has_side_effects=True, vmem_limit_bytes=66 * 1000 * 1000),
            name="lanczos",
        )(psi_t, jnp.transpose(left_blk, (1, 0, 2)), mpo_tensor.reshape(-1), jnp.transpose(right_blk, (1, 0, 2)))
        v_next = jnp.transpose(v_out, (0, 3, 1, 2)).reshape(psi_blk.shape)
        return scalars[:LANCZOS_STEPS, 0, 0], scalars[LANCZOS_STEPS:, 0, 0], v_next

    return jax.shard_map(
        local_steps,
        mesh=mesh,
        in_specs=(P("row", None, "col"), P("row", None, None), P(), P("col", None, None)),
        out_specs=(P(), P(), P("row", None, "col")),
        check_vma=False,
    )
```

```python
import functools

import jax
import jax.numpy as jnp
from jax import lax
from jax.experimental import pallas as pl
from jax.experimental.pallas import tpu as pltpu
from jax.sharding import PartitionSpec as P

LANCZOS_STEPS = 4
EXACT_PREC = lax.Precision.HIGHEST
MESH = pl.DeviceIdType.MESH
ROWS = 8
SPLIT = 2
PIECES = 2
GATHER_ORDER = (
    "a0,h103,p2,h113,h123,h202,h212,h301,h311,m00*,h104,h221,m01+",
    "h114,h124,m01-,h203,p3,h213,m02+,h302,m02-,h312,a1,m03+,h222",
    "h204,m03-,h321,m10*,h214,h303,m11+,h313,m11-,h223,m04*,h322",
    "b0,h304,m12+,h314,h224,m12-,h323,m13+,m13-,h324,b1,m14*",
)
REDUCE_ORDER = (
    "l00,f000,l01,l02,f030,f010,f020,x1,d0,b3,f011,f021,l10,f100",
    "l11,l12,f130,x2,l20,c0,f110,f120,f111,f121,f200,l21,l22,p0",
    "h001,h011,f230,x3,l30,h021,c1,f300,l31,h002,h012,f210,f220",
    "f211,f221,h022,l32,p1,h101,h111,f330,f310,f320,f311,f321",
    "h003,h013,h023,h121,c2,h102,h112,h004,h014,h024,h122,h201",
    "h211,c3",
)
PAIR = range(2)
TRIPLE = range(3)
WAYS = (1, -1)
GONE, HERE = True, False


def fold(body, count, unroll=4):
    while count % unroll:
        unroll //= 2

    def trip(i, carry):
        for u in range(unroll):
            body(i * unroll + u)
        return carry

    lax.fori_loop(0, count // unroll, trip, 0)


def lanczos_kernel(
    nz, nx, wa, wb,
    psi_ref, l_hbm, w_ref, r_hbm,
    scal_ref, vout_ref,
    vbuf, lbuf, rbuf, ubuf, tbuf, vv, rd, yb, hx, fx, yx, ob, red, sc,
    ag_s, ag_r, rd_s, rd_r, hx_s, hx_r, fx_s, fx_r, yx_s, yx_r,
    ar_s, ar_r, rr_s, rr_r, io_s, io_r, ld_s, credit,
):
    hops = nz // 2
    half, mb = wb // 2, wb // SPLIT
    part = half // (2 * nx)
    bit = part // PIECES
    chunks = range(2 * SPLIT)
    col, row = lax.axis_index("col"), lax.axis_index("row")
    div, mod = lax.div, lax.rem
    z, y, x, c = div(col, 4), mod(col, 4), div(row, 2), mod(row, 2)
    yh, sub = div(y, 2), mod(y, 2)
    yl = mod(div(y + 1, 2), 2)

    def dev(zz=None, yy=None, xx=None, cc=None):
        zz = z if zz is None else zz
        yy = y if yy is None else yy
        xx = x if xx is None else xx
        cc = c if cc is None else cc
        return {"col": zz * 4 + yy, "row": xx * 2 + cc}

    zs = {off: mod(z + off + nz, nz) for off in range(-hops, nz)}
    xs = {off: mod(x + off + nx, nx) for off in range(-1, nx)}
    starts = {off: (at * 2 + yh) * wb for off, at in zs.items()}
    others = {off: (at * 2 + 1 - yh) * wb for off, at in zs.items()}
    own = starts[0]

    sibling = dev(cc=1 - c)
    yl_partner = dev(yy=y + 1 - 2 * sub)
    yh_partner = dev(yy=3 - y)
    z_next = {d: dev(zz=zs[d]) for d in WAYS}
    x_next = {d: dev(xx=xs[d]) for d in WAYS}
    x_side = {d: dev(yy=y + 1 - 2 * sub, xx=xs[d]) for d in WAYS}

    def remote(src, dst, send, recv, to):
        return pltpu.make_async_remote_copy(
            src_ref=src, dst_ref=dst, send_sem=send, recv_sem=recv, device_id=to, device_id_type=MESH
        )

    def span(start, count):
        return pl.ds(pl.multiple_of(start, ROWS), count)

    def block(i):
        return span(i * ROWS, ROWS)

    def cut(q):
        return mb * (96, 96, 64, 32)[q] // 128

    def lines(q):
        return TRIPLE if cut(q) else TRIPLE[1:]

    def piece(p, q, base, kind, d, h, mid, to):
        start, count = (0, cut(q)) if kind == 0 else (cut(q), mb - cut(q))
        if h == hops:
            count //= 2
            start += count if d < 0 else 0
        at = vbuf.at[p, q // SPLIT, span(base + (q % SPLIT) * mb + start, count), :]
        return remote(at, at, ag_s.at[q, mid], ag_r.at[p, q, mid], to)

    def z_copy(p, q, d, line, h, gone):
        base = (others if line == 2 else starts)[-d * (h - 1 if gone else h)]
        mid = ((0 if d > 0 else 3) + line) * hops + h - 1
        return piece(p, q, base, min(line, 1), d, h, mid, z_next[d])

    def pair_copy(p, q, kind, d, h, gone):
        mid = 6 * hops + (2 * h + max(d, 0) if h else 0 if kind else 1)
        return piece(p, q, (starts if gone else others)[-d * h], kind, d, h, mid, yh_partner)

    def own_sends(p, q):
        pair_copy(p, q, 1, 0, 0, GONE).start()
        for line in lines(q)[:-1]:
            for d in WAYS:
                z_copy(p, q, d, line, 1, GONE).start()
        if cut(q):
            pair_copy(p, q, 0, 0, 0, GONE).start()

    def take_pair(p, q):
        pair_copy(p, q, 1, 0, 0, HERE).wait_recv()
        for d in WAYS:
            z_copy(p, q, d, 2, 1, GONE).start()

    def take_hop(p, q, line, h):
        for d in WAYS:
            z_copy(p, q, d, line, h, HERE).wait_recv()
            if h < hops:
                z_copy(p, q, d, line, h + 1, GONE).start()
            if line == 0:
                pair_copy(p, q, 0, d, h, GONE).start()

    def drain_gather(p):
        for q in chunks:
            first = range(0 if cut(q) else 1, 2)
            for kind in first:
                pair_copy(p, q, kind, 0, 0, GONE).wait_send()
            for d in WAYS:
                for h in range(1, hops + 1):
                    for line in lines(q):
                        z_copy(p, q, d, line, h, GONE).wait_send()
                    for _ in first[1:]:
                        pair_copy(p, q, 0, d, h, GONE).wait_send()

    plane = nx * 8

    line = [mod(row * 4 + y + d, plane) for d in range(plane)]
    groups = (
        (0, plane, row * 4 + y, [{"col": z * 4 + mod(at, 4), "row": div(at, 4)} for at in line]),
        (plane, nz, z, [dev(zz=zs[d]) for d in range(nz)]),
    )

    def sum_send(which, stage, tile):
        base, count, me, peers = groups[stage]
        red[which, base + me] = tile
        at = red.at[which, base + me]
        for d in range(1, count):
            remote(at, at, ar_s.at[which, stage], ar_r.at[which, stage], peers[d]).start()

    def sum_take(which, stage):
        base, count, _, _ = groups[stage]
        at = red.at[which, pl.ds(base, count - 1)]
        pltpu.make_async_copy(at, at, ar_r.at[which, stage]).wait()
        pltpu.make_async_copy(at, at, ar_s.at[which, stage]).wait()
        total = red[which, base]
        for i in range(1, count):
            total = total + red[which, base + i]
        return total

    def sum_pass(which, stage):
        sum_send(which, stage, sum_take(which, stage - 1))

    lanes = red.shape[-1]

    def narrow(tile):
        out = tile[:, :lanes]
        for i in range(1, wa // lanes):
            out = out + tile[:, i * lanes : (i + 1) * lanes]
        return out

    def own_block(i):
        return span(own + i * ROWS, ROWS)

    def accumulate(term):
        def trip(i, acc):
            for s in PAIR:
                acc = acc + term(s, i)
            return acc

        return lax.fori_loop(0, wb // ROWS, trip, jnp.zeros((ROWS, wa), jnp.float32), unroll=4)

    def alpha_open(p):
        acc = accumulate(lambda s, i: vv[p, s, block(i), :] * vbuf[p, s, own_block(i), :])
        sum_send(0, 0, narrow(acc))

    def alpha_close(slot):
        value = jnp.full((ROWS, wa), jnp.sum(sum_take(0, 1)), jnp.float32)
        sc[0] = value
        scal_ref[slot] = value[:, :lanes]

    def beta_open(p):
        alpha, beta = sc[0], sc[2]

        def term(s, i):
            u = vbuf[p, s, own_block(i), :] - alpha * vv[p, s, block(i), :] - beta * vv[1 - p, s, block(i), :]
            vv[1 - p, s, block(i), :] = u
            return u * u

        sum_send(1, 0, narrow(accumulate(term)))

    def beta_close(slot):
        value = jnp.sqrt(jnp.full((ROWS, wa), jnp.sum(sum_take(1, 1)), jnp.float32))
        sc[1] = value
        scal_ref[LANCZOS_STEPS + slot] = value[:, :lanes]

    def scale(p):
        def trip(i):
            for s in PAIR:
                vv[1 - p, s, block(i), :] = vv[1 - p, s, block(i), :] / sc[1]

        fold(trip, wb // ROWS)

    def r_rows(e, of_sub, xx, cc):
        start = (e // PIECES) * wb + of_sub * half + (xx * 2 + cc) * part + (e % PIECES) * bit
        return rbuf.at[span(start, bit), :]

    def r_copy(way, e, gone):
        if way == 0:
            src = r_hbm.at[e // PIECES, span(row * part + (e % PIECES) * bit, bit), :]
            return remote(src, r_rows(e, sub if gone else 1 - sub, x, c), rr_s.at[0, e], rr_r.at[0, e], yl_partner)
        over = isinstance(way, tuple)
        from_way = way[0] if over else way
        slot = from_way % 4
        d = from_way if from_way in WAYS else 1 if e % PIECES == 0 else -1
        away = {0: 0, 2: 2}.get(from_way, -d) - (d if gone and not over else 0)
        away = -d if gone and not over and from_way == 2 else 0 if gone and not over else away
        at = r_rows(e, 1 - sub, xs[away], 1 - c if over and not gone else c)
        slot = slot + 4 if over else slot
        return remote(at, at, rr_s.at[slot, e], rr_r.at[slot, e], sibling if over else x_next[d])

    def r_take(way, e):
        for d in WAYS if way == 1 else (way,):
            r_copy(d, e, HERE).wait_recv()
            r_copy((d,), e, GONE).start()
            if way == 0:
                for n in WAYS:
                    r_copy(n, e, GONE).start()
            elif way == 1 and d == (1 if e % PIECES == 0 else -1):
                r_copy(2, e, GONE).start()

    def r_last():
        for e in range(3 * PIECES):
            for way in (0, 1, -1, 2):
                r_copy((way,), e, HERE).wait_recv()
                r_copy((way,), e, GONE).wait_send()
                r_copy(way, e, GONE).wait_send()

    def right_group(p, s, h, way):
        d = 1 if way == "+" else -1
        for q in range(s * SPLIT, s * SPLIT + SPLIT):
            for e in (d,) if way != "*" else WAYS if h else (0,):
                if cut(q):
                    pair_copy(p, q, 0, e, h, HERE).wait_recv()

        def one(i, carry):
            start = pl.multiple_of((zs[-d * h] * 2 + i) * wb, wb)
            ubuf[s] = ubuf[s] + jnp.dot(
                rbuf[:, pl.ds(start, wb)],
                vbuf[p, s, pl.ds(start, wb), :],
                precision=EXACT_PREC,
                preferred_element_type=jnp.float32,
            )
            return carry

        lax.fori_loop(0, 2, one, 0)

    def clear_products():
        def trip(i):
            for s in PAIR:
                ubuf[s, block(i), :] = jnp.zeros((ROWS, wa), jnp.float32)

        fold(trip, 3 * wb // ROWS)

    def mix(q):
        t, base = q // SPLIT, (q % SPLIT) * mb

        def trip(i):
            tiles = [[ubuf[s, span(r * wb + base + i * ROWS, ROWS), :] for s in PAIR] for r in TRIPLE]
            for l in TRIPLE:
                acc = None
                for r in TRIPLE:
                    for s in PAIR:
                        term = w_ref[((l * 3 + r) * 2 + s) * 2 + t] * tiles[r][s]
                        acc = term if acc is None else acc + term
                tbuf[t, span(base + i * ROWS, ROWS), l * wa : (l + 1) * wa] = acc

        fold(trip, mb // ROWS, 1)
        if q == chunks[-1]:
            clear_products()

    def sib_copy(q, i):
        return remote(yb.at[i], rd.at[q, i], rd_s.at[i], rd_r.at[q, i], sibling)

    def left_products(q, part):
        def one(n, carry):
            theirs = n < (2, 2, 0)[part]
            i = mod(n, 2) if part == 0 else n + 3 - part
            away = jnp.where(i < 2, i + 2, 3 - i)
            start = (mod(x + away, nx) * 2 + jnp.where(theirs, 1 - c, c)) * 2 * wa
            yb[jnp.where(theirs, i, i + 4)] = jnp.dot(
                tbuf[q // SPLIT, (q % SPLIT) * mb : (q % SPLIT + 1) * mb, :],
                lbuf[:, pl.ds(pl.multiple_of(start, 2 * wa), 2 * wa)],
                precision=EXACT_PREC,
                preferred_element_type=jnp.float32,
            )

            @pl.when(theirs)
            def _():
                sib_copy(q, i).start()

            return carry

        for i in ((0, 1), (2, 3), ())[part] if q else ():
            sib_copy(q - 1, i).wait_send()
        lax.fori_loop(0, (3, 2, 3)[part], one, 0)

    lane_at = {GONE: (1 - yl) * wa, HERE: yl * wa}

    def lane(theirs):
        return pl.ds(pl.multiple_of(lane_at[theirs], wa), wa)

    def half_copy(p, q, d, theirs):
        slot, side = 0 if d > 0 else 1, 0 if theirs else 1
        src = rd.at[q, 0, pl.ds(slot * mb // 2, mb // 2), lane(theirs)]
        return remote(src, hx.at[p, q, slot, side], hx_s.at[q, slot, side], hx_r.at[p, q, slot, side], x_next[d])

    def full_copy(p, q, d, theirs):
        slot, side = 0 if d > 0 else 1, 0 if theirs else 1
        src = rd.at[q, 2 - slot, :, lane(theirs)]
        to = (x_side if theirs else x_next)[d]
        return remote(src, fx.at[p, q, slot, side], fx_s.at[q, slot, side], fx_r.at[p, q, slot, side], to)

    def cross_copy(p, q):
        return remote(rd.at[q, 3, :, lane(GONE)], yx.at[p, q], yx_s.at[q], yx_r.at[p, q], yl_partner)

    def left_sum(p, q, i, side):
        if side == 0:
            sib_copy(q, i).wait_recv()

            def add(k):
                rows = block(k)
                rd[q, i, rows, :] = rd[q, i, rows, :] + yb[i + 4, rows, :]

            fold(add, mb // ROWS)
        if i == 0:
            for theirs in (GONE, HERE):
                for d in WAYS:
                    half_copy(p, q, d, theirs).start()
        elif i < 3:
            d, theirs = 2 * i - 3, side == 0
            lanes_at = lane(theirs)
            half_copy(p, q, d, theirs).wait_recv()

            def add_half(k):
                rows = span(k * ROWS + (0 if d > 0 else mb // 2), ROWS)
                rd[q, i, rows, lanes_at] = rd[q, i, rows, lanes_at] + hx[p, q, i % 2, side, block(k), :]

            fold(add_half, mb // 2 // ROWS)
            full_copy(p, q, d, theirs).start()
        else:
            cross_copy(p, q).start()

    def close_chunk(p, q, more):
        for theirs in (GONE, HERE):
            for d in WAYS:
                full_copy(p, q, d, theirs).wait_recv()
        cross_copy(p, q).wait_recv()
        alpha, beta, old = sc[0], sc[1], sc[2]
        s, mine = q // SPLIT, lane(HERE)

        def step(k):
            rows, at = block(k), own_block(k + (q % SPLIT) * mb // ROWS)
            g = rd[q, 3, rows, mine] + yx[p, q, rows, :]
            for slot in PAIR:
                g = g + (fx[p, q, slot, 0, rows, :] + fx[p, q, slot, 1, rows, :])
            vbuf[1 - p, s, at, :] = (g - alpha * vbuf[p, s, at, :] - old * vbuf[1 - p, s, at, :]) / beta

        fold(step, mb // ROWS)

        @pl.when(more)
        def _():
            own_sends(1 - p, q)

    def drain_sums(p, q):
        for theirs in (GONE, HERE):
            for d in WAYS:
                half_copy(p, q, d, theirs).wait_send()
                full_copy(p, q, d, theirs).wait_send()
        cross_copy(p, q).wait_send()

    def l_load(l):
        return pltpu.make_async_copy(l_hbm.at[l, span(yl * wa, wa), :], lbuf.at[pl.ds(l * wa, wa), :], ld_s.at[l])

    def r_load(r):
        return pltpu.make_async_copy(r_hbm.at[r], rbuf.at[span(r * wb + sub * half, half), :], ld_s.at[3 + r])

    def psi_at(s, of_sub):
        return vbuf.at[0, s, span(own + of_sub * half, half), :]

    def psi_load(s):
        return pltpu.make_async_copy(psi_ref.at[yl, s], psi_at(s, sub), ld_s.at[6 + s])

    def psi_copy(s, gone):
        return remote(psi_ref.at[1 - yl, s], psi_at(s, sub if gone else 1 - sub), io_s.at[s], io_r.at[s], yl_partner)

    for s in PAIR:
        psi_load(s).start()
    barrier = pltpu.get_barrier_semaphore()
    for _, count, _, peers in groups:
        for d in range(1, count):
            pl.semaphore_signal(barrier, inc=1, device_id=peers[d], device_id_type=MESH)
    pl.semaphore_wait(barrier, plane + nz - 2)
    for s in PAIR:
        psi_copy(s, GONE).start()
    for e in range(3 * PIECES):
        r_copy(0, e, GONE).start()
    for r in TRIPLE:
        r_load(r).start()
    for l in TRIPLE:
        l_load(l).start()
    pl.semaphore_signal(credit, inc=1, device_id=sibling, device_id_type=MESH)

    def clear(i):
        for s in PAIR:
            vbuf[1, s, own_block(i), :] = jnp.zeros((ROWS, wa), jnp.float32)
            for p in PAIR:
                vv[p, s, block(i), :] = jnp.zeros((ROWS, wa), jnp.float32)

    fold(clear, wb // ROWS)
    clear_products()
    sc[2] = jnp.zeros((ROWS, wa), jnp.float32)
    def work(name, p, more, slot):
        kind, tail = name[0], name[1:]
        if kind == "m":
            return functools.partial(right_group, p, int(tail[0]), int(tail[1]), tail[2])
        args = [int(digit) for digit in tail]
        if kind in "ab":
            calls = {
                "a0": lambda: alpha_open(p),
                "b0": lambda: (alpha_close(slot), beta_open(p)),
                "b3": lambda: (beta_close(slot), scale(p)),
            }
            return calls.get(name, functools.partial(sum_pass, "ab".index(kind), args[0]))
        if kind == "c":
            return functools.partial(close_chunk, p, *args, more)
        if kind == "d":
            return functools.partial(drain_gather, p)
        if kind in "lx":
            return functools.partial({"l": left_products, "x": mix}[kind], *args)
        return functools.partial({"p": take_pair, "h": take_hop, "f": left_sum}[kind], p, *args)

    gather_order = ",".join(GATHER_ORDER).split(",")
    reduce_order = ",".join(REDUCE_ORDER).split(",")
    r_plan = []
    for e in range(3 * PIECES + 4):
        for way in TRIPLE:
            if 0 <= e - 2 * way < 3 * PIECES:
                r_plan.append(functools.partial(r_take, way, e - 2 * way))

    for s in PAIR:
        psi_load(s).wait()
        psi_copy(s, HERE).wait_recv()
        own_sends(0, s * SPLIT)
    served = [name for name in reduce_order if name[0] in "phc"]
    for n, name in enumerate(served):
        if name[0] != "c":
            work(name, 0, None, None)()
        elif int(name[1]) % SPLIT:
            own_sends(0, int(name[1]))
        if n % 2 == 0 and n * 3 > len(served):
            r_plan.pop(0)()
    for r in TRIPLE:
        r_load(r).wait()
        l_load(r).wait()
    for s in PAIR:
        psi_copy(s, GONE).wait_send()

    def lanczos_step(j, carry):
        p = mod(j, 2)
        slot = mod(j + LANCZOS_STEPS - 1, LANCZOS_STEPS)
        more = j < LANCZOS_STEPS - 1

        rest = list(r_plan)
        for name in gather_order:
            if name[0] == "m" and rest is not None or name[0] in "ph" and rest:
                now = len(rest) if name[0] == "m" else 2

                @pl.when(j == 0)
                def _():
                    for _ in range(min(now, len(rest))):
                        rest.pop(0)()
                    if name[0] == "m":
                        r_last()

                rest = None if name[0] == "m" else rest
            work(name, p, more, slot)()
        mix(0)

        pl.semaphore_wait(credit, 1)
        for name in reduce_order:
            if name[0] in "ph":
                pl.when(more)(work(name, 1 - p, more, slot))
            else:
                work(name, p, more, slot)()
        for i in range(4):
            sib_copy(chunks[-1], i).wait_send()
        for q in chunks:
            drain_sums(p, q)

        @pl.when(more)
        def _():
            pl.semaphore_signal(credit, inc=1, device_id=sibling, device_id_type=MESH)

        sc[2] = jnp.where(j > 0, sc[1], jnp.zeros((ROWS, wa), jnp.float32))
        return carry

    lax.fori_loop(0, LANCZOS_STEPS, lanczos_step, 0)

    p = LANCZOS_STEPS % 2

    def out_copy(s):
        src = vv.at[1 - p, s, span((1 - sub) * half, half), :]
        return remote(src, ob.at[s], io_s.at[2 + s], io_r.at[2 + s], yl_partner)

    alpha_open(p)
    sum_pass(0, 1)
    alpha_close(LANCZOS_STEPS - 1)
    beta_open(p)
    for s in PAIR:
        out_copy(s).start()
    sum_pass(1, 1)
    beta_close(LANCZOS_STEPS - 1)
    for s in PAIR:
        out_copy(s).wait_recv()

        def put(i):
            vout_ref[yl, s, block(i), :] = vv[1 - p, s, span(sub * half + i * ROWS, ROWS), :] / sc[1]
            vout_ref[1 - yl, s, block(i), :] = ob[s, block(i), :] / sc[1]

        fold(put, half // ROWS)
        out_copy(s).wait_send()


def solution(mesh):
    nz, nx = mesh.shape["col"] // 4, mesh.shape["row"] // 2

    def local_steps(psi_blk, left_blk, mpo_tensor, right_blk):
        wa, wb = psi_blk.shape[0] // 2, psi_blk.shape[2] * 2
        da, db = left_blk.shape[2], right_blk.shape[2]
        half = wb // 2
        hops = nz // 2
        mb = wb // SPLIT
        parts = 2 * SPLIT
        lanes = 128 if wa % 128 == 0 else wa
        f32 = jnp.float32
        psi_t = jnp.transpose(psi_blk.reshape(2, wa, 2, half), (0, 2, 3, 1))
        kernel = functools.partial(lanczos_kernel, nz, nx, wa, wb)
        vmem, dma = pltpu.VMEM, pltpu.SemaphoreType.DMA
        ids = 8 * hops + 2
        scalars, v_out = pl.pallas_call(
            kernel,
            out_shape=(
                jax.ShapeDtypeStruct((2 * LANCZOS_STEPS, ROWS, lanes), f32),
                jax.ShapeDtypeStruct((2, 2, half, wa), f32),
            ),
            in_specs=[
                pl.BlockSpec(memory_space=pl.ANY),
                pl.BlockSpec(memory_space=pl.ANY),
                pl.BlockSpec(memory_space=pltpu.SMEM),
                pl.BlockSpec(memory_space=pl.ANY),
            ],
            out_specs=(pl.BlockSpec(memory_space=pltpu.VMEM),) * 2,
            scratch_shapes=[
                vmem((2, 2, db, wa), f32),
                vmem((3 * wa, da), f32),
                vmem((3 * wb, db), f32),
                vmem((2, 3 * wb, wa), f32),
                vmem((2, wb, 3 * wa), f32),
                vmem((2, 2, wb, wa), f32),
                vmem((parts, 4, mb, 2 * wa), f32),
                vmem((8, mb, 2 * wa), f32),
                vmem((2, parts, 2, 2, mb // 2, wa), f32),
                vmem((2, parts, 2, 2, mb, wa), f32),
                vmem((2, parts, mb, wa), f32),
                vmem((2, half, wa), f32),
                vmem((2, nx * 8 + nz, ROWS, lanes), f32),
                vmem((3, ROWS, wa), f32),
                dma((parts, ids)),
                dma((2, parts, ids)),
                dma((4,)),
                dma((parts, 4)),
                dma((parts, 2, 2)),
                dma((2, parts, 2, 2)),
                dma((parts, 2, 2)),
                dma((2, parts, 2, 2)),
                dma((parts,)),
                dma((2, parts)),
                dma((2, 2)),
                dma((2, 2)),
                dma((8, 3 * PIECES)),
                dma((8, 3 * PIECES)),
                dma((4,)),
                dma((4,)),
                dma((8,)),
                pltpu.SemaphoreType.REGULAR,
            ],
            compiler_params=pltpu.CompilerParams(collective_id=0, has_side_effects=True, vmem_limit_bytes=66 * 1000 * 1000),
            name="lanczos",
        )(psi_t, jnp.transpose(left_blk, (1, 0, 2)), mpo_tensor.reshape(-1), jnp.transpose(right_blk, (1, 0, 2)))
        v_next = jnp.transpose(v_out, (0, 3, 1, 2)).reshape(psi_blk.shape)
        return scalars[:LANCZOS_STEPS, 0, 0], scalars[LANCZOS_STEPS:, 0, 0], v_next

    return jax.shard_map(
        local_steps,
        mesh=mesh,
        in_specs=(P("row", None, "col"), P("row", None, None), P(), P("col", None, None)),
        out_specs=(P(), P(), P("row", None, "col")),
        check_vma=False,
    )
```

```python
import functools

import jax
import jax.numpy as jnp
from jax import lax
from jax.experimental import pallas as pl
from jax.experimental.pallas import tpu as pltpu
from jax.sharding import PartitionSpec as P

LANCZOS_STEPS = 4
EXACT_PREC = lax.Precision.HIGHEST
MESH = pl.DeviceIdType.MESH
ROWS = 8
SPLIT = 2
PIECES = 2
START_ORDER = (
    "h001,r00,p0,h011,c1,h021,h002,r01,r02,r10,h101,p1,r03,h022",
    "r11,h121,h012,r04,h023,h102,h013,c3,r05,r20,r12,r13,r21,h111",
    "h122,h003,h112,r14,r15,h201,r22,h113,p2,h211",
)
GATHER_ORDER = (
    "h004,h114,r23,h014,h123,r24,r25,a0,h301,h103,w,h202,h024",
    "m02+,h221,m02-,p3,m01+,h311,h104,h212,h302,m00*,h203,m01-",
    "m10*,h222,m03+,a1,h321,h124,m11+,h303,h312,m03-,h223,m11-",
    "h322,m04*,h204,h304,b0,m12+,h213,h313,h224,m12-,h323,m13-",
    "m13+,h314,h214,b1,h324,m14*",
)
REDUCE_ORDER = (
    "d0,l00,f000,x2,x1,l01,f030,l02,f020,b3,f010,f011,l10,f021",
    "l11,f100,l12,f130,l20,f120,c0,f110,l21,p0,f121,f111,x3,f200",
    "h001,l22,h011,h021,l30,f300,f230,c1,h002,f220,f210,l31,p1",
    "h111,f211,h012,f221,l32,f320,h101,f310,h022,f311,h003,h112",
    "f330,h121,c2,f321,h122,h013,h113,h102,h023,h211,p2,h201,c3",
)
PAIR = range(2)
TRIPLE = range(3)
WAYS = (1, -1)
GONE, HERE = True, False


def fold(body, count, unroll=4):
    while count % unroll:
        unroll //= 2

    def trip(i, carry):
        for u in range(unroll):
            body(i * unroll + u)
        return carry

    lax.fori_loop(0, count // unroll, trip, 0)


def lanczos_kernel(
    nz, nx, wa, wb,
    psi_ref, l_hbm, w_ref, r_hbm,
    scal_ref, vout_ref,
    vbuf, lbuf, rbuf, ubuf, tbuf, vv, rd, yb, hx, fx, yx, ob, red, sc,
    ag_s, ag_r, rd_s, rd_r, hx_s, hx_r, fx_s, fx_r, yx_s, yx_r,
    ar_s, ar_r, rr_s, rr_r, io_s, io_r, ld_s, credit,
):
    hops = nz // 2
    half, mb = wb // 2, wb // SPLIT
    part = half // (2 * nx)
    bit = part // PIECES
    chunks = range(2 * SPLIT)
    col, row = lax.axis_index("col"), lax.axis_index("row")
    div, mod = lax.div, lax.rem
    z, y, x, c = div(col, 4), mod(col, 4), div(row, 2), mod(row, 2)
    yh, sub = div(y, 2), mod(y, 2)
    yl = mod(div(y + 1, 2), 2)

    def dev(zz=None, yy=None, xx=None, cc=None):
        zz = z if zz is None else zz
        yy = y if yy is None else yy
        xx = x if xx is None else xx
        cc = c if cc is None else cc
        return {"col": zz * 4 + yy, "row": xx * 2 + cc}

    zs = {off: mod(z + off + nz, nz) for off in range(-hops, nz)}
    xs = {off: mod(x + off + nx, nx) for off in range(-1, nx)}
    starts = {off: (at * 2 + yh) * wb for off, at in zs.items()}
    others = {off: (at * 2 + 1 - yh) * wb for off, at in zs.items()}
    own = starts[0]

    sibling = dev(cc=1 - c)
    yl_partner = dev(yy=y + 1 - 2 * sub)
    yh_partner = dev(yy=3 - y)
    z_next = {d: dev(zz=zs[d]) for d in WAYS}
    x_next = {d: dev(xx=xs[d]) for d in WAYS}
    x_side = {d: dev(yy=y + 1 - 2 * sub, xx=xs[d]) for d in WAYS}

    def remote(src, dst, send, recv, to):
        return pltpu.make_async_remote_copy(
            src_ref=src, dst_ref=dst, send_sem=send, recv_sem=recv, device_id=to, device_id_type=MESH
        )

    def span(start, count):
        return pl.ds(pl.multiple_of(start, ROWS), count)

    def block(i):
        return span(i * ROWS, ROWS)

    def cut(q):
        return mb * (96, 96, 64, 32)[q] // 128

    def lines(q):
        return TRIPLE if cut(q) else TRIPLE[1:]

    def piece(p, q, base, kind, d, h, mid, to):
        start, count = (0, cut(q)) if kind == 0 else (cut(q), mb - cut(q))
        if h == hops:
            count //= 2
            start += count if d < 0 else 0
        at = vbuf.at[p, q // SPLIT, span(base + (q % SPLIT) * mb + start, count), :]
        return remote(at, at, ag_s.at[q, mid], ag_r.at[p, q, mid], to)

    def z_copy(p, q, d, line, h, gone):
        base = (others if line == 2 else starts)[-d * (h - 1 if gone else h)]
        mid = ((0 if d > 0 else 3) + line) * hops + h - 1
        return piece(p, q, base, min(line, 1), d, h, mid, z_next[d])

    def pair_copy(p, q, kind, d, h, gone):
        mid = 6 * hops + (2 * h + max(d, 0) if h else 0 if kind else 1)
        return piece(p, q, (starts if gone else others)[-d * h], kind, d, h, mid, yh_partner)

    def own_sends(p, q):
        pair_copy(p, q, 1, 0, 0, GONE).start()
        for line in lines(q)[:-1]:
            for d in WAYS:
                z_copy(p, q, d, line, 1, GONE).start()
        if cut(q):
            pair_copy(p, q, 0, 0, 0, GONE).start()

    def take_pair(p, q):
        pair_copy(p, q, 1, 0, 0, HERE).wait_recv()
        for d in WAYS:
            z_copy(p, q, d, 2, 1, GONE).start()

    def take_hop(p, q, line, h):
        for d in WAYS:
            z_copy(p, q, d, line, h, HERE).wait_recv()
            if h < hops:
                z_copy(p, q, d, line, h + 1, GONE).start()
            if line == 0:
                pair_copy(p, q, 0, d, h, GONE).start()

    def drain_gather(p):
        for q in chunks:
            first = range(0 if cut(q) else 1, 2)
            for kind in first:
                pair_copy(p, q, kind, 0, 0, GONE).wait_send()
            for d in WAYS:
                for h in range(1, hops + 1):
                    for line in lines(q):
                        z_copy(p, q, d, line, h, GONE).wait_send()
                    for _ in first[1:]:
                        pair_copy(p, q, 0, d, h, GONE).wait_send()

    plane = nx * 8

    line = [mod(row * 4 + y + d, plane) for d in range(plane)]
    groups = (
        (0, plane, row * 4 + y, [{"col": z * 4 + mod(at, 4), "row": div(at, 4)} for at in line]),
        (plane, nz, z, [dev(zz=zs[d]) for d in range(nz)]),
    )

    def sum_send(which, stage, tile):
        base, count, me, peers = groups[stage]
        red[which, base + me] = tile
        at = red.at[which, base + me]
        for d in range(1, count):
            remote(at, at, ar_s.at[which, stage], ar_r.at[which, stage], peers[d]).start()

    def sum_take(which, stage):
        base, count, _, _ = groups[stage]
        at = red.at[which, pl.ds(base, count - 1)]
        pltpu.make_async_copy(at, at, ar_r.at[which, stage]).wait()
        pltpu.make_async_copy(at, at, ar_s.at[which, stage]).wait()
        total = red[which, base]
        for i in range(1, count):
            total = total + red[which, base + i]
        return total

    def sum_pass(which, stage):
        sum_send(which, stage, sum_take(which, stage - 1))

    lanes = red.shape[-1]

    def narrow(tile):
        out = tile[:, :lanes]
        for i in range(1, wa // lanes):
            out = out + tile[:, i * lanes : (i + 1) * lanes]
        return out

    def own_block(i):
        return span(own + i * ROWS, ROWS)

    def accumulate(term):
        def trip(i, acc):
            for s in PAIR:
                acc = acc + term(s, i)
            return acc

        return lax.fori_loop(0, wb // ROWS, trip, jnp.zeros((ROWS, wa), jnp.float32), unroll=4)

    def alpha_open(p):
        acc = accumulate(lambda s, i: vv[p, s, block(i), :] * vbuf[p, s, own_block(i), :])
        sum_send(0, 0, narrow(acc))

    def alpha_close(slot):
        value = jnp.full((ROWS, wa), jnp.sum(sum_take(0, 1)), jnp.float32)
        sc[0] = value
        scal_ref[slot] = value[:, :lanes]

    def beta_open(p):
        alpha, beta = sc[0], sc[2]

        def term(s, i):
            u = vbuf[p, s, own_block(i), :] - alpha * vv[p, s, block(i), :] - beta * vv[1 - p, s, block(i), :]
            vv[1 - p, s, block(i), :] = u
            return u * u

        sum_send(1, 0, narrow(accumulate(term)))

    def beta_close(slot):
        value = jnp.sqrt(jnp.full((ROWS, wa), jnp.sum(sum_take(1, 1)), jnp.float32))
        sc[1] = value
        scal_ref[LANCZOS_STEPS + slot] = value[:, :lanes]

    def scale(p):
        def trip(i):
            for s in PAIR:
                vv[1 - p, s, block(i), :] = vv[1 - p, s, block(i), :] / sc[1]

        fold(trip, wb // ROWS)

    def r_rows(e, of_sub, xx, cc):
        start = (e // PIECES) * wb + of_sub * half + (xx * 2 + cc) * part + (e % PIECES) * bit
        return rbuf.at[span(start, bit), :]

    def r_copy(way, e, gone):
        if way == 0:
            src = r_hbm.at[e // PIECES, span(row * part + (e % PIECES) * bit, bit), :]
            return remote(src, r_rows(e, sub if gone else 1 - sub, x, c), rr_s.at[0, e], rr_r.at[0, e], yl_partner)
        over = isinstance(way, tuple)
        from_way = way[0] if over else way
        slot = from_way % 4
        d = from_way if from_way in WAYS else 1 if e % PIECES == 0 else -1
        away = {0: 0, 2: 2}.get(from_way, -d) - (d if gone and not over else 0)
        away = -d if gone and not over and from_way == 2 else 0 if gone and not over else away
        at = r_rows(e, 1 - sub, xs[away], 1 - c if over and not gone else c)
        slot = slot + 4 if over else slot
        return remote(at, at, rr_s.at[slot, e], rr_r.at[slot, e], sibling if over else x_next[d])

    def r_take(way, e):
        for d in WAYS if way == 1 else (way,):
            r_copy(d, e, HERE).wait_recv()
            r_copy((d,), e, GONE).start()
            if way == 0:
                for n in WAYS:
                    r_copy(n, e, GONE).start()
            elif way == 1 and d == (1 if e % PIECES == 0 else -1):
                r_copy(2, e, GONE).start()

    def r_last():
        for e in range(3 * PIECES):
            for way in (0, 1, -1, 2):
                r_copy((way,), e, HERE).wait_recv()
                r_copy((way,), e, GONE).wait_send()
                r_copy(way, e, GONE).wait_send()

    def right_group(p, s, h, way):
        d = 1 if way == "+" else -1
        for q in range(s * SPLIT, s * SPLIT + SPLIT):
            for e in (d,) if way != "*" else WAYS if h else (0,):
                if cut(q):
                    pair_copy(p, q, 0, e, h, HERE).wait_recv()

        def one(i, carry):
            start = pl.multiple_of((zs[-d * h] * 2 + i) * wb, wb)
            ubuf[s] = ubuf[s] + jnp.dot(
                rbuf[:, pl.ds(start, wb)],
                vbuf[p, s, pl.ds(start, wb), :],
                precision=EXACT_PREC,
                preferred_element_type=jnp.float32,
            )
            return carry

        lax.fori_loop(0, 2, one, 0)

    def clear_products():
        def trip(i):
            for s in PAIR:
                ubuf[s, block(i), :] = jnp.zeros((ROWS, wa), jnp.float32)

        fold(trip, 3 * wb // ROWS)

    def mix(q):
        t, base = q // SPLIT, (q % SPLIT) * mb

        def trip(i):
            tiles = [[ubuf[s, span(r * wb + base + i * ROWS, ROWS), :] for s in PAIR] for r in TRIPLE]
            for l in TRIPLE:
                acc = None
                for r in TRIPLE:
                    for s in PAIR:
                        term = w_ref[l, s, t, r] * tiles[r][s]
                        acc = term if acc is None else acc + term
                tbuf[t, span(base + i * ROWS, ROWS), l * wa : (l + 1) * wa] = acc

        fold(trip, mb // ROWS, 1)
        if q == chunks[-1]:
            clear_products()

    def sib_copy(q, i):
        return remote(yb.at[i], rd.at[q, i], rd_s.at[i], rd_r.at[q, i], sibling)

    def left_products(q, part):
        def one(n, carry):
            theirs = (n < 2, n > 0, n < 0)[part]
            i = n + 1 if part == 2 else jnp.where(n == 1 - part, 3, n * part)
            away = jnp.where(i < 2, i + 2, 3 - i)
            start = (mod(x + away, nx) * 2 + jnp.where(theirs, 1 - c, c)) * 2 * wa
            yb[jnp.where(theirs, i, i + 4)] = jnp.dot(
                tbuf[q // SPLIT, (q % SPLIT) * mb : (q % SPLIT + 1) * mb, :],
                lbuf[:, pl.ds(pl.multiple_of(start, 2 * wa), 2 * wa)],
                precision=EXACT_PREC,
                preferred_element_type=jnp.float32,
            )

            @pl.when(theirs)
            def _():
                sib_copy(q, i).start()

            return carry

        for i in ((0, 3), (1, 2), ())[part] if q else ():
            sib_copy(q - 1, i).wait_send()
        lax.fori_loop(0, (3, 3, 2)[part], one, 0)

    lane_at = {GONE: (1 - yl) * wa, HERE: yl * wa}

    def lane(theirs):
        return pl.ds(pl.multiple_of(lane_at[theirs], wa), wa)

    def half_copy(p, q, d, theirs):
        slot, side = 0 if d > 0 else 1, 0 if theirs else 1
        src = rd.at[q, 0, pl.ds(slot * mb // 2, mb // 2), lane(theirs)]
        return remote(src, hx.at[p, q, slot, side], hx_s.at[q, slot, side], hx_r.at[p, q, slot, side], x_next[d])

    def full_copy(p, q, d, theirs):
        slot, side = 0 if d > 0 else 1, 0 if theirs else 1
        src = rd.at[q, 2 - slot, :, lane(theirs)]
        to = (x_side if theirs else x_next)[d]
        return remote(src, fx.at[p, q, slot, side], fx_s.at[q, slot, side], fx_r.at[p, q, slot, side], to)

    def cross_copy(p, q):
        return remote(rd.at[q, 3, :, lane(GONE)], yx.at[p, q], yx_s.at[q], yx_r.at[p, q], yl_partner)

    def left_sum(p, q, i, side):
        if side == 0:
            sib_copy(q, i).wait_recv()

            def add(k):
                rows = block(k)
                rd[q, i, rows, :] = rd[q, i, rows, :] + yb[i + 4, rows, :]

            fold(add, mb // ROWS)
        if i == 0:
            for theirs in (GONE, HERE):
                for d in WAYS:
                    half_copy(p, q, d, theirs).start()
        elif i < 3:
            d, theirs = 2 * i - 3, side == 0
            lanes_at = lane(theirs)
            half_copy(p, q, d, theirs).wait_recv()

            def add_half(k):
                rows = span(k * ROWS + (0 if d > 0 else mb // 2), ROWS)
                rd[q, i, rows, lanes_at] = rd[q, i, rows, lanes_at] + hx[p, q, i % 2, side, block(k), :]

            fold(add_half, mb // 2 // ROWS)
            full_copy(p, q, d, theirs).start()
        else:
            cross_copy(p, q).start()

    def close_chunk(p, q, more):
        for theirs in (GONE, HERE):
            for d in WAYS:
                full_copy(p, q, d, theirs).wait_recv()
        cross_copy(p, q).wait_recv()
        alpha, beta, old = sc[0], sc[1], sc[2]
        s, mine = q // SPLIT, lane(HERE)

        def step(k):
            rows, at = block(k), own_block(k + (q % SPLIT) * mb // ROWS)
            g = rd[q, 3, rows, mine] + yx[p, q, rows, :]
            for slot in PAIR:
                g = g + (fx[p, q, slot, 0, rows, :] + fx[p, q, slot, 1, rows, :])
            vbuf[1 - p, s, at, :] = (g - alpha * vbuf[p, s, at, :] - old * vbuf[1 - p, s, at, :]) / beta

        fold(step, mb // ROWS)

        @pl.when(more)
        def _():
            own_sends(1 - p, q)

    def drain_sums(p, q):
        for theirs in (GONE, HERE):
            for d in WAYS:
                half_copy(p, q, d, theirs).wait_send()
                full_copy(p, q, d, theirs).wait_send()
        cross_copy(p, q).wait_send()

    def l_load(l):
        return pltpu.make_async_copy(l_hbm.at[l, span(yl * wa, wa), :], lbuf.at[pl.ds(l * wa, wa), :], ld_s.at[l])

    def r_load(r):
        return pltpu.make_async_copy(r_hbm.at[r], rbuf.at[span(r * wb + sub * half, half), :], ld_s.at[3 + r])

    def psi_at(s, of_sub):
        return vbuf.at[0, s, span(own + of_sub * half, half), :]

    def psi_load(s):
        return pltpu.make_async_copy(psi_ref.at[yl, s], psi_at(s, sub), ld_s.at[6 + s])

    def psi_copy(s, gone):
        return remote(psi_ref.at[1 - yl, s], psi_at(s, sub if gone else 1 - sub), io_s.at[s], io_r.at[s], yl_partner)

    for s in PAIR:
        psi_load(s).start()
    barrier = pltpu.get_barrier_semaphore()
    for _, count, _, peers in groups:
        for d in range(1, count):
            pl.semaphore_signal(barrier, inc=1, device_id=peers[d], device_id_type=MESH)
    pl.semaphore_wait(barrier, plane + nz - 2)
    for s in PAIR:
        psi_copy(s, GONE).start()
    for e in range(3 * PIECES):
        r_copy(0, e, GONE).start()
    for r in TRIPLE:
        r_load(r).start()
    for l in TRIPLE:
        l_load(l).start()
    pl.semaphore_signal(credit, inc=1, device_id=sibling, device_id_type=MESH)

    def clear(i):
        for s in PAIR:
            vbuf[1, s, own_block(i), :] = jnp.zeros((ROWS, wa), jnp.float32)
            for p in PAIR:
                vv[p, s, block(i), :] = jnp.zeros((ROWS, wa), jnp.float32)

    fold(clear, wb // ROWS)
    clear_products()
    sc[2] = jnp.zeros((ROWS, wa), jnp.float32)
    def work(name, p, more, slot):
        kind, tail = name[0], name[1:]
        if kind == "m":
            return functools.partial(right_group, p, int(tail[0]), int(tail[1]), tail[2])
        args = [int(digit) for digit in tail]
        if kind in "ab":
            calls = {
                "a0": lambda: alpha_open(p),
                "b0": lambda: (alpha_close(slot), beta_open(p)),
                "b3": lambda: (beta_close(slot), scale(p)),
            }
            return calls.get(name, functools.partial(sum_pass, "ab".index(kind), args[0]))
        if kind == "c":
            return functools.partial(close_chunk, p, *args, more)
        if kind == "d":
            return functools.partial(drain_gather, p)
        if kind == "w":
            return r_last
        if kind == "r":
            return functools.partial(r_take, *args)
        if kind in "lx":
            return functools.partial({"l": left_products, "x": mix}[kind], *args)
        return functools.partial({"p": take_pair, "h": take_hop, "f": left_sum}[kind], p, *args)

    start_order, gather_order, reduce_order = (
        ",".join(order).split(",") for order in (START_ORDER, GATHER_ORDER, REDUCE_ORDER)
    )
    for s in PAIR:
        psi_load(s).wait()
        psi_copy(s, HERE).wait_recv()
        own_sends(0, s * SPLIT)
    for name in start_order:
        if name[0] == "c":
            own_sends(0, int(name[1]))
        else:
            work(name, 0, None, None)()
    for r in TRIPLE:
        r_load(r).wait()
        l_load(r).wait()
    for s in PAIR:
        psi_copy(s, GONE).wait_send()

    def lanczos_step(j, carry):
        p = mod(j, 2)
        slot = mod(j + LANCZOS_STEPS - 1, LANCZOS_STEPS)
        more = j < LANCZOS_STEPS - 1

        for name in gather_order:
            if name[0] in "rw":
                pl.when(j == 0)(work(name, p, more, slot))
            else:
                work(name, p, more, slot)()
        mix(0)

        pl.semaphore_wait(credit, 1)
        for name in reduce_order:
            if name[0] in "ph":
                pl.when(more)(work(name, 1 - p, more, slot))
            else:
                work(name, p, more, slot)()
        for i in range(4):
            sib_copy(chunks[-1], i).wait_send()
        for q in chunks:
            drain_sums(p, q)

        @pl.when(more)
        def _():
            pl.semaphore_signal(credit, inc=1, device_id=sibling, device_id_type=MESH)

        sc[2] = jnp.where(j > 0, sc[1], jnp.zeros((ROWS, wa), jnp.float32))
        return carry

    lax.fori_loop(0, LANCZOS_STEPS, lanczos_step, 0)

    p = LANCZOS_STEPS % 2

    def out_copy(s):
        src = vv.at[1 - p, s, span((1 - sub) * half, half), :]
        return remote(src, ob.at[s], io_s.at[2 + s], io_r.at[2 + s], yl_partner)

    alpha_open(p)
    sum_pass(0, 1)
    alpha_close(LANCZOS_STEPS - 1)
    beta_open(p)
    for s in PAIR:
        out_copy(s).start()
    sum_pass(1, 1)
    beta_close(LANCZOS_STEPS - 1)
    for s in PAIR:
        out_copy(s).wait_recv()

        def put(i):
            vout_ref[yl, s, block(i), :] = vv[1 - p, s, span(sub * half + i * ROWS, ROWS), :] / sc[1]
            vout_ref[1 - yl, s, block(i), :] = ob[s, block(i), :] / sc[1]

        fold(put, half // ROWS)
        out_copy(s).wait_send()


def solution(mesh):
    nz, nx = mesh.shape["col"] // 4, mesh.shape["row"] // 2

    def local_steps(psi_blk, left_blk, mpo_tensor, right_blk):
        wa, wb = psi_blk.shape[0] // 2, psi_blk.shape[2] * 2
        da, db = left_blk.shape[2], right_blk.shape[2]
        half = wb // 2
        hops = nz // 2
        mb = wb // SPLIT
        parts = 2 * SPLIT
        lanes = 128 if wa % 128 == 0 else wa
        f32 = jnp.float32
        psi_t = jnp.transpose(psi_blk.reshape(2, wa, 2, half), (0, 2, 3, 1))
        kernel = functools.partial(lanczos_kernel, nz, nx, wa, wb)
        vmem, dma = pltpu.VMEM, pltpu.SemaphoreType.DMA
        ids = 8 * hops + 2
        scalars, v_out = pl.pallas_call(
            kernel,
            out_shape=(
                jax.ShapeDtypeStruct((2 * LANCZOS_STEPS, ROWS, lanes), f32),
                jax.ShapeDtypeStruct((2, 2, half, wa), f32),
            ),
            in_specs=[
                pl.BlockSpec(memory_space=pl.ANY),
                pl.BlockSpec(memory_space=pl.ANY),
                pl.BlockSpec(memory_space=pltpu.SMEM),
                pl.BlockSpec(memory_space=pl.ANY),
            ],
            out_specs=(pl.BlockSpec(memory_space=pltpu.VMEM),) * 2,
            scratch_shapes=[
                vmem((2, 2, db, wa), f32),
                vmem((3 * wa, da), f32),
                vmem((3 * wb, db), f32),
                vmem((2, 3 * wb, wa), f32),
                vmem((2, wb, 3 * wa), f32),
                vmem((2, 2, wb, wa), f32),
                vmem((parts, 4, mb, 2 * wa), f32),
                vmem((8, mb, 2 * wa), f32),
                vmem((2, parts, 2, 2, mb // 2, wa), f32),
                vmem((2, parts, 2, 2, mb, wa), f32),
                vmem((2, parts, mb, wa), f32),
                vmem((2, half, wa), f32),
                vmem((2, nx * 8 + nz, ROWS, lanes), f32),
                vmem((3, ROWS, wa), f32),
                dma((parts, ids)),
                dma((2, parts, ids)),
                dma((4,)),
                dma((parts, 4)),
                dma((parts, 2, 2)),
                dma((2, parts, 2, 2)),
                dma((parts, 2, 2)),
                dma((2, parts, 2, 2)),
                dma((parts,)),
                dma((2, parts)),
                dma((2, 2)),
                dma((2, 2)),
                dma((8, 3 * PIECES)),
                dma((8, 3 * PIECES)),
                dma((4,)),
                dma((4,)),
                dma((8,)),
                pltpu.SemaphoreType.REGULAR,
            ],
            compiler_params=pltpu.CompilerParams(collective_id=0, has_side_effects=True, vmem_limit_bytes=66 * 1000 * 1000),
            name="lanczos",
        )(psi_t, jnp.transpose(left_blk, (1, 0, 2)), jnp.transpose(mpo_tensor, (0, 2, 3, 1)), jnp.transpose(right_blk, (1, 0, 2)))
        v_next = jnp.transpose(v_out, (0, 3, 1, 2)).reshape(psi_blk.shape)
        return scalars[:LANCZOS_STEPS, 0, 0], scalars[LANCZOS_STEPS:, 0, 0], v_next

    return jax.shard_map(
        local_steps,
        mesh=mesh,
        in_specs=(P("row", None, "col"), P("row", None, None), P(), P("col", None, None)),
        out_specs=(P(), P(), P("row", None, "col")),
        check_vma=False,
    )
```

```python
import functools

import jax
import jax.numpy as jnp
from jax import lax
from jax.experimental import pallas as pl
from jax.experimental.pallas import tpu as pltpu
from jax.sharding import PartitionSpec as P

LANCZOS_STEPS = 4
EXACT_PREC = lax.Precision.HIGHEST
MESH = pl.DeviceIdType.MESH
ROWS = 8
SPLIT = 2
PIECES = 2
START_ORDER = (
    "p0,c1,r00,r01,h001,r02,h011,h111,h101,p1,r03,r11,h012,h201",
    "r10,r05,r04,c3,h021,h121,h102,h002,r15,r12,p2,h112,h022,h211",
    "r13,r21,r14,h003,r22,h301,r20,h122,h023,r24,h013,h113,h103",
)
GATHER_ORDER = (
    "a0,r23,p3,h311,r25,w,m01+,m02-,m02+,h221,h302,h202,h123,h024",
    "m01-,h104,m10*,h004,h114,h321,m00*,h212,m03-,a1,h222,m11+",
    "h303,h312,m11-,h322,m03+,h203,h213,m12-,b0,h014,h124,h223",
    "m04*,h304,h313,m12+,h323,h204,m13+,m13-,h214,h324,b1,h224",
    "h314,m14*",
)
REDUCE_ORDER = (
    "x1,l00,f000,l01,f030,l02,f010,f020,l10,f100,l11,f011,f021",
    "l12,f130,x2,f120,f110,l20,d0,b3,c0,f200,f121,f111,l21,f230",
    "l22,f220,f210,p0,x3,h001,h011,l30,c1,f300,l31,f330,h021,f221",
    "f211,h002,p1,h101,l32,h111,f320,f310,h012,f311,h022,f321,c2",
    "h112,h102,h003,h121,c3,h201,h122,h013,h103,h113,h023,h301",
    "h211,p2",
)
PAIR = range(2)
TRIPLE = range(3)
WAYS = (1, -1)
GONE, HERE = True, False


def fold(body, count, unroll=4):
    while count % unroll:
        unroll //= 2

    def trip(i, carry):
        for u in range(unroll):
            body(i * unroll + u)
        return carry

    lax.fori_loop(0, count // unroll, trip, 0)


def lanczos_kernel(
    nz, nx, wa, wb,
    psi_ref, l_hbm, w_ref, r_hbm,
    scal_ref, vout_ref,
    vbuf, lbuf, rbuf, ubuf, tbuf, vv, rd, yb, hx, fx, yx, ob, red, sc,
    ag_s, ag_r, rd_s, rd_r, hx_s, hx_r, fx_s, fx_r, yx_s, yx_r,
    ar_s, ar_r, rr_s, rr_r, io_s, io_r, ld_s, credit,
):
    hops = nz // 2
    half, mb = wb // 2, wb // SPLIT
    part = half // (2 * nx)
    bit = part // PIECES
    chunks = range(2 * SPLIT)
    col, row = lax.axis_index("col"), lax.axis_index("row")
    div, mod = lax.div, lax.rem
    z, y, x, c = div(col, 4), mod(col, 4), div(row, 2), mod(row, 2)
    yh, sub = div(y, 2), mod(y, 2)
    yl = mod(div(y + 1, 2), 2)

    def dev(zz=None, yy=None, xx=None, cc=None):
        zz = z if zz is None else zz
        yy = y if yy is None else yy
        xx = x if xx is None else xx
        cc = c if cc is None else cc
        return {"col": zz * 4 + yy, "row": xx * 2 + cc}

    zs = {off: mod(z + off + nz, nz) for off in range(-hops, nz)}
    xs = {off: mod(x + off + nx, nx) for off in range(-1, nx)}
    starts = {off: (at * 2 + yh) * wb for off, at in zs.items()}
    others = {off: (at * 2 + 1 - yh) * wb for off, at in zs.items()}
    own = starts[0]

    sibling = dev(cc=1 - c)
    yl_partner = dev(yy=y + 1 - 2 * sub)
    yh_partner = dev(yy=3 - y)
    z_next = {d: dev(zz=zs[d]) for d in WAYS}
    x_next = {d: dev(xx=xs[d]) for d in WAYS}
    x_side = {d: dev(yy=y + 1 - 2 * sub, xx=xs[d]) for d in WAYS}

    def remote(src, dst, send, recv, to):
        return pltpu.make_async_remote_copy(
            src_ref=src, dst_ref=dst, send_sem=send, recv_sem=recv, device_id=to, device_id_type=MESH
        )

    def span(start, count):
        return pl.ds(pl.multiple_of(start, ROWS), count)

    def block(i):
        return span(i * ROWS, ROWS)

    def cut(q):
        return mb * (96, 96, 64, 32)[q] // 128

    def lines(q):
        return TRIPLE if cut(q) else TRIPLE[1:]

    def piece(p, q, base, kind, d, h, mid, to):
        start, count = (0, cut(q)) if kind == 0 else (cut(q), mb - cut(q))
        if h == hops:
            count //= 2
            start += count if d < 0 else 0
        at = vbuf.at[p, q // SPLIT, span(base + (q % SPLIT) * mb + start, count), :]
        return remote(at, at, ag_s.at[q, mid], ag_r.at[p, q, mid], to)

    def z_copy(p, q, d, line, h, gone):
        base = (others if line == 2 else starts)[-d * (h - 1 if gone else h)]
        mid = ((0 if d > 0 else 3) + line) * hops + h - 1
        return piece(p, q, base, min(line, 1), d, h, mid, z_next[d])

    def pair_copy(p, q, kind, d, h, gone):
        mid = 6 * hops + (2 * h + max(d, 0) if h else 0 if kind else 1)
        return piece(p, q, (starts if gone else others)[-d * h], kind, d, h, mid, yh_partner)

    def own_sends(p, q):
        pair_copy(p, q, 1, 0, 0, GONE).start()
        for line in lines(q)[:-1]:
            for d in WAYS:
                z_copy(p, q, d, line, 1, GONE).start()
        if cut(q):
            pair_copy(p, q, 0, 0, 0, GONE).start()

    def take_pair(p, q):
        pair_copy(p, q, 1, 0, 0, HERE).wait_recv()
        for d in WAYS:
            z_copy(p, q, d, 2, 1, GONE).start()

    def take_hop(p, q, line, h):
        for d in WAYS:
            z_copy(p, q, d, line, h, HERE).wait_recv()
            if h < hops:
                z_copy(p, q, d, line, h + 1, GONE).start()
            if line == 0:
                pair_copy(p, q, 0, d, h, GONE).start()

    def drain_gather(p):
        for q in chunks:
            first = range(0 if cut(q) else 1, 2)
            for kind in first:
                pair_copy(p, q, kind, 0, 0, GONE).wait_send()
            for d in WAYS:
                for h in range(1, hops + 1):
                    for line in lines(q):
                        z_copy(p, q, d, line, h, GONE).wait_send()
                    for _ in first[1:]:
                        pair_copy(p, q, 0, d, h, GONE).wait_send()

    plane = nx * 8

    line = [mod(row * 4 + y + d, plane) for d in range(plane)]
    groups = (
        (0, plane, row * 4 + y, [{"col": z * 4 + mod(at, 4), "row": div(at, 4)} for at in line]),
        (plane, nz, z, [dev(zz=zs[d]) for d in range(nz)]),
    )

    def sum_send(which, stage, tile):
        base, count, me, peers = groups[stage]
        red[which, base + me] = tile
        at = red.at[which, base + me]
        for d in range(1, count):
            remote(at, at, ar_s.at[which, stage], ar_r.at[which, stage], peers[d]).start()

    def sum_take(which, stage):
        base, count, _, _ = groups[stage]
        at = red.at[which, pl.ds(base, count - 1)]
        pltpu.make_async_copy(at, at, ar_r.at[which, stage]).wait()
        pltpu.make_async_copy(at, at, ar_s.at[which, stage]).wait()
        total = red[which, base]
        for i in range(1, count):
            total = total + red[which, base + i]
        return total

    def sum_pass(which, stage):
        sum_send(which, stage, sum_take(which, stage - 1))

    lanes = red.shape[-1]

    def narrow(tile):
        out = tile[:, :lanes]
        for i in range(1, wa // lanes):
            out = out + tile[:, i * lanes : (i + 1) * lanes]
        return out

    def own_block(i):
        return span(own + i * ROWS, ROWS)

    def accumulate(term):
        def trip(i, acc):
            for s in PAIR:
                acc = acc + term(s, i)
            return acc

        return lax.fori_loop(0, wb // ROWS, trip, jnp.zeros((ROWS, wa), jnp.float32), unroll=4)

    def alpha_open(p):
        acc = accumulate(lambda s, i: vv[p, s, block(i), :] * vbuf[p, s, own_block(i), :])
        sum_send(0, 0, narrow(acc))

    def alpha_close(slot):
        value = jnp.full((ROWS, wa), jnp.sum(sum_take(0, 1)), jnp.float32)
        sc[0] = value
        scal_ref[slot] = value[:, :lanes]

    def beta_open(p):
        alpha, beta = sc[0], sc[2]

        def term(s, i):
            u = vbuf[p, s, own_block(i), :] - alpha * vv[p, s, block(i), :] - beta * vv[1 - p, s, block(i), :]
            vv[1 - p, s, block(i), :] = u
            return u * u

        sum_send(1, 0, narrow(accumulate(term)))

    def beta_close(slot):
        value = jnp.sqrt(jnp.full((ROWS, wa), jnp.sum(sum_take(1, 1)), jnp.float32))
        sc[1] = value
        scal_ref[LANCZOS_STEPS + slot] = value[:, :lanes]

    def scale(p):
        def trip(i):
            for s in PAIR:
                vv[1 - p, s, block(i), :] = vv[1 - p, s, block(i), :] / sc[1]

        fold(trip, wb // ROWS)

    def r_rows(e, of_sub, xx, cc):
        start = (e // PIECES) * wb + of_sub * half + (xx * 2 + cc) * part + (e % PIECES) * bit
        return rbuf.at[span(start, bit), :]

    def r_copy(way, e, gone):
        if way == 0:
            src = r_hbm.at[e // PIECES, span(row * part + (e % PIECES) * bit, bit), :]
            return remote(src, r_rows(e, sub if gone else 1 - sub, x, c), rr_s.at[0, e], rr_r.at[0, e], yl_partner)
        over = isinstance(way, tuple)
        from_way = way[0] if over else way
        slot = from_way % 4
        d = from_way if from_way in WAYS else 1 if e % PIECES == 0 else -1
        away = {0: 0, 2: 2}.get(from_way, -d) - (d if gone and not over else 0)
        away = -d if gone and not over and from_way == 2 else 0 if gone and not over else away
        at = r_rows(e, 1 - sub, xs[away], 1 - c if over and not gone else c)
        slot = slot + 4 if over else slot
        return remote(at, at, rr_s.at[slot, e], rr_r.at[slot, e], sibling if over else x_next[d])

    def r_take(way, e):
        for d in WAYS if way == 1 else (way,):
            r_copy(d, e, HERE).wait_recv()
            r_copy((d,), e, GONE).start()
            if way == 0:
                for n in WAYS:
                    r_copy(n, e, GONE).start()
            elif way == 1 and d == (1 if e % PIECES == 0 else -1):
                r_copy(2, e, GONE).start()

    def r_last():
        for e in range(3 * PIECES):
            for way in (0, 1, -1, 2):
                r_copy((way,), e, HERE).wait_recv()
                r_copy((way,), e, GONE).wait_send()
                r_copy(way, e, GONE).wait_send()

    def right_group(p, s, h, way):
        d = 1 if way == "+" else -1
        for q in range(s * SPLIT, s * SPLIT + SPLIT):
            for e in (d,) if way != "*" else WAYS if h else (0,):
                if cut(q):
                    pair_copy(p, q, 0, e, h, HERE).wait_recv()

        def one(i, carry):
            start = pl.multiple_of((zs[-d * h] * 2 + i) * wb, wb)
            ubuf[s] = ubuf[s] + jnp.dot(
                rbuf[:, pl.ds(start, wb)],
                vbuf[p, s, pl.ds(start, wb), :],
                precision=EXACT_PREC,
                preferred_element_type=jnp.float32,
            )
            return carry

        lax.fori_loop(0, 2, one, 0)

    def clear_products():
        def trip(i):
            for s in PAIR:
                ubuf[s, block(i), :] = jnp.zeros((ROWS, wa), jnp.float32)

        fold(trip, 3 * wb // ROWS)

    def mix(q):
        t, base = q // SPLIT, (q % SPLIT) * mb

        def trip(i):
            tiles = [[ubuf[s, span(r * wb + base + i * ROWS, ROWS), :] for s in PAIR] for r in TRIPLE]
            for l in TRIPLE:
                acc = None
                for r in TRIPLE:
                    for s in PAIR:
                        term = w_ref[l, s, t, r] * tiles[r][s]
                        acc = term if acc is None else acc + term
                tbuf[t, span(base + i * ROWS, ROWS), l * wa : (l + 1) * wa] = acc

        fold(trip, mb // ROWS, 1)
        if q == chunks[-1]:
            clear_products()

    def sib_copy(q, i):
        return remote(yb.at[i], rd.at[q, i], rd_s.at[i], rd_r.at[q, i], sibling)

    def left_products(q, part):
        def one(n, carry):
            theirs = (n < 2, n > 0, n < 0)[part]
            i = n + 1 if part == 2 else jnp.where(n == 1 - part, 3, n * part)
            away = jnp.where(i < 2, i + 2, 3 - i)
            start = (mod(x + away, nx) * 2 + jnp.where(theirs, 1 - c, c)) * 2 * wa
            yb[jnp.where(theirs, i, i + 4)] = jnp.dot(
                tbuf[q // SPLIT, (q % SPLIT) * mb : (q % SPLIT + 1) * mb, :],
                lbuf[:, pl.ds(pl.multiple_of(start, 2 * wa), 2 * wa)],
                precision=EXACT_PREC,
                preferred_element_type=jnp.float32,
            )

            @pl.when(theirs)
            def _():
                sib_copy(q, i).start()

            return carry

        for i in ((0, 3), (1, 2), ())[part] if q else ():
            sib_copy(q - 1, i).wait_send()
        lax.fori_loop(0, (3, 3, 2)[part], one, 0)

    lane_at = {GONE: (1 - yl) * wa, HERE: yl * wa}

    def lane(theirs):
        return pl.ds(pl.multiple_of(lane_at[theirs], wa), wa)

    def half_copy(p, q, d, theirs):
        slot, side = 0 if d > 0 else 1, 0 if theirs else 1
        src = rd.at[q, 0, pl.ds(slot * mb // 2, mb // 2), lane(theirs)]
        return remote(src, hx.at[p, q, slot, side], hx_s.at[q, slot, side], hx_r.at[p, q, slot, side], x_next[d])

    def full_copy(p, q, d, theirs):
        slot, side = 0 if d > 0 else 1, 0 if theirs else 1
        src = rd.at[q, 2 - slot, :, lane(theirs)]
        to = (x_side if theirs else x_next)[d]
        return remote(src, fx.at[p, q, slot, side], fx_s.at[q, slot, side], fx_r.at[p, q, slot, side], to)

    def cross_copy(p, q):
        return remote(rd.at[q, 3, :, lane(GONE)], yx.at[p, q], yx_s.at[q], yx_r.at[p, q], yl_partner)

    def left_sum(p, q, i, side):
        if side == 0:
            sib_copy(q, i).wait_recv()

            def add(k):
                rows = block(k)
                rd[q, i, rows, :] = rd[q, i, rows, :] + yb[i + 4, rows, :]

            fold(add, mb // ROWS)
        if i == 0:
            for theirs in (GONE, HERE):
                for d in WAYS:
                    half_copy(p, q, d, theirs).start()
        elif i < 3:
            d, theirs = 2 * i - 3, side == 0
            lanes_at = lane(theirs)
            half_copy(p, q, d, theirs).wait_recv()

            def add_half(k):
                rows = span(k * ROWS + (0 if d > 0 else mb // 2), ROWS)
                rd[q, i, rows, lanes_at] = rd[q, i, rows, lanes_at] + hx[p, q, i % 2, side, block(k), :]

            fold(add_half, mb // 2 // ROWS)
            full_copy(p, q, d, theirs).start()
        else:
            cross_copy(p, q).start()

    def close_chunk(p, q, more):
        for theirs in (GONE, HERE):
            for d in WAYS:
                full_copy(p, q, d, theirs).wait_recv()
        cross_copy(p, q).wait_recv()
        alpha, beta, old = sc[0], sc[1], sc[2]
        s, mine = q // SPLIT, lane(HERE)

        def step(k):
            rows, at = block(k), own_block(k + (q % SPLIT) * mb // ROWS)
            g = rd[q, 3, rows, mine] + yx[p, q, rows, :]
            for slot in PAIR:
                g = g + (fx[p, q, slot, 0, rows, :] + fx[p, q, slot, 1, rows, :])
            vbuf[1 - p, s, at, :] = (g - alpha * vbuf[p, s, at, :] - old * vbuf[1 - p, s, at, :]) / beta

        fold(step, mb // ROWS)

        @pl.when(more)
        def _():
            own_sends(1 - p, q)

    def drain_sums(p, q):
        for theirs in (GONE, HERE):
            for d in WAYS:
                half_copy(p, q, d, theirs).wait_send()
                full_copy(p, q, d, theirs).wait_send()
        cross_copy(p, q).wait_send()

    def l_load(l):
        return pltpu.make_async_copy(l_hbm.at[l, span(yl * wa, wa), :], lbuf.at[pl.ds(l * wa, wa), :], ld_s.at[l])

    def r_load(r):
        return pltpu.make_async_copy(r_hbm.at[r], rbuf.at[span(r * wb + sub * half, half), :], ld_s.at[3 + r])

    def psi_at(s, of_sub):
        return vbuf.at[0, s, span(own + of_sub * half, half), :]

    def psi_load(s):
        return pltpu.make_async_copy(psi_ref.at[yl, s], psi_at(s, sub), ld_s.at[6 + s])

    def psi_copy(s, gone):
        return remote(psi_ref.at[1 - yl, s], psi_at(s, sub if gone else 1 - sub), io_s.at[s], io_r.at[s], yl_partner)

    for s in PAIR:
        psi_load(s).start()
    barrier = pltpu.get_barrier_semaphore()
    for _, count, _, peers in groups:
        for d in range(1, count):
            pl.semaphore_signal(barrier, inc=1, device_id=peers[d], device_id_type=MESH)
    pl.semaphore_wait(barrier, plane + nz - 2)
    for s in PAIR:
        psi_copy(s, GONE).start()
    for e in range(3 * PIECES):
        r_copy(0, e, GONE).start()
    for r in TRIPLE:
        r_load(r).start()
    for l in TRIPLE:
        l_load(l).start()
    pl.semaphore_signal(credit, inc=1, device_id=sibling, device_id_type=MESH)

    def clear(i):
        for s in PAIR:
            vbuf[1, s, own_block(i), :] = jnp.zeros((ROWS, wa), jnp.float32)
            for p in PAIR:
                vv[p, s, block(i), :] = jnp.zeros((ROWS, wa), jnp.float32)

    fold(clear, wb // ROWS)
    clear_products()
    sc[2] = jnp.zeros((ROWS, wa), jnp.float32)
    def work(name, p, more, slot):
        kind, tail = name[0], name[1:]
        if kind == "m":
            return functools.partial(right_group, p, int(tail[0]), int(tail[1]), tail[2])
        args = [int(digit) for digit in tail]
        if kind in "ab":
            calls = {
                "a0": lambda: alpha_open(p),
                "b0": lambda: (alpha_close(slot), beta_open(p)),
                "b3": lambda: (beta_close(slot), scale(p)),
            }
            return calls.get(name, functools.partial(sum_pass, "ab".index(kind), args[0]))
        if kind == "c":
            return functools.partial(close_chunk, p, *args, more)
        if kind == "d":
            return functools.partial(drain_gather, p)
        if kind == "w":
            return r_last
        if kind == "r":
            return functools.partial(r_take, *args)
        if kind in "lx":
            return functools.partial({"l": left_products, "x": mix}[kind], *args)
        return functools.partial({"p": take_pair, "h": take_hop, "f": left_sum}[kind], p, *args)

    start_order, gather_order, reduce_order = (
        ",".join(order).split(",") for order in (START_ORDER, GATHER_ORDER, REDUCE_ORDER)
    )
    for s in PAIR:
        psi_load(s).wait()
        psi_copy(s, HERE).wait_recv()
        own_sends(0, s * SPLIT)
    for name in start_order:
        if name[0] == "c":
            own_sends(0, int(name[1]))
        else:
            work(name, 0, None, None)()
    for r in TRIPLE:
        r_load(r).wait()
        l_load(r).wait()
    for s in PAIR:
        psi_copy(s, GONE).wait_send()

    def lanczos_step(j, carry):
        p = mod(j, 2)
        slot = mod(j + LANCZOS_STEPS - 1, LANCZOS_STEPS)
        more = j < LANCZOS_STEPS - 1

        for name in gather_order:
            if name[0] in "rw":
                pl.when(j == 0)(work(name, p, more, slot))
            else:
                work(name, p, more, slot)()
        mix(0)

        pl.semaphore_wait(credit, 1)
        for name in reduce_order:
            if name[0] in "ph":
                pl.when(more)(work(name, 1 - p, more, slot))
            else:
                work(name, p, more, slot)()
        for i in range(4):
            sib_copy(chunks[-1], i).wait_send()
        for q in chunks:
            drain_sums(p, q)

        @pl.when(more)
        def _():
            pl.semaphore_signal(credit, inc=1, device_id=sibling, device_id_type=MESH)

        sc[2] = jnp.where(j > 0, sc[1], jnp.zeros((ROWS, wa), jnp.float32))
        return carry

    lax.fori_loop(0, LANCZOS_STEPS, lanczos_step, 0)

    p = LANCZOS_STEPS % 2

    def out_copy(s):
        src = vv.at[1 - p, s, span((1 - sub) * half, half), :]
        return remote(src, ob.at[s], io_s.at[2 + s], io_r.at[2 + s], yl_partner)

    alpha_open(p)
    sum_pass(0, 1)
    alpha_close(LANCZOS_STEPS - 1)
    beta_open(p)
    for s in PAIR:
        out_copy(s).start()
    sum_pass(1, 1)
    beta_close(LANCZOS_STEPS - 1)
    for s in PAIR:
        out_copy(s).wait_recv()

        def put(i):
            vout_ref[yl, s, block(i), :] = vv[1 - p, s, span(sub * half + i * ROWS, ROWS), :] / sc[1]
            vout_ref[1 - yl, s, block(i), :] = ob[s, block(i), :] / sc[1]

        fold(put, half // ROWS)
        out_copy(s).wait_send()


def solution(mesh):
    nz, nx = mesh.shape["col"] // 4, mesh.shape["row"] // 2

    def local_steps(psi_blk, left_blk, mpo_tensor, right_blk):
        wa, wb = psi_blk.shape[0] // 2, psi_blk.shape[2] * 2
        da, db = left_blk.shape[2], right_blk.shape[2]
        half = wb // 2
        hops = nz // 2
        mb = wb // SPLIT
        parts = 2 * SPLIT
        lanes = 128 if wa % 128 == 0 else wa
        f32 = jnp.float32
        psi_t = jnp.transpose(psi_blk.reshape(2, wa, 2, half), (0, 2, 3, 1))
        kernel = functools.partial(lanczos_kernel, nz, nx, wa, wb)
        vmem, dma = pltpu.VMEM, pltpu.SemaphoreType.DMA
        ids = 8 * hops + 2
        scalars, v_out = pl.pallas_call(
            kernel,
            out_shape=(
                jax.ShapeDtypeStruct((2 * LANCZOS_STEPS, ROWS, lanes), f32),
                jax.ShapeDtypeStruct((2, 2, half, wa), f32),
            ),
            in_specs=[
                pl.BlockSpec(memory_space=pl.ANY),
                pl.BlockSpec(memory_space=pl.ANY),
                pl.BlockSpec(memory_space=pltpu.SMEM),
                pl.BlockSpec(memory_space=pl.ANY),
            ],
            out_specs=(pl.BlockSpec(memory_space=pltpu.VMEM),) * 2,
            scratch_shapes=[
                vmem((2, 2, db, wa), f32),
                vmem((3 * wa, da), f32),
                vmem((3 * wb, db), f32),
                vmem((2, 3 * wb, wa), f32),
                vmem((2, wb, 3 * wa), f32),
                vmem((2, 2, wb, wa), f32),
                vmem((parts, 4, mb, 2 * wa), f32),
                vmem((8, mb, 2 * wa), f32),
                vmem((2, parts, 2, 2, mb // 2, wa), f32),
                vmem((2, parts, 2, 2, mb, wa), f32),
                vmem((2, parts, mb, wa), f32),
                vmem((2, half, wa), f32),
                vmem((2, nx * 8 + nz, ROWS, lanes), f32),
                vmem((3, ROWS, wa), f32),
                dma((parts, ids)),
                dma((2, parts, ids)),
                dma((4,)),
                dma((parts, 4)),
                dma((parts, 2, 2)),
                dma((2, parts, 2, 2)),
                dma((parts, 2, 2)),
                dma((2, parts, 2, 2)),
                dma((parts,)),
                dma((2, parts)),
                dma((2, 2)),
                dma((2, 2)),
                dma((8, 3 * PIECES)),
                dma((8, 3 * PIECES)),
                dma((4,)),
                dma((4,)),
                dma((8,)),
                pltpu.SemaphoreType.REGULAR,
            ],
            compiler_params=pltpu.CompilerParams(collective_id=0, has_side_effects=True, vmem_limit_bytes=66 * 1000 * 1000),
            name="lanczos",
        )(psi_t, jnp.transpose(left_blk, (1, 0, 2)), jnp.transpose(mpo_tensor, (0, 2, 3, 1)), jnp.transpose(right_blk, (1, 0, 2)))
        v_next = jnp.transpose(v_out, (0, 3, 1, 2)).reshape(psi_blk.shape)
        return scalars[:LANCZOS_STEPS, 0, 0], scalars[LANCZOS_STEPS:, 0, 0], v_next

    return jax.shard_map(
        local_steps,
        mesh=mesh,
        in_specs=(P("row", None, "col"), P("row", None, None), P(), P("col", None, None)),
        out_specs=(P(), P(), P("row", None, "col")),
        check_vma=False,
    )
```

```python
import functools

import jax
import jax.numpy as jnp
from jax import lax
from jax.experimental import pallas as pl
from jax.experimental.pallas import tpu as pltpu
from jax.sharding import PartitionSpec as P

LANCZOS_STEPS = 4
EXACT_PREC = lax.Precision.HIGHEST
MESH = pl.DeviceIdType.MESH
ROWS = 8
SPLIT = 2
PIECES = 2
START_ORDER = (
    "r00,c1,r01,p1,r02,p0,h111,h001,r03,h011,r11,h121,h101,r10",
    "h012,h021,r05,h002,h102,r20,c3,r04,r15,r21,r13,p2,h022,r12",
    "h201,r14,h103,h112",
)
GATHER_ORDER = (
    "n00*,r25,h122,h023,h301,h013,p3,a0,r24,r22,h003,r23,w,k01-",
    "h221,n02+,h211,k02-,m10*,h302,h311,h202,n02-,n01-,h123,h113",
    "h104,k01+,h321,n01+,h212,m03+,m11-,k02+,a1,m03-,h303,h312",
    "m11+,h114,k00*,h004,h024,h222,h322,h203,m12-,m12+,h014,h213",
    "b0,h223,h124,h313,m04*,h323,h304,h204,m13-,b1,h214,m13+,h324",
    "h224,h314,m14*",
)
REDUCE_ORDER = (
    "l00,x1,b3,f000,l01,f030,l02,f010,f020,l10,f021,x2,f100,l11",
    "f130,f011,l12,d0,f110,f120,l20,f121,f111,c0,f200,l21,p0,f230",
    "l22,x3,h001,c1,h011,f210,f220,h021,l30,f211,f300,h002,l31",
    "f330,f221,h101,h012,h022,l32,h111,f320,f310,f311,f321,p1,c2",
    "h102,h121,h112,p2,c3,h201,h103",
)
PAIR = range(2)
TRIPLE = range(3)
WAYS = (1, -1)
GONE, HERE = True, False


def fold(body, count, unroll=4):
    while count % unroll:
        unroll //= 2

    def trip(i, carry):
        for u in range(unroll):
            body(i * unroll + u)
        return carry

    lax.fori_loop(0, count // unroll, trip, 0)


def lanczos_kernel(
    nz, nx, wa, wb,
    psi_ref, l_hbm, w_ref, r_hbm,
    scal_ref, vout_ref,
    vbuf, lbuf, rbuf, ubuf, tbuf, vv, rd, yb, hx, fx, yx, ob, red, sc,
    ag_s, ag_r, rd_s, rd_r, hx_s, hx_r, fx_s, fx_r, yx_s, yx_r,
    ar_s, ar_r, rr_s, rr_r, io_s, io_r, ld_s, credit,
):
    hops = nz // 2
    half, mb = wb // 2, wb // SPLIT
    part = half // (2 * nx)
    bit = part // PIECES
    chunks = range(2 * SPLIT)
    col, row = lax.axis_index("col"), lax.axis_index("row")
    div, mod = lax.div, lax.rem
    z, y, x, c = div(col, 4), mod(col, 4), div(row, 2), mod(row, 2)
    yh, sub = div(y, 2), mod(y, 2)
    yl = mod(div(y + 1, 2), 2)

    def dev(zz=None, yy=None, xx=None, cc=None):
        zz = z if zz is None else zz
        yy = y if yy is None else yy
        xx = x if xx is None else xx
        cc = c if cc is None else cc
        return {"col": zz * 4 + yy, "row": xx * 2 + cc}

    zs = {off: mod(z + off + nz, nz) for off in range(-hops, nz)}
    xs = {off: mod(x + off + nx, nx) for off in range(-1, nx)}
    starts = {off: (at * 2 + yh) * wb for off, at in zs.items()}
    others = {off: (at * 2 + 1 - yh) * wb for off, at in zs.items()}
    own = starts[0]

    sibling = dev(cc=1 - c)
    yl_partner = dev(yy=y + 1 - 2 * sub)
    yh_partner = dev(yy=3 - y)
    z_next = {d: dev(zz=zs[d]) for d in WAYS}
    x_next = {d: dev(xx=xs[d]) for d in WAYS}
    x_side = {d: dev(yy=y + 1 - 2 * sub, xx=xs[d]) for d in WAYS}

    def remote(src, dst, send, recv, to):
        return pltpu.make_async_remote_copy(
            src_ref=src, dst_ref=dst, send_sem=send, recv_sem=recv, device_id=to, device_id_type=MESH
        )

    def span(start, count):
        return pl.ds(pl.multiple_of(start, ROWS), count)

    def block(i):
        return span(i * ROWS, ROWS)

    def cut(q):
        return mb * (96, 96, 64, 32)[q] // 128

    def lines(q):
        return TRIPLE if cut(q) else TRIPLE[1:]

    def piece(p, q, base, kind, d, h, mid, to):
        start, count = (0, cut(q)) if kind == 0 else (cut(q), mb - cut(q))
        if h == hops:
            count //= 2
            start += count if d < 0 else 0
        at = vbuf.at[p, q // SPLIT, span(base + (q % SPLIT) * mb + start, count), :]
        return remote(at, at, ag_s.at[q, mid], ag_r.at[p, q, mid], to)

    def z_copy(p, q, d, line, h, gone):
        base = (others if line == 2 else starts)[-d * (h - 1 if gone else h)]
        mid = ((0 if d > 0 else 3) + line) * hops + h - 1
        return piece(p, q, base, min(line, 1), d, h, mid, z_next[d])

    def pair_copy(p, q, kind, d, h, gone):
        mid = 6 * hops + (2 * h + max(d, 0) if h else 0 if kind else 1)
        return piece(p, q, (starts if gone else others)[-d * h], kind, d, h, mid, yh_partner)

    def own_sends(p, q):
        pair_copy(p, q, 1, 0, 0, GONE).start()
        for line in lines(q)[:-1]:
            for d in WAYS:
                z_copy(p, q, d, line, 1, GONE).start()
        if cut(q):
            pair_copy(p, q, 0, 0, 0, GONE).start()

    def take_pair(p, q):
        pair_copy(p, q, 1, 0, 0, HERE).wait_recv()
        for d in WAYS:
            z_copy(p, q, d, 2, 1, GONE).start()

    def take_hop(p, q, line, h):
        for d in WAYS:
            z_copy(p, q, d, line, h, HERE).wait_recv()
            if h < hops:
                z_copy(p, q, d, line, h + 1, GONE).start()
            if line == 0:
                pair_copy(p, q, 0, d, h, GONE).start()

    def drain_gather(p):
        for q in chunks:
            first = range(0 if cut(q) else 1, 2)
            for kind in first:
                pair_copy(p, q, kind, 0, 0, GONE).wait_send()
            for d in WAYS:
                for h in range(1, hops + 1):
                    for line in lines(q):
                        z_copy(p, q, d, line, h, GONE).wait_send()
                    for _ in first[1:]:
                        pair_copy(p, q, 0, d, h, GONE).wait_send()

    plane = nx * 8

    line = [mod(row * 4 + y + d, plane) for d in range(plane)]
    groups = (
        (0, plane, row * 4 + y, [{"col": z * 4 + mod(at, 4), "row": div(at, 4)} for at in line]),
        (plane, nz, z, [dev(zz=zs[d]) for d in range(nz)]),
    )

    def sum_send(which, stage, tile):
        base, count, me, peers = groups[stage]
        red[which, base + me] = tile
        at = red.at[which, base + me]
        for d in range(1, count):
            remote(at, at, ar_s.at[which, stage], ar_r.at[which, stage], peers[d]).start()

    def sum_take(which, stage):
        base, count, _, _ = groups[stage]
        at = red.at[which, pl.ds(base, count - 1)]
        pltpu.make_async_copy(at, at, ar_r.at[which, stage]).wait()
        pltpu.make_async_copy(at, at, ar_s.at[which, stage]).wait()
        total = red[which, base]
        for i in range(1, count):
            total = total + red[which, base + i]
        return total

    def sum_pass(which, stage):
        sum_send(which, stage, sum_take(which, stage - 1))

    lanes = red.shape[-1]

    def narrow(tile):
        out = tile[:, :lanes]
        for i in range(1, wa // lanes):
            out = out + tile[:, i * lanes : (i + 1) * lanes]
        return out

    def own_block(i):
        return span(own + i * ROWS, ROWS)

    def accumulate(term):
        def trip(i, acc):
            for s in PAIR:
                acc = acc + term(s, i)
            return acc

        return lax.fori_loop(0, wb // ROWS, trip, jnp.zeros((ROWS, wa), jnp.float32), unroll=4)

    def alpha_open(p):
        acc = accumulate(lambda s, i: vv[p, s, block(i), :] * vbuf[p, s, own_block(i), :])
        sum_send(0, 0, narrow(acc))

    def alpha_close(slot):
        value = jnp.full((ROWS, wa), jnp.sum(sum_take(0, 1)), jnp.float32)
        sc[0] = value
        scal_ref[slot] = value[:, :lanes]

    def beta_open(p):
        alpha, beta = sc[0], sc[2]

        def term(s, i):
            u = vbuf[p, s, own_block(i), :] - alpha * vv[p, s, block(i), :] - beta * vv[1 - p, s, block(i), :]
            vv[1 - p, s, block(i), :] = u
            return u * u

        sum_send(1, 0, narrow(accumulate(term)))

    def beta_close(slot):
        value = jnp.sqrt(jnp.full((ROWS, wa), jnp.sum(sum_take(1, 1)), jnp.float32))
        sc[1] = value
        scal_ref[LANCZOS_STEPS + slot] = value[:, :lanes]

    def scale(p):
        def trip(i):
            for s in PAIR:
                vv[1 - p, s, block(i), :] = vv[1 - p, s, block(i), :] / sc[1]

        fold(trip, wb // ROWS)

    def r_rows(e, of_sub, xx, cc):
        start = (e // PIECES) * wb + of_sub * half + (xx * 2 + cc) * part + (e % PIECES) * bit
        return rbuf.at[span(start, bit), :]

    def r_copy(way, e, gone):
        if way == 0:
            src = r_hbm.at[e // PIECES, span(row * part + (e % PIECES) * bit, bit), :]
            return remote(src, r_rows(e, sub if gone else 1 - sub, x, c), rr_s.at[0, e], rr_r.at[0, e], yl_partner)
        over = isinstance(way, tuple)
        from_way = way[0] if over else way
        slot = from_way % 4
        d = from_way if from_way in WAYS else 1 if e % PIECES == 0 else -1
        away = {0: 0, 2: 2}.get(from_way, -d) - (d if gone and not over else 0)
        away = -d if gone and not over and from_way == 2 else 0 if gone and not over else away
        at = r_rows(e, 1 - sub, xs[away], 1 - c if over and not gone else c)
        slot = slot + 4 if over else slot
        return remote(at, at, rr_s.at[slot, e], rr_r.at[slot, e], sibling if over else x_next[d])

    def r_take(way, e):
        for d in WAYS if way == 1 else (way,):
            r_copy(d, e, HERE).wait_recv()
            r_copy((d,), e, GONE).start()
            if way == 0:
                for n in WAYS:
                    r_copy(n, e, GONE).start()
            elif way == 1 and d == (1 if e % PIECES == 0 else -1):
                r_copy(2, e, GONE).start()

    def r_last():
        for e in range(3 * PIECES):
            for way in (0, 1, -1, 2):
                r_copy((way,), e, HERE).wait_recv()
                r_copy((way,), e, GONE).wait_send()
                r_copy(way, e, GONE).wait_send()

    def right_group(p, s, h, way):
        d = 1 if way == "+" else -1
        for q in range(s * SPLIT, s * SPLIT + SPLIT):
            for e in (d,) if way != "*" else WAYS if h else (0,):
                if cut(q):
                    pair_copy(p, q, 0, e, h, HERE).wait_recv()

        def one(i, carry):
            start = pl.multiple_of((zs[-d * h] * 2 + i) * wb, wb)
            ubuf[s] = ubuf[s] + jnp.dot(
                rbuf[:, pl.ds(start, wb)],
                vbuf[p, s, pl.ds(start, wb), :],
                precision=EXACT_PREC,
                preferred_element_type=jnp.float32,
            )
            return carry

        lax.fori_loop(0, 2, one, 0)

    def clear_products():
        def trip(i):
            for s in PAIR:
                ubuf[s, block(i), :] = jnp.zeros((ROWS, wa), jnp.float32)

        fold(trip, 3 * wb // ROWS)

    def mix(q):
        t, base = q // SPLIT, (q % SPLIT) * mb

        def trip(i):
            tiles = [[ubuf[s, span(r * wb + base + i * ROWS, ROWS), :] for s in PAIR] for r in TRIPLE]
            for l in TRIPLE:
                acc = None
                for r in TRIPLE:
                    for s in PAIR:
                        term = w_ref[l, s, t, r] * tiles[r][s]
                        acc = term if acc is None else acc + term
                tbuf[t, span(base + i * ROWS, ROWS), l * wa : (l + 1) * wa] = acc

        fold(trip, mb // ROWS, 1)
        if q == chunks[-1]:
            clear_products()

    def sib_copy(q, i):
        return remote(yb.at[i], rd.at[q, i], rd_s.at[i], rd_r.at[q, i], sibling)

    def left_products(q, part):
        def one(n, carry):
            theirs = (n < 2, n > 0, n < 0)[part]
            i = n + 1 if part == 2 else jnp.where(n == 1 - part, 3, n * part)
            away = jnp.where(i < 2, i + 2, 3 - i)
            start = (mod(x + away, nx) * 2 + jnp.where(theirs, 1 - c, c)) * 2 * wa
            yb[jnp.where(theirs, i, i + 4)] = jnp.dot(
                tbuf[q // SPLIT, (q % SPLIT) * mb : (q % SPLIT + 1) * mb, :],
                lbuf[:, pl.ds(pl.multiple_of(start, 2 * wa), 2 * wa)],
                precision=EXACT_PREC,
                preferred_element_type=jnp.float32,
            )

            @pl.when(theirs)
            def _():
                sib_copy(q, i).start()

            return carry

        for i in ((0, 3), (1, 2), ())[part] if q else ():
            sib_copy(q - 1, i).wait_send()
        lax.fori_loop(0, (3, 3, 2)[part], one, 0)

    lane_at = {GONE: (1 - yl) * wa, HERE: yl * wa}

    def lane(theirs):
        return pl.ds(pl.multiple_of(lane_at[theirs], wa), wa)

    def half_copy(p, q, d, theirs):
        slot, side = 0 if d > 0 else 1, 0 if theirs else 1
        src = rd.at[q, 0, pl.ds(slot * mb // 2, mb // 2), lane(theirs)]
        return remote(src, hx.at[p, q, slot, side], hx_s.at[q, slot, side], hx_r.at[p, q, slot, side], x_next[d])

    def full_copy(p, q, d, theirs):
        slot, side = 0 if d > 0 else 1, 0 if theirs else 1
        src = rd.at[q, 2 - slot, :, lane(theirs)]
        to = (x_side if theirs else x_next)[d]
        return remote(src, fx.at[p, q, slot, side], fx_s.at[q, slot, side], fx_r.at[p, q, slot, side], to)

    def cross_copy(p, q):
        return remote(rd.at[q, 3, :, lane(GONE)], yx.at[p, q], yx_s.at[q], yx_r.at[p, q], yl_partner)

    def left_sum(p, q, i, side):
        if side == 0:
            sib_copy(q, i).wait_recv()

            def add(k):
                rows = block(k)
                rd[q, i, rows, :] = rd[q, i, rows, :] + yb[i + 4, rows, :]

            fold(add, mb // ROWS)
        if i == 0:
            for theirs in (GONE, HERE):
                for d in WAYS:
                    half_copy(p, q, d, theirs).start()
        elif i < 3:
            d, theirs = 2 * i - 3, side == 0
            lanes_at = lane(theirs)
            half_copy(p, q, d, theirs).wait_recv()

            def add_half(k):
                rows = span(k * ROWS + (0 if d > 0 else mb // 2), ROWS)
                rd[q, i, rows, lanes_at] = rd[q, i, rows, lanes_at] + hx[p, q, i % 2, side, block(k), :]

            fold(add_half, mb // 2 // ROWS)
            full_copy(p, q, d, theirs).start()
        else:
            cross_copy(p, q).start()

    def close_chunk(p, q, more):
        for theirs in (GONE, HERE):
            for d in WAYS:
                full_copy(p, q, d, theirs).wait_recv()
        cross_copy(p, q).wait_recv()
        alpha, beta, old = sc[0], sc[1], sc[2]
        s, mine = q // SPLIT, lane(HERE)

        def step(k):
            rows, at = block(k), own_block(k + (q % SPLIT) * mb // ROWS)
            g = rd[q, 3, rows, mine] + yx[p, q, rows, :]
            for slot in PAIR:
                g = g + (fx[p, q, slot, 0, rows, :] + fx[p, q, slot, 1, rows, :])
            vbuf[1 - p, s, at, :] = (g - alpha * vbuf[p, s, at, :] - old * vbuf[1 - p, s, at, :]) / beta

        fold(step, mb // ROWS)

        @pl.when(more)
        def _():
            own_sends(1 - p, q)

    def drain_sums(p, q):
        for theirs in (GONE, HERE):
            for d in WAYS:
                half_copy(p, q, d, theirs).wait_send()
                full_copy(p, q, d, theirs).wait_send()
        cross_copy(p, q).wait_send()

    def l_load(l):
        return pltpu.make_async_copy(l_hbm.at[l, span(yl * wa, wa), :], lbuf.at[pl.ds(l * wa, wa), :], ld_s.at[l])

    def r_load(r):
        return pltpu.make_async_copy(r_hbm.at[r], rbuf.at[span(r * wb + sub * half, half), :], ld_s.at[3 + r])

    def psi_at(s, of_sub):
        return vbuf.at[0, s, span(own + of_sub * half, half), :]

    def psi_load(s):
        return pltpu.make_async_copy(psi_ref.at[yl, s], psi_at(s, sub), ld_s.at[6 + s])

    def psi_copy(s, gone):
        return remote(psi_ref.at[1 - yl, s], psi_at(s, sub if gone else 1 - sub), io_s.at[s], io_r.at[s], yl_partner)

    for s in PAIR:
        psi_load(s).start()
    barrier = pltpu.get_barrier_semaphore()
    for _, count, _, peers in groups:
        for d in range(1, count):
            pl.semaphore_signal(barrier, inc=1, device_id=peers[d], device_id_type=MESH)
    pl.semaphore_wait(barrier, plane + nz - 2)
    for s in PAIR:
        psi_copy(s, GONE).start()
    for e in range(3 * PIECES):
        r_copy(0, e, GONE).start()
    for r in TRIPLE:
        r_load(r).start()
    for l in TRIPLE:
        l_load(l).start()
    pl.semaphore_signal(credit, inc=1, device_id=sibling, device_id_type=MESH)

    def clear(i):
        for s in PAIR:
            vbuf[1, s, own_block(i), :] = jnp.zeros((ROWS, wa), jnp.float32)
            for p in PAIR:
                vv[p, s, block(i), :] = jnp.zeros((ROWS, wa), jnp.float32)

    fold(clear, wb // ROWS)
    clear_products()
    sc[2] = jnp.zeros((ROWS, wa), jnp.float32)
    def work(name, p, more, slot):
        kind, tail = name[0], name[1:]
        if kind in "mnk":
            return functools.partial(right_group, p, int(tail[0]), int(tail[1]), tail[2])
        args = [int(digit) for digit in tail]
        if kind in "ab":
            calls = {
                "a0": lambda: alpha_open(p),
                "b0": lambda: (alpha_close(slot), beta_open(p)),
                "b3": lambda: (beta_close(slot), scale(p)),
            }
            return calls.get(name, functools.partial(sum_pass, "ab".index(kind), args[0]))
        if kind == "c":
            return functools.partial(close_chunk, p, *args, more)
        if kind == "d":
            return functools.partial(drain_gather, p)
        if kind == "w":
            return r_last
        if kind == "r":
            return functools.partial(r_take, *args)
        if kind in "lx":
            return functools.partial({"l": left_products, "x": mix}[kind], *args)
        return functools.partial({"p": take_pair, "h": take_hop, "f": left_sum}[kind], p, *args)

    start_order, gather_order, reduce_order = (
        ",".join(order).split(",") for order in (START_ORDER, GATHER_ORDER, REDUCE_ORDER)
    )
    for s in PAIR:
        psi_load(s).wait()
        psi_copy(s, HERE).wait_recv()
        own_sends(0, s * SPLIT)
    for name in start_order:
        if name[0] == "c":
            own_sends(0, int(name[1]))
        else:
            work(name, 0, None, None)()
    for r in TRIPLE:
        r_load(r).wait()
        l_load(r).wait()
    for s in PAIR:
        psi_copy(s, GONE).wait_send()

    def lanczos_step(j, carry):
        p = mod(j, 2)
        slot = mod(j + LANCZOS_STEPS - 1, LANCZOS_STEPS)
        more = j < LANCZOS_STEPS - 1

        for name in gather_order:
            if name[0] in "rwk":
                pl.when(j == 0)(work(name, p, more, slot))
            elif name[0] == "n":
                pl.when(j > 0)(work(name, p, more, slot))
            else:
                work(name, p, more, slot)()
        mix(0)

        pl.semaphore_wait(credit, 1)
        for name in reduce_order:
            if name[0] in "ph":
                pl.when(more)(work(name, 1 - p, more, slot))
            else:
                work(name, p, more, slot)()
        for i in range(4):
            sib_copy(chunks[-1], i).wait_send()
        for q in chunks:
            drain_sums(p, q)

        @pl.when(more)
        def _():
            pl.semaphore_signal(credit, inc=1, device_id=sibling, device_id_type=MESH)

        sc[2] = jnp.where(j > 0, sc[1], jnp.zeros((ROWS, wa), jnp.float32))
        return carry

    lax.fori_loop(0, LANCZOS_STEPS, lanczos_step, 0)

    p = LANCZOS_STEPS % 2

    def out_copy(s):
        src = vv.at[1 - p, s, span((1 - sub) * half, half), :]
        return remote(src, ob.at[s], io_s.at[2 + s], io_r.at[2 + s], yl_partner)

    alpha_open(p)
    sum_pass(0, 1)
    alpha_close(LANCZOS_STEPS - 1)
    beta_open(p)
    for s in PAIR:
        out_copy(s).start()
    sum_pass(1, 1)
    beta_close(LANCZOS_STEPS - 1)
    for s in PAIR:
        out_copy(s).wait_recv()

        def put(i):
            vout_ref[yl, s, block(i), :] = vv[1 - p, s, span(sub * half + i * ROWS, ROWS), :] / sc[1]
            vout_ref[1 - yl, s, block(i), :] = ob[s, block(i), :] / sc[1]

        fold(put, half // ROWS)
        out_copy(s).wait_send()


def solution(mesh):
    nz, nx = mesh.shape["col"] // 4, mesh.shape["row"] // 2

    def local_steps(psi_blk, left_blk, mpo_tensor, right_blk):
        wa, wb = psi_blk.shape[0] // 2, psi_blk.shape[2] * 2
        da, db = left_blk.shape[2], right_blk.shape[2]
        half = wb // 2
        hops = nz // 2
        mb = wb // SPLIT
        parts = 2 * SPLIT
        lanes = 128 if wa % 128 == 0 else wa
        f32 = jnp.float32
        psi_t = jnp.transpose(psi_blk.reshape(2, wa, 2, half), (0, 2, 3, 1))
        kernel = functools.partial(lanczos_kernel, nz, nx, wa, wb)
        vmem, dma = pltpu.VMEM, pltpu.SemaphoreType.DMA
        ids = 8 * hops + 2
        scalars, v_out = pl.pallas_call(
            kernel,
            out_shape=(
                jax.ShapeDtypeStruct((2 * LANCZOS_STEPS, ROWS, lanes), f32),
                jax.ShapeDtypeStruct((2, 2, half, wa), f32),
            ),
            in_specs=[
                pl.BlockSpec(memory_space=pl.ANY),
                pl.BlockSpec(memory_space=pl.ANY),
                pl.BlockSpec(memory_space=pltpu.SMEM),
                pl.BlockSpec(memory_space=pl.ANY),
            ],
            out_specs=(pl.BlockSpec(memory_space=pltpu.VMEM),) * 2,
            scratch_shapes=[
                vmem((2, 2, db, wa), f32),
                vmem((3 * wa, da), f32),
                vmem((3 * wb, db), f32),
                vmem((2, 3 * wb, wa), f32),
                vmem((2, wb, 3 * wa), f32),
                vmem((2, 2, wb, wa), f32),
                vmem((parts, 4, mb, 2 * wa), f32),
                vmem((8, mb, 2 * wa), f32),
                vmem((2, parts, 2, 2, mb // 2, wa), f32),
                vmem((2, parts, 2, 2, mb, wa), f32),
                vmem((2, parts, mb, wa), f32),
                vmem((2, half, wa), f32),
                vmem((2, nx * 8 + nz, ROWS, lanes), f32),
                vmem((3, ROWS, wa), f32),
                dma((parts, ids)),
                dma((2, parts, ids)),
                dma((4,)),
                dma((parts, 4)),
                dma((parts, 2, 2)),
                dma((2, parts, 2, 2)),
                dma((parts, 2, 2)),
                dma((2, parts, 2, 2)),
                dma((parts,)),
                dma((2, parts)),
                dma((2, 2)),
                dma((2, 2)),
                dma((8, 3 * PIECES)),
                dma((8, 3 * PIECES)),
                dma((4,)),
                dma((4,)),
                dma((8,)),
                pltpu.SemaphoreType.REGULAR,
            ],
            compiler_params=pltpu.CompilerParams(collective_id=0, has_side_effects=True, vmem_limit_bytes=66 * 1000 * 1000),
            name="lanczos",
        )(psi_t, jnp.transpose(left_blk, (1, 0, 2)), jnp.transpose(mpo_tensor, (0, 2, 3, 1)), jnp.transpose(right_blk, (1, 0, 2)))
        v_next = jnp.transpose(v_out, (0, 3, 1, 2)).reshape(psi_blk.shape)
        return scalars[:LANCZOS_STEPS, 0, 0], scalars[LANCZOS_STEPS:, 0, 0], v_next

    return jax.shard_map(
        local_steps,
        mesh=mesh,
        in_specs=(P("row", None, "col"), P("row", None, None), P(), P("col", None, None)),
        out_specs=(P(), P(), P("row", None, "col")),
        check_vma=False,
    )
```

```python
import functools

import jax
import jax.numpy as jnp
from jax import lax
from jax.experimental import pallas as pl
from jax.experimental.pallas import tpu as pltpu
from jax.sharding import PartitionSpec as P

LANCZOS_STEPS = 4
EXACT_PREC = lax.Precision.HIGHEST
MESH = pl.DeviceIdType.MESH
ROWS = 8
SPLIT = 2
PIECES = 2
START_ORDER = (
    "p0,c1,h001,r00,r01,h011,r02,h101,h021,r10,p1,h111,c3,r03",
    "h012,h102,r11,r05,h301,r04,r12,h211,h002,r15,h022,h121,r20",
    "h112,h201,r14,p2,r13,h122",
)
GATHER_ORDER = (
    "n02+,h311,a0,r25,r21,h103,n02-,n01+,r22,h113,r24,h023,h013",
    "h212,h003,r23,w,p3,m10*,k01+,k01-,h202,n00*,h221,h114,h024",
    "h104,k02-,a1,k02+,h123,h302,h321,m03-,h312,k00*,n01-,m11-",
    "h303,h004,h222,h203,m03+,h322,m12-,h124,b0,m11+,h223,h313",
    "h304,h213,h014,h204,m04*,h323,m13+,m12+,m13-,h324,h224,h314",
    "h214,m14*,b1",
)
REDUCE_ORDER = (
    "x1,l00,f000,l01,l02,f020,f010,d0,x2,l10,f030,f100,f021,l11",
    "f130,f011,l12,f110,f120,b3,l20,f200,c0,f111,l21,f230,f121",
    "l22,p0,f210,f220,h001,f211,x3,h011,l30,h021,f300,f221,c1,l31",
    "h002,f330,l32,f320,h022,p1,h012,f321,h101,h111,f310,h121,c2",
    "f311,h102,h112,c3,h211,h301,h122,p2,h201",
)
PAIR = range(2)
TRIPLE = range(3)
WAYS = (1, -1)
GONE, HERE = True, False


def fold(body, count, unroll=4):
    while count % unroll:
        unroll //= 2

    def trip(i, carry):
        for u in range(unroll):
            body(i * unroll + u)
        return carry

    lax.fori_loop(0, count // unroll, trip, 0)


def lanczos_kernel(
    nz, nx, wa, wb,
    psi_ref, l_hbm, w_ref, r_hbm,
    scal_ref, vout_ref,
    vbuf, lbuf, rbuf, ubuf, tbuf, vv, rd, yb, hx, fx, yx, ob, red, sc,
    ag_s, ag_r, rd_s, rd_r, hx_s, hx_r, fx_s, fx_r, yx_s, yx_r,
    ar_s, ar_r, rr_s, rr_r, io_s, io_r, ld_s, credit,
):
    hops = nz // 2
    half, mb = wb // 2, wb // SPLIT
    part = half // (2 * nx)
    bit = part // PIECES
    chunks = range(2 * SPLIT)
    col, row = lax.axis_index("col"), lax.axis_index("row")
    div, mod = lax.div, lax.rem
    z, y, x, c = div(col, 4), mod(col, 4), div(row, 2), mod(row, 2)
    yh, sub = div(y, 2), mod(y, 2)
    yl = mod(div(y + 1, 2), 2)

    def dev(zz=None, yy=None, xx=None, cc=None):
        zz = z if zz is None else zz
        yy = y if yy is None else yy
        xx = x if xx is None else xx
        cc = c if cc is None else cc
        return {"col": zz * 4 + yy, "row": xx * 2 + cc}

    zs = {off: mod(z + off + nz, nz) for off in range(-hops, nz)}
    xs = {off: mod(x + off + nx, nx) for off in range(-1, nx)}
    starts = {off: (at * 2 + yh) * wb for off, at in zs.items()}
    others = {off: (at * 2 + 1 - yh) * wb for off, at in zs.items()}
    own = starts[0]

    sibling = dev(cc=1 - c)
    yl_partner = dev(yy=y + 1 - 2 * sub)
    yh_partner = dev(yy=3 - y)
    z_next = {d: dev(zz=zs[d]) for d in WAYS}
    x_next = {d: dev(xx=xs[d]) for d in WAYS}
    x_side = {d: dev(yy=y + 1 - 2 * sub, xx=xs[d]) for d in WAYS}

    def remote(src, dst, send, recv, to):
        return pltpu.make_async_remote_copy(
            src_ref=src, dst_ref=dst, send_sem=send, recv_sem=recv, device_id=to, device_id_type=MESH
        )

    def span(start, count):
        return pl.ds(pl.multiple_of(start, ROWS), count)

    def block(i):
        return span(i * ROWS, ROWS)

    def cut(q):
        return mb * (96, 96, 64, 32)[q] // 128

    def lines(q):
        return TRIPLE if cut(q) else TRIPLE[1:]

    def piece(p, q, base, kind, d, h, mid, to):
        start, count = (0, cut(q)) if kind == 0 else (cut(q), mb - cut(q))
        if h == hops:
            count //= 2
            start += count if d < 0 else 0
        at = vbuf.at[p, q // SPLIT, span(base + (q % SPLIT) * mb + start, count), :]
        return remote(at, at, ag_s.at[q, mid], ag_r.at[p, q, mid], to)

    def z_copy(p, q, d, line, h, gone):
        base = (others if line == 2 else starts)[-d * (h - 1 if gone else h)]
        mid = ((0 if d > 0 else 3) + line) * hops + h - 1
        return piece(p, q, base, min(line, 1), d, h, mid, z_next[d])

    def pair_copy(p, q, kind, d, h, gone):
        mid = 6 * hops + (2 * h + max(d, 0) if h else 0 if kind else 1)
        return piece(p, q, (starts if gone else others)[-d * h], kind, d, h, mid, yh_partner)

    def own_sends(p, q):
        pair_copy(p, q, 1, 0, 0, GONE).start()
        for line in lines(q)[:-1]:
            for d in WAYS:
                z_copy(p, q, d, line, 1, GONE).start()
        if cut(q):
            pair_copy(p, q, 0, 0, 0, GONE).start()

    def take_pair(p, q):
        pair_copy(p, q, 1, 0, 0, HERE).wait_recv()
        for d in WAYS:
            z_copy(p, q, d, 2, 1, GONE).start()

    def take_hop(p, q, line, h):
        for d in WAYS:
            z_copy(p, q, d, line, h, HERE).wait_recv()
            if h < hops:
                z_copy(p, q, d, line, h + 1, GONE).start()
            if line == 0:
                pair_copy(p, q, 0, d, h, GONE).start()

    def drain_gather(p):
        for q in chunks:
            first = range(0 if cut(q) else 1, 2)
            for kind in first:
                pair_copy(p, q, kind, 0, 0, GONE).wait_send()
            for d in WAYS:
                for h in range(1, hops + 1):
                    for line in lines(q):
                        z_copy(p, q, d, line, h, GONE).wait_send()
                    for _ in first[1:]:
                        pair_copy(p, q, 0, d, h, GONE).wait_send()

    plane = nx * 8

    line = [mod(row * 4 + y + d, plane) for d in range(plane)]
    groups = (
        (0, plane, row * 4 + y, [{"col": z * 4 + mod(at, 4), "row": div(at, 4)} for at in line]),
        (plane, nz, z, [dev(zz=zs[d]) for d in range(nz)]),
    )

    def sum_send(which, stage, tile):
        base, count, me, peers = groups[stage]
        red[which, base + me] = tile
        at = red.at[which, base + me]
        for d in range(1, count):
            remote(at, at, ar_s.at[which, stage], ar_r.at[which, stage], peers[d]).start()

    def sum_take(which, stage):
        base, count, _, _ = groups[stage]
        at = red.at[which, pl.ds(base, count - 1)]
        pltpu.make_async_copy(at, at, ar_r.at[which, stage]).wait()
        pltpu.make_async_copy(at, at, ar_s.at[which, stage]).wait()
        total = red[which, base]
        for i in range(1, count):
            total = total + red[which, base + i]
        return total

    def sum_pass(which, stage):
        sum_send(which, stage, sum_take(which, stage - 1))

    lanes = red.shape[-1]

    def narrow(tile):
        out = tile[:, :lanes]
        for i in range(1, wa // lanes):
            out = out + tile[:, i * lanes : (i + 1) * lanes]
        return out

    def own_block(i):
        return span(own + i * ROWS, ROWS)

    def accumulate(term):
        def trip(i, acc):
            for s in PAIR:
                acc = acc + term(s, i)
            return acc

        return lax.fori_loop(0, wb // ROWS, trip, jnp.zeros((ROWS, wa), jnp.float32), unroll=4)

    def alpha_open(p):
        acc = accumulate(lambda s, i: vv[p, s, block(i), :] * vbuf[p, s, own_block(i), :])
        sum_send(0, 0, narrow(acc))

    def alpha_close(slot):
        value = jnp.full((ROWS, wa), jnp.sum(sum_take(0, 1)), jnp.float32)
        sc[0] = value
        scal_ref[slot] = value[:, :lanes]

    def beta_open(p):
        alpha, beta = sc[0], sc[2]

        def term(s, i):
            u = vbuf[p, s, own_block(i), :] - alpha * vv[p, s, block(i), :] - beta * vv[1 - p, s, block(i), :]
            vv[1 - p, s, block(i), :] = u
            return u * u

        sum_send(1, 0, narrow(accumulate(term)))

    def beta_close(slot):
        value = jnp.sqrt(jnp.full((ROWS, wa), jnp.sum(sum_take(1, 1)), jnp.float32))
        sc[1] = value
        scal_ref[LANCZOS_STEPS + slot] = value[:, :lanes]

    def scale(p):
        def trip(i):
            for s in PAIR:
                vv[1 - p, s, block(i), :] = vv[1 - p, s, block(i), :] / sc[1]

        fold(trip, wb // ROWS)

    def r_rows(e, of_sub, xx, cc):
        start = (e // PIECES) * wb + of_sub * half + (xx * 2 + cc) * part + (e % PIECES) * bit
        return rbuf.at[span(start, bit), :]

    def r_copy(way, e, gone):
        if way == 0:
            src = r_hbm.at[e // PIECES, span(row * part + (e % PIECES) * bit, bit), :]
            return remote(src, r_rows(e, sub if gone else 1 - sub, x, c), rr_s.at[0, e], rr_r.at[0, e], yl_partner)
        over = isinstance(way, tuple)
        from_way = way[0] if over else way
        slot = from_way % 4
        d = from_way if from_way in WAYS else 1 if e % PIECES == 0 else -1
        away = {0: 0, 2: 2}.get(from_way, -d) - (d if gone and not over else 0)
        away = -d if gone and not over and from_way == 2 else 0 if gone and not over else away
        at = r_rows(e, 1 - sub, xs[away], 1 - c if over and not gone else c)
        slot = slot + 4 if over else slot
        return remote(at, at, rr_s.at[slot, e], rr_r.at[slot, e], sibling if over else x_next[d])

    def r_take(way, e):
        for d in WAYS if way == 1 else (way,):
            r_copy(d, e, HERE).wait_recv()
            r_copy((d,), e, GONE).start()
            if way == 0:
                for n in WAYS:
                    r_copy(n, e, GONE).start()
            elif way == 1 and d == (1 if e % PIECES == 0 else -1):
                r_copy(2, e, GONE).start()

    def r_last():
        for e in range(3 * PIECES):
            for way in (0, 1, -1, 2):
                r_copy((way,), e, HERE).wait_recv()
                r_copy((way,), e, GONE).wait_send()
                r_copy(way, e, GONE).wait_send()

    def right_group(p, s, h, way):
        d = 1 if way == "+" else -1
        for q in range(s * SPLIT, s * SPLIT + SPLIT):
            for e in (d,) if way != "*" else WAYS if h else (0,):
                if cut(q):
                    pair_copy(p, q, 0, e, h, HERE).wait_recv()

        def one(i, carry):
            start = pl.multiple_of((zs[-d * h] * 2 + i) * wb, wb)
            ubuf[s] = ubuf[s] + jnp.dot(
                rbuf[:, pl.ds(start, wb)],
                vbuf[p, s, pl.ds(start, wb), :],
                precision=EXACT_PREC,
                preferred_element_type=jnp.float32,
            )
            return carry

        lax.fori_loop(0, 2, one, 0)

    def clear_products():
        def trip(i):
            for s in PAIR:
                ubuf[s, block(i), :] = jnp.zeros((ROWS, wa), jnp.float32)

        fold(trip, 3 * wb // ROWS)

    def mix(q):
        t, base = q // SPLIT, (q % SPLIT) * mb

        def trip(i):
            tiles = [[ubuf[s, span(r * wb + base + i * ROWS, ROWS), :] for s in PAIR] for r in TRIPLE]
            for l in TRIPLE:
                acc = None
                for r in TRIPLE:
                    for s in PAIR:
                        term = w_ref[l, s, t, r] * tiles[r][s]
                        acc = term if acc is None else acc + term
                tbuf[t, span(base + i * ROWS, ROWS), l * wa : (l + 1) * wa] = acc

        fold(trip, mb // ROWS, 1)
        if q == chunks[-1]:
            clear_products()

    def sib_copy(q, i):
        return remote(yb.at[i], rd.at[q, i], rd_s.at[i], rd_r.at[q, i], sibling)

    def left_products(q, part):
        def one(n, carry):
            theirs = (n < 2, n > 0, n < 0)[part]
            i = n + 1 if part == 2 else jnp.where(n == 1 - part, 3, n * part)
            away = jnp.where(i < 2, i + 2, 3 - i)
            start = (mod(x + away, nx) * 2 + jnp.where(theirs, 1 - c, c)) * 2 * wa
            yb[jnp.where(theirs, i, i + 4)] = jnp.dot(
                tbuf[q // SPLIT, (q % SPLIT) * mb : (q % SPLIT + 1) * mb, :],
                lbuf[:, pl.ds(pl.multiple_of(start, 2 * wa), 2 * wa)],
                precision=EXACT_PREC,
                preferred_element_type=jnp.float32,
            )

            @pl.when(theirs)
            def _():
                sib_copy(q, i).start()

            return carry

        for i in ((0, 3), (1, 2), ())[part] if q else ():
            sib_copy(q - 1, i).wait_send()
        lax.fori_loop(0, (3, 3, 2)[part], one, 0)

    lane_at = {GONE: (1 - yl) * wa, HERE: yl * wa}

    def lane(theirs):
        return pl.ds(pl.multiple_of(lane_at[theirs], wa), wa)

    def half_copy(p, q, d, theirs):
        slot, side = 0 if d > 0 else 1, 0 if theirs else 1
        src = rd.at[q, 0, pl.ds(slot * mb // 2, mb // 2), lane(theirs)]
        return remote(src, hx.at[p, q, slot, side], hx_s.at[q, slot, side], hx_r.at[p, q, slot, side], x_next[d])

    def full_copy(p, q, d, theirs):
        slot, side = 0 if d > 0 else 1, 0 if theirs else 1
        src = rd.at[q, 2 - slot, :, lane(theirs)]
        to = (x_side if theirs else x_next)[d]
        return remote(src, fx.at[p, q, slot, side], fx_s.at[q, slot, side], fx_r.at[p, q, slot, side], to)

    def cross_copy(p, q):
        return remote(rd.at[q, 3, :, lane(GONE)], yx.at[p, q], yx_s.at[q], yx_r.at[p, q], yl_partner)

    def left_sum(p, q, i, side):
        if side == 0:
            sib_copy(q, i).wait_recv()

            def add(k):
                rows = block(k)
                rd[q, i, rows, :] = rd[q, i, rows, :] + yb[i + 4, rows, :]

            fold(add, mb // ROWS)
        if i == 0:
            for theirs in (GONE, HERE):
                for d in WAYS:
                    half_copy(p, q, d, theirs).start()
        elif i < 3:
            d, theirs = 2 * i - 3, side == 0
            lanes_at = lane(theirs)
            half_copy(p, q, d, theirs).wait_recv()

            def add_half(k):
                rows = span(k * ROWS + (0 if d > 0 else mb // 2), ROWS)
                rd[q, i, rows, lanes_at] = rd[q, i, rows, lanes_at] + hx[p, q, i % 2, side, block(k), :]

            fold(add_half, mb // 2 // ROWS)
            full_copy(p, q, d, theirs).start()
        else:
            cross_copy(p, q).start()

    def close_chunk(p, q, more):
        for theirs in (GONE, HERE):
            for d in WAYS:
                full_copy(p, q, d, theirs).wait_recv()
        cross_copy(p, q).wait_recv()
        alpha, beta, old = sc[0], sc[1], sc[2]
        s, mine = q // SPLIT, lane(HERE)

        def step(k):
            rows, at = block(k), own_block(k + (q % SPLIT) * mb // ROWS)
            g = rd[q, 3, rows, mine] + yx[p, q, rows, :]
            for slot in PAIR:
                g = g + (fx[p, q, slot, 0, rows, :] + fx[p, q, slot, 1, rows, :])
            vbuf[1 - p, s, at, :] = (g - alpha * vbuf[p, s, at, :] - old * vbuf[1 - p, s, at, :]) / beta

        fold(step, mb // ROWS)

        @pl.when(more)
        def _():
            own_sends(1 - p, q)

    def drain_sums(p, q):
        for theirs in (GONE, HERE):
            for d in WAYS:
                half_copy(p, q, d, theirs).wait_send()
                full_copy(p, q, d, theirs).wait_send()
        cross_copy(p, q).wait_send()

    def l_load(l):
        return pltpu.make_async_copy(l_hbm.at[l, span(yl * wa, wa), :], lbuf.at[pl.ds(l * wa, wa), :], ld_s.at[l])

    def r_load(r):
        return pltpu.make_async_copy(r_hbm.at[r], rbuf.at[span(r * wb + sub * half, half), :], ld_s.at[3 + r])

    def psi_at(s, of_sub):
        return vbuf.at[0, s, span(own + of_sub * half, half), :]

    def psi_load(s):
        return pltpu.make_async_copy(psi_ref.at[yl, s], psi_at(s, sub), ld_s.at[6 + s])

    def psi_copy(s, gone):
        return remote(psi_ref.at[1 - yl, s], psi_at(s, sub if gone else 1 - sub), io_s.at[s], io_r.at[s], yl_partner)

    for s in PAIR:
        psi_load(s).start()
    barrier = pltpu.get_barrier_semaphore()
    for _, count, _, peers in groups:
        for d in range(1, count):
            pl.semaphore_signal(barrier, inc=1, device_id=peers[d], device_id_type=MESH)
    pl.semaphore_wait(barrier, plane + nz - 2)
    for s in PAIR:
        psi_copy(s, GONE).start()
    for e in range(3 * PIECES):
        r_copy(0, e, GONE).start()
    for r in TRIPLE:
        r_load(r).start()
    for l in TRIPLE:
        l_load(l).start()
    pl.semaphore_signal(credit, inc=1, device_id=sibling, device_id_type=MESH)

    def clear(i):
        for s in PAIR:
            vbuf[1, s, own_block(i), :] = jnp.zeros((ROWS, wa), jnp.float32)
            for p in PAIR:
                vv[p, s, block(i), :] = jnp.zeros((ROWS, wa), jnp.float32)

    fold(clear, wb // ROWS)
    clear_products()
    sc[2] = jnp.zeros((ROWS, wa), jnp.float32)
    def work(name, p, more, slot):
        kind, tail = name[0], name[1:]
        if kind in "mnk":
            return functools.partial(right_group, p, int(tail[0]), int(tail[1]), tail[2])
        args = [int(digit) for digit in tail]
        if kind in "ab":
            calls = {
                "a0": lambda: alpha_open(p),
                "b0": lambda: (alpha_close(slot), beta_open(p)),
                "b3": lambda: (beta_close(slot), scale(p)),
            }
            return calls.get(name, functools.partial(sum_pass, "ab".index(kind), args[0]))
        if kind == "c":
            return functools.partial(close_chunk, p, *args, more)
        if kind == "d":
            return functools.partial(drain_gather, p)
        if kind == "w":
            return r_last
        if kind == "r":
            return functools.partial(r_take, *args)
        if kind in "lx":
            return functools.partial({"l": left_products, "x": mix}[kind], *args)
        return functools.partial({"p": take_pair, "h": take_hop, "f": left_sum}[kind], p, *args)

    start_order, gather_order, reduce_order = (
        ",".join(order).split(",") for order in (START_ORDER, GATHER_ORDER, REDUCE_ORDER)
    )
    for s in PAIR:
        psi_load(s).wait()
        psi_copy(s, HERE).wait_recv()
        own_sends(0, s * SPLIT)
    for name in start_order:
        if name[0] == "c":
            own_sends(0, int(name[1]))
        else:
            work(name, 0, None, None)()
    for r in TRIPLE:
        r_load(r).wait()
        l_load(r).wait()
    for s in PAIR:
        psi_copy(s, GONE).wait_send()

    def lanczos_step(j, carry):
        p = mod(j, 2)
        slot = mod(j + LANCZOS_STEPS - 1, LANCZOS_STEPS)
        more = j < LANCZOS_STEPS - 1

        for name in gather_order:
            if name[0] in "rwk":
                pl.when(j == 0)(work(name, p, more, slot))
            elif name[0] == "n":
                pl.when(j > 0)(work(name, p, more, slot))
            else:
                work(name, p, more, slot)()
        mix(0)

        pl.semaphore_wait(credit, 1)
        for name in reduce_order:
            if name[0] in "ph":
                pl.when(more)(work(name, 1 - p, more, slot))
            else:
                work(name, p, more, slot)()
        for i in range(4):
            sib_copy(chunks[-1], i).wait_send()
        for q in chunks:
            drain_sums(p, q)

        @pl.when(more)
        def _():
            pl.semaphore_signal(credit, inc=1, device_id=sibling, device_id_type=MESH)

        sc[2] = jnp.where(j > 0, sc[1], jnp.zeros((ROWS, wa), jnp.float32))
        return carry

    lax.fori_loop(0, LANCZOS_STEPS, lanczos_step, 0)

    p = LANCZOS_STEPS % 2

    def out_copy(s):
        src = vv.at[1 - p, s, span((1 - sub) * half, half), :]
        return remote(src, ob.at[s], io_s.at[2 + s], io_r.at[2 + s], yl_partner)

    alpha_open(p)
    sum_pass(0, 1)
    alpha_close(LANCZOS_STEPS - 1)
    beta_open(p)
    for s in PAIR:
        out_copy(s).start()
    sum_pass(1, 1)
    beta_close(LANCZOS_STEPS - 1)
    for s in PAIR:
        out_copy(s).wait_recv()

        def put(i):
            vout_ref[yl, s, block(i), :] = vv[1 - p, s, span(sub * half + i * ROWS, ROWS), :] / sc[1]
            vout_ref[1 - yl, s, block(i), :] = ob[s, block(i), :] / sc[1]

        fold(put, half // ROWS)
        out_copy(s).wait_send()


def solution(mesh):
    nz, nx = mesh.shape["col"] // 4, mesh.shape["row"] // 2

    def local_steps(psi_blk, left_blk, mpo_tensor, right_blk):
        wa, wb = psi_blk.shape[0] // 2, psi_blk.shape[2] * 2
        da, db = left_blk.shape[2], right_blk.shape[2]
        half = wb // 2
        hops = nz // 2
        mb = wb // SPLIT
        parts = 2 * SPLIT
        lanes = 128 if wa % 128 == 0 else wa
        f32 = jnp.float32
        psi_t = jnp.transpose(psi_blk.reshape(2, wa, 2, half), (0, 2, 3, 1))
        kernel = functools.partial(lanczos_kernel, nz, nx, wa, wb)
        vmem, dma = pltpu.VMEM, pltpu.SemaphoreType.DMA
        ids = 8 * hops + 2
        scalars, v_out = pl.pallas_call(
            kernel,
            out_shape=(
                jax.ShapeDtypeStruct((2 * LANCZOS_STEPS, ROWS, lanes), f32),
                jax.ShapeDtypeStruct((2, 2, half, wa), f32),
            ),
            in_specs=[
                pl.BlockSpec(memory_space=pl.ANY),
                pl.BlockSpec(memory_space=pl.ANY),
                pl.BlockSpec(memory_space=pltpu.SMEM),
                pl.BlockSpec(memory_space=pl.ANY),
            ],
            out_specs=(pl.BlockSpec(memory_space=pltpu.VMEM),) * 2,
            scratch_shapes=[
                vmem((2, 2, db, wa), f32),
                vmem((3 * wa, da), f32),
                vmem((3 * wb, db), f32),
                vmem((2, 3 * wb, wa), f32),
                vmem((2, wb, 3 * wa), f32),
                vmem((2, 2, wb, wa), f32),
                vmem((parts, 4, mb, 2 * wa), f32),
                vmem((8, mb, 2 * wa), f32),
                vmem((2, parts, 2, 2, mb // 2, wa), f32),
                vmem((2, parts, 2, 2, mb, wa), f32),
                vmem((2, parts, mb, wa), f32),
                vmem((2, half, wa), f32),
                vmem((2, nx * 8 + nz, ROWS, lanes), f32),
                vmem((3, ROWS, wa), f32),
                dma((parts, ids)),
                dma((2, parts, ids)),
                dma((4,)),
                dma((parts, 4)),
                dma((parts, 2, 2)),
                dma((2, parts, 2, 2)),
                dma((parts, 2, 2)),
                dma((2, parts, 2, 2)),
                dma((parts,)),
                dma((2, parts)),
                dma((2, 2)),
                dma((2, 2)),
                dma((8, 3 * PIECES)),
                dma((8, 3 * PIECES)),
                dma((4,)),
                dma((4,)),
                dma((8,)),
                pltpu.SemaphoreType.REGULAR,
            ],
            compiler_params=pltpu.CompilerParams(collective_id=0, has_side_effects=True, vmem_limit_bytes=66 * 1000 * 1000),
            name="lanczos",
        )(psi_t, jnp.transpose(left_blk, (1, 0, 2)), jnp.transpose(mpo_tensor, (0, 2, 3, 1)), jnp.transpose(right_blk, (1, 0, 2)))
        v_next = jnp.transpose(v_out, (0, 3, 1, 2)).reshape(psi_blk.shape)
        return scalars[:LANCZOS_STEPS, 0, 0], scalars[LANCZOS_STEPS:, 0, 0], v_next

    return jax.shard_map(
        local_steps,
        mesh=mesh,
        in_specs=(P("row", None, "col"), P("row", None, None), P(), P("col", None, None)),
        out_specs=(P(), P(), P("row", None, "col")),
        check_vma=False,
    )
```

```python
import functools

import jax
import jax.numpy as jnp
from jax import lax
from jax.experimental import pallas as pl
from jax.experimental.pallas import tpu as pltpu
from jax.sharding import PartitionSpec as P

LANCZOS_STEPS = 4
EXACT_PREC = lax.Precision.HIGHEST
MESH = pl.DeviceIdType.MESH
ROWS = 8
SPLIT = 2
PIECES = 2
START_ORDER = (
    "r00,c1,r01,h011,h001,r02,p0,h101,r10,r11,h012,c3,p1,r03,h021",
    "h002,r05,r04,h102,h111,h121,h022,r12,r15,h003,r20,p2,r21",
    "h112,r13,r14,h113,r22,h013,h103,r24,r25,h023,h211,r23",
)
GATHER_ORDER = (
    "a0,h301,h122,h201,p3,h221,h311,w,m00*,m10*,m01-,h302,m02+",
    "m02-,h123,h024,h014,m01+,h202,h321,m03-,m03+,a1,h212,h222",
    "h303,m11+,h104,h312,m11-,h322,h004,m12-,h203,h124,h213,m12+",
    "h223,h114,b0,h304,h313,m04*,h323,h204,m13-,m13+,h214,h314",
    "h224,h324,m14*,b1",
)
REDUCE_ORDER = (
    "l00,x1,f000,l01,f030,l02,f010,f020,l10,x2,b3,f100,l11,f011",
    "f021,f130,l12,f110,f120,l20,d0,c0,f200,f111,l21,p0,f230,f121",
    "l22,h001,x3,f210,f220,h011,l30,h021,f211,c1,f221,h002,f300",
    "p1,l31,h101,f330,l32,h111,f320,c2,h121,f310,f321,h102,f311",
    "h112,p2,h012,h022,c3,h103,h023,h211,h013,h113,h003",
)
PAIR = range(2)
TRIPLE = range(3)
WAYS = (1, -1)
GONE, HERE = True, False


def fold(body, count, unroll=4):
    while count % unroll:
        unroll //= 2

    def trip(i, carry):
        for u in range(unroll):
            body(i * unroll + u)
        return carry

    lax.fori_loop(0, count // unroll, trip, 0)


def lanczos_kernel(
    nz, nx, wa, wb,
    psi_ref, l_hbm, w_ref, r_hbm,
    scal_ref, vout_ref,
    vbuf, lbuf, rbuf, ubuf, tbuf, vv, rd, yb, hx, fx, yx, ob, red, sc,
    ag_s, ag_r, rd_s, rd_r, hx_s, hx_r, fx_s, fx_r, yx_s, yx_r,
    ar_s, ar_r, rr_s, rr_r, io_s, io_r, ld_s, credit,
):
    hops = nz // 2
    half, mb = wb // 2, wb // SPLIT
    part = half // (2 * nx)
    bit = part // PIECES
    chunks = range(2 * SPLIT)
    col, row = lax.axis_index("col"), lax.axis_index("row")
    div, mod = lax.div, lax.rem
    z, y, x, c = div(col, 4), mod(col, 4), div(row, 2), mod(row, 2)
    yh, sub = div(y, 2), mod(y, 2)
    yl = mod(div(y + 1, 2), 2)

    def dev(zz=None, yy=None, xx=None, cc=None):
        zz = z if zz is None else zz
        yy = y if yy is None else yy
        xx = x if xx is None else xx
        cc = c if cc is None else cc
        return {"col": zz * 4 + yy, "row": xx * 2 + cc}

    zs = {off: mod(z + off + nz, nz) for off in range(-hops, nz)}
    xs = {off: mod(x + off + nx, nx) for off in range(-1, nx)}
    starts = {off: (at * 2 + yh) * wb for off, at in zs.items()}
    others = {off: (at * 2 + 1 - yh) * wb for off, at in zs.items()}
    own = starts[0]

    sibling = dev(cc=1 - c)
    yl_partner = dev(yy=y + 1 - 2 * sub)
    yh_partner = dev(yy=3 - y)
    z_next = {d: dev(zz=zs[d]) for d in WAYS}
    x_next = {d: dev(xx=xs[d]) for d in WAYS}
    x_side = {d: dev(yy=y + 1 - 2 * sub, xx=xs[d]) for d in WAYS}

    def remote(src, dst, send, recv, to):
        return pltpu.make_async_remote_copy(
            src_ref=src, dst_ref=dst, send_sem=send, recv_sem=recv, device_id=to, device_id_type=MESH
        )

    def span(start, count):
        return pl.ds(pl.multiple_of(start, ROWS), count)

    def block(i):
        return span(i * ROWS, ROWS)

    def cut(q):
        return mb * (96, 96, 64, 32)[q] // 128

    def lines(q):
        return TRIPLE if cut(q) else TRIPLE[1:]

    def piece(p, q, base, kind, d, h, mid, to):
        start, count = (0, cut(q)) if kind == 0 else (cut(q), mb - cut(q))
        if h == hops:
            count //= 2
            start += count if d < 0 else 0
        at = vbuf.at[p, q // SPLIT, span(base + (q % SPLIT) * mb + start, count), :]
        return remote(at, at, ag_s.at[q, mid], ag_r.at[p, q, mid], to)

    def z_copy(p, q, d, line, h, gone):
        base = (others if line == 2 else starts)[-d * (h - 1 if gone else h)]
        mid = ((0 if d > 0 else 3) + line) * hops + h - 1
        return piece(p, q, base, min(line, 1), d, h, mid, z_next[d])

    def pair_copy(p, q, kind, d, h, gone):
        mid = 6 * hops + (2 * h + max(d, 0) if h else 0 if kind else 1)
        return piece(p, q, (starts if gone else others)[-d * h], kind, d, h, mid, yh_partner)

    def own_sends(p, q):
        pair_copy(p, q, 1, 0, 0, GONE).start()
        for line in lines(q)[:-1]:
            for d in WAYS:
                z_copy(p, q, d, line, 1, GONE).start()
        if cut(q):
            pair_copy(p, q, 0, 0, 0, GONE).start()

    def take_pair(p, q):
        pair_copy(p, q, 1, 0, 0, HERE).wait_recv()
        for d in WAYS:
            z_copy(p, q, d, 2, 1, GONE).start()

    def take_hop(p, q, line, h):
        for d in WAYS:
            z_copy(p, q, d, line, h, HERE).wait_recv()
            if h < hops:
                z_copy(p, q, d, line, h + 1, GONE).start()
            if line == 0:
                pair_copy(p, q, 0, d, h, GONE).start()

    def drain_gather(p):
        for q in chunks:
            first = range(0 if cut(q) else 1, 2)
            for kind in first:
                pair_copy(p, q, kind, 0, 0, GONE).wait_send()
            for d in WAYS:
                for h in range(1, hops + 1):
                    for line in lines(q):
                        z_copy(p, q, d, line, h, GONE).wait_send()
                    for _ in first[1:]:
                        pair_copy(p, q, 0, d, h, GONE).wait_send()

    plane = nx * 8

    line = [mod(row * 4 + y + d, plane) for d in range(plane)]
    groups = (
        (0, plane, row * 4 + y, [{"col": z * 4 + mod(at, 4), "row": div(at, 4)} for at in line]),
        (plane, nz, z, [dev(zz=zs[d]) for d in range(nz)]),
    )

    def sum_send(which, stage, tile):
        base, count, me, peers = groups[stage]
        red[which, base + me] = tile
        at = red.at[which, base + me]
        for d in range(1, count):
            remote(at, at, ar_s.at[which, stage], ar_r.at[which, stage], peers[d]).start()

    def sum_take(which, stage):
        base, count, _, _ = groups[stage]
        at = red.at[which, pl.ds(base, count - 1)]
        pltpu.make_async_copy(at, at, ar_r.at[which, stage]).wait()
        pltpu.make_async_copy(at, at, ar_s.at[which, stage]).wait()
        total = red[which, base]
        for i in range(1, count):
            total = total + red[which, base + i]
        return total

    def sum_pass(which, stage):
        sum_send(which, stage, sum_take(which, stage - 1))

    lanes = red.shape[-1]

    def narrow(tile):
        out = tile[:, :lanes]
        for i in range(1, wa // lanes):
            out = out + tile[:, i * lanes : (i + 1) * lanes]
        return out

    def own_block(i):
        return span(own + i * ROWS, ROWS)

    def accumulate(term):
        def trip(i, acc):
            for s in PAIR:
                acc = acc + term(s, i)
            return acc

        return lax.fori_loop(0, wb // ROWS, trip, jnp.zeros((ROWS, wa), jnp.float32), unroll=4)

    def alpha_open(p):
        acc = accumulate(lambda s, i: vv[p, s, block(i), :] * vbuf[p, s, own_block(i), :])
        sum_send(0, 0, narrow(acc))

    def alpha_close(slot):
        value = jnp.full((ROWS, wa), jnp.sum(sum_take(0, 1)), jnp.float32)
        sc[0] = value
        scal_ref[slot] = value[:, :lanes]

    def beta_open(p):
        alpha, beta = sc[0], sc[2]

        def term(s, i):
            u = vbuf[p, s, own_block(i), :] - alpha * vv[p, s, block(i), :] - beta * vv[1 - p, s, block(i), :]
            vv[1 - p, s, block(i), :] = u
            return u * u

        sum_send(1, 0, narrow(accumulate(term)))

    def beta_close(slot):
        value = jnp.sqrt(jnp.full((ROWS, wa), jnp.sum(sum_take(1, 1)), jnp.float32))
        sc[1] = value
        scal_ref[LANCZOS_STEPS + slot] = value[:, :lanes]

    def scale(p):
        def trip(i):
            for s in PAIR:
                vv[1 - p, s, block(i), :] = vv[1 - p, s, block(i), :] / sc[1]

        fold(trip, wb // ROWS)

    def r_rows(e, of_sub, xx, cc):
        start = (e // PIECES) * wb + of_sub * half + (xx * 2 + cc) * part + (e % PIECES) * bit
        return rbuf.at[span(start, bit), :]

    def r_copy(way, e, gone):
        if way == 0:
            src = r_hbm.at[e // PIECES, span(row * part + (e % PIECES) * bit, bit), :]
            return remote(src, r_rows(e, sub if gone else 1 - sub, x, c), rr_s.at[0, e], rr_r.at[0, e], yl_partner)
        over = isinstance(way, tuple)
        from_way = way[0] if over else way
        slot = from_way % 4
        d = from_way if from_way in WAYS else 1 if e % PIECES == 0 else -1
        away = {0: 0, 2: 2}.get(from_way, -d) - (d if gone and not over else 0)
        away = -d if gone and not over and from_way == 2 else 0 if gone and not over else away
        at = r_rows(e, 1 - sub, xs[away], 1 - c if over and not gone else c)
        slot = slot + 4 if over else slot
        return remote(at, at, rr_s.at[slot, e], rr_r.at[slot, e], sibling if over else x_next[d])

    def r_take(way, e):
        for d in WAYS if way == 1 else (way,):
            r_copy(d, e, HERE).wait_recv()
            r_copy((d,), e, GONE).start()
            if way == 0:
                for n in WAYS:
                    r_copy(n, e, GONE).start()
            elif way == 1 and d == (1 if e % PIECES == 0 else -1):
                r_copy(2, e, GONE).start()

    def r_last():
        for e in range(3 * PIECES):
            for way in (0, 1, -1, 2):
                r_copy((way,), e, HERE).wait_recv()
                r_copy((way,), e, GONE).wait_send()
                r_copy(way, e, GONE).wait_send()

    def right_group(p, s, h, way):
        d = 1 if way == "+" else -1
        for q in range(s * SPLIT, s * SPLIT + SPLIT):
            for e in (d,) if way != "*" else WAYS if h else (0,):
                if cut(q):
                    pair_copy(p, q, 0, e, h, HERE).wait_recv()

        def one(i, carry):
            start = pl.multiple_of((zs[-d * h] * 2 + i) * wb, wb)
            ubuf[s] = ubuf[s] + jnp.dot(
                rbuf[:, pl.ds(start, wb)],
                vbuf[p, s, pl.ds(start, wb), :],
                precision=EXACT_PREC,
                preferred_element_type=jnp.float32,
            )
            return carry

        lax.fori_loop(0, 2, one, 0)

    def clear_products():
        def trip(i):
            for s in PAIR:
                ubuf[s, block(i), :] = jnp.zeros((ROWS, wa), jnp.float32)

        fold(trip, 3 * wb // ROWS)

    def mix(q):
        t, base = q // SPLIT, (q % SPLIT) * mb

        def trip(i):
            tiles = [[ubuf[s, span(r * wb + base + i * ROWS, ROWS), :] for s in PAIR] for r in TRIPLE]
            for l in TRIPLE:
                acc = None
                for r in TRIPLE:
                    for s in PAIR:
                        term = w_ref[l, s, t, r] * tiles[r][s]
                        acc = term if acc is None else acc + term
                tbuf[t, span(base + i * ROWS, ROWS), l * wa : (l + 1) * wa] = acc

        fold(trip, mb // ROWS, 1)
        if q == chunks[-1]:
            clear_products()

    def sib_copy(q, i):
        return remote(yb.at[i], rd.at[q, i], rd_s.at[i], rd_r.at[q, i], sibling)

    def left_products(q, part):
        def one(n, carry):
            theirs = (n < 2, n > 0, n < 0)[part]
            i = n + 1 if part == 2 else jnp.where(n == 1 - part, 3, n * part)
            away = jnp.where(i < 2, i + 2, 3 - i)
            start = (mod(x + away, nx) * 2 + jnp.where(theirs, 1 - c, c)) * 2 * wa
            yb[jnp.where(theirs, i, i + 4)] = jnp.dot(
                tbuf[q // SPLIT, (q % SPLIT) * mb : (q % SPLIT + 1) * mb, :],
                lbuf[:, pl.ds(pl.multiple_of(start, 2 * wa), 2 * wa)],
                precision=EXACT_PREC,
                preferred_element_type=jnp.float32,
            )

            @pl.when(theirs)
            def _():
                sib_copy(q, i).start()

            return carry

        for i in ((0, 3), (1, 2), ())[part] if q else ():
            sib_copy(q - 1, i).wait_send()
        lax.fori_loop(0, (3, 3, 2)[part], one, 0)

    lane_at = {GONE: (1 - yl) * wa, HERE: yl * wa}

    def lane(theirs):
        return pl.ds(pl.multiple_of(lane_at[theirs], wa), wa)

    def half_copy(p, q, d, theirs):
        slot, side = 0 if d > 0 else 1, 0 if theirs else 1
        src = rd.at[q, 0, pl.ds(slot * mb // 2, mb // 2), lane(theirs)]
        return remote(src, hx.at[p, q, slot, side], hx_s.at[q, slot, side], hx_r.at[p, q, slot, side], x_next[d])

    def full_copy(p, q, d, theirs):
        slot, side = 0 if d > 0 else 1, 0 if theirs else 1
        src = rd.at[q, 2 - slot, :, lane(theirs)]
        to = (x_side if theirs else x_next)[d]
        return remote(src, fx.at[p, q, slot, side], fx_s.at[q, slot, side], fx_r.at[p, q, slot, side], to)

    def cross_copy(p, q):
        return remote(rd.at[q, 3, :, lane(GONE)], yx.at[p, q], yx_s.at[q], yx_r.at[p, q], yl_partner)

    def left_sum(p, q, i, side):
        if side == 0:
            sib_copy(q, i).wait_recv()

            def add(k):
                rows = block(k)
                rd[q, i, rows, :] = rd[q, i, rows, :] + yb[i + 4, rows, :]

            fold(add, mb // ROWS)
        if i == 0:
            for theirs in (GONE, HERE):
                for d in WAYS:
                    half_copy(p, q, d, theirs).start()
        elif i < 3:
            d, theirs = 2 * i - 3, side == 0
            lanes_at = lane(theirs)
            half_copy(p, q, d, theirs).wait_recv()

            def add_half(k):
                rows = span(k * ROWS + (0 if d > 0 else mb // 2), ROWS)
                rd[q, i, rows, lanes_at] = rd[q, i, rows, lanes_at] + hx[p, q, i % 2, side, block(k), :]

            fold(add_half, mb // 2 // ROWS)
            full_copy(p, q, d, theirs).start()
        else:
            cross_copy(p, q).start()

    def close_chunk(p, q, more):
        for theirs in (GONE, HERE):
            for d in WAYS:
                full_copy(p, q, d, theirs).wait_recv()
        cross_copy(p, q).wait_recv()
        alpha, beta, old = sc[0], sc[1], sc[2]
        s, mine = q // SPLIT, lane(HERE)

        def step(k):
            rows, at = block(k), own_block(k + (q % SPLIT) * mb // ROWS)
            g = rd[q, 3, rows, mine] + yx[p, q, rows, :]
            for slot in PAIR:
                g = g + (fx[p, q, slot, 0, rows, :] + fx[p, q, slot, 1, rows, :])
            vbuf[1 - p, s, at, :] = (g - alpha * vbuf[p, s, at, :] - old * vbuf[1 - p, s, at, :]) / beta

        fold(step, mb // ROWS)

        @pl.when(more)
        def _():
            own_sends(1 - p, q)

    def drain_sums(p, q):
        for theirs in (GONE, HERE):
            for d in WAYS:
                half_copy(p, q, d, theirs).wait_send()
                full_copy(p, q, d, theirs).wait_send()
        cross_copy(p, q).wait_send()

    def l_load(l):
        return pltpu.make_async_copy(l_hbm.at[l, span(yl * wa, wa), :], lbuf.at[pl.ds(l * wa, wa), :], ld_s.at[l])

    def r_load(r):
        return pltpu.make_async_copy(r_hbm.at[r], rbuf.at[span(r * wb + sub * half, half), :], ld_s.at[3 + r])

    def psi_at(s, of_sub):
        return vbuf.at[0, s, span(own + of_sub * half, half), :]

    def psi_load(s):
        return pltpu.make_async_copy(psi_ref.at[yl, s], psi_at(s, sub), ld_s.at[6 + s])

    def psi_copy(s, gone):
        return remote(psi_ref.at[1 - yl, s], psi_at(s, sub if gone else 1 - sub), io_s.at[s], io_r.at[s], yl_partner)

    for s in PAIR:
        psi_load(s).start()
    barrier = pltpu.get_barrier_semaphore()
    for _, count, _, peers in groups:
        for d in range(1, count):
            pl.semaphore_signal(barrier, inc=1, device_id=peers[d], device_id_type=MESH)
    pl.semaphore_wait(barrier, plane + nz - 2)
    for s in PAIR:
        psi_copy(s, GONE).start()
    for e in range(3 * PIECES):
        r_copy(0, e, GONE).start()
    for r in TRIPLE:
        r_load(r).start()
    for l in TRIPLE:
        l_load(l).start()
    pl.semaphore_signal(credit, inc=1, device_id=sibling, device_id_type=MESH)

    def clear(i):
        for s in PAIR:
            vbuf[1, s, own_block(i), :] = jnp.zeros((ROWS, wa), jnp.float32)
            for p in PAIR:
                vv[p, s, block(i), :] = jnp.zeros((ROWS, wa), jnp.float32)

    fold(clear, wb // ROWS)
    clear_products()
    sc[2] = jnp.zeros((ROWS, wa), jnp.float32)
    def work(name, p, more, slot):
        kind, tail = name[0], name[1:]
        if kind == "m":
            return functools.partial(right_group, p, int(tail[0]), int(tail[1]), tail[2])
        args = [int(digit) for digit in tail]
        if kind in "ab":
            calls = {
                "a0": lambda: alpha_open(p),
                "b0": lambda: (alpha_close(slot), beta_open(p)),
                "b3": lambda: (beta_close(slot), scale(p)),
            }
            return calls.get(name, functools.partial(sum_pass, "ab".index(kind), args[0]))
        if kind == "c":
            return functools.partial(close_chunk, p, *args, more)
        if kind == "d":
            return functools.partial(drain_gather, p)
        if kind == "w":
            return r_last
        if kind == "r":
            return functools.partial(r_take, *args)
        if kind in "lx":
            return functools.partial({"l": left_products, "x": mix}[kind], *args)
        return functools.partial({"p": take_pair, "h": take_hop, "f": left_sum}[kind], p, *args)

    start_order, gather_order, reduce_order = (
        ",".join(order).split(",") for order in (START_ORDER, GATHER_ORDER, REDUCE_ORDER)
    )
    for s in PAIR:
        psi_load(s).wait()
        psi_copy(s, HERE).wait_recv()
        own_sends(0, s * SPLIT)
    for name in start_order:
        if name[0] == "c":
            own_sends(0, int(name[1]))
        else:
            work(name, 0, None, None)()
    for r in TRIPLE:
        r_load(r).wait()
        l_load(r).wait()
    for s in PAIR:
        psi_copy(s, GONE).wait_send()

    def lanczos_step(j, carry):
        p = mod(j, 2)
        slot = mod(j + LANCZOS_STEPS - 1, LANCZOS_STEPS)
        more = j < LANCZOS_STEPS - 1

        for name in gather_order:
            if name[0] in "rw":
                pl.when(j == 0)(work(name, p, more, slot))
            else:
                work(name, p, more, slot)()
        mix(0)

        pl.semaphore_wait(credit, 1)
        for name in reduce_order:
            if name[0] in "ph":
                pl.when(more)(work(name, 1 - p, more, slot))
            else:
                work(name, p, more, slot)()
        for i in range(4):
            sib_copy(chunks[-1], i).wait_send()
        for q in chunks:
            drain_sums(p, q)

        @pl.when(more)
        def _():
            pl.semaphore_signal(credit, inc=1, device_id=sibling, device_id_type=MESH)

        sc[2] = jnp.where(j > 0, sc[1], jnp.zeros((ROWS, wa), jnp.float32))
        return carry

    lax.fori_loop(0, LANCZOS_STEPS, lanczos_step, 0)

    p = LANCZOS_STEPS % 2

    def out_copy(s):
        src = vv.at[1 - p, s, span((1 - sub) * half, half), :]
        return remote(src, ob.at[s], io_s.at[2 + s], io_r.at[2 + s], yl_partner)

    alpha_open(p)
    sum_pass(0, 1)
    alpha_close(LANCZOS_STEPS - 1)
    beta_open(p)
    for s in PAIR:
        out_copy(s).start()
    sum_pass(1, 1)
    beta_close(LANCZOS_STEPS - 1)
    for s in PAIR:
        out_copy(s).wait_recv()

        def put(i):
            vout_ref[yl, s, block(i), :] = vv[1 - p, s, span(sub * half + i * ROWS, ROWS), :] / sc[1]
            vout_ref[1 - yl, s, block(i), :] = ob[s, block(i), :] / sc[1]

        fold(put, half // ROWS)
        out_copy(s).wait_send()


def solution(mesh):
    nz, nx = mesh.shape["col"] // 4, mesh.shape["row"] // 2

    def local_steps(psi_blk, left_blk, mpo_tensor, right_blk):
        wa, wb = psi_blk.shape[0] // 2, psi_blk.shape[2] * 2
        da, db = left_blk.shape[2], right_blk.shape[2]
        half = wb // 2
        hops = nz // 2
        mb = wb // SPLIT
        parts = 2 * SPLIT
        lanes = 128 if wa % 128 == 0 else wa
        f32 = jnp.float32
        psi_t = jnp.transpose(psi_blk.reshape(2, wa, 2, half), (0, 2, 3, 1))
        kernel = functools.partial(lanczos_kernel, nz, nx, wa, wb)
        vmem, dma = pltpu.VMEM, pltpu.SemaphoreType.DMA
        ids = 8 * hops + 2
        scalars, v_out = pl.pallas_call(
            kernel,
            out_shape=(
                jax.ShapeDtypeStruct((2 * LANCZOS_STEPS, ROWS, lanes), f32),
                jax.ShapeDtypeStruct((2, 2, half, wa), f32),
            ),
            in_specs=[
                pl.BlockSpec(memory_space=pl.ANY),
                pl.BlockSpec(memory_space=pl.ANY),
                pl.BlockSpec(memory_space=pltpu.SMEM),
                pl.BlockSpec(memory_space=pl.ANY),
            ],
            out_specs=(pl.BlockSpec(memory_space=pltpu.VMEM),) * 2,
            scratch_shapes=[
                vmem((2, 2, db, wa), f32),
                vmem((3 * wa, da), f32),
                vmem((3 * wb, db), f32),
                vmem((2, 3 * wb, wa), f32),
                vmem((2, wb, 3 * wa), f32),
                vmem((2, 2, wb, wa), f32),
                vmem((parts, 4, mb, 2 * wa), f32),
                vmem((8, mb, 2 * wa), f32),
                vmem((2, parts, 2, 2, mb // 2, wa), f32),
                vmem((2, parts, 2, 2, mb, wa), f32),
                vmem((2, parts, mb, wa), f32),
                vmem((2, half, wa), f32),
                vmem((2, nx * 8 + nz, ROWS, lanes), f32),
                vmem((3, ROWS, wa), f32),
                dma((parts, ids)),
                dma((2, parts, ids)),
                dma((4,)),
                dma((parts, 4)),
                dma((parts, 2, 2)),
                dma((2, parts, 2, 2)),
                dma((parts, 2, 2)),
                dma((2, parts, 2, 2)),
                dma((parts,)),
                dma((2, parts)),
                dma((2, 2)),
                dma((2, 2)),
                dma((8, 3 * PIECES)),
                dma((8, 3 * PIECES)),
                dma((4,)),
                dma((4,)),
                dma((8,)),
                pltpu.SemaphoreType.REGULAR,
            ],
            compiler_params=pltpu.CompilerParams(collective_id=0, has_side_effects=True, vmem_limit_bytes=66 * 1000 * 1000),
            name="lanczos",
        )(psi_t, jnp.transpose(left_blk, (1, 0, 2)), jnp.transpose(mpo_tensor, (0, 2, 3, 1)), jnp.transpose(right_blk, (1, 0, 2)))
        v_next = jnp.transpose(v_out, (0, 3, 1, 2)).reshape(psi_blk.shape)
        return scalars[:LANCZOS_STEPS, 0, 0], scalars[LANCZOS_STEPS:, 0, 0], v_next

    return jax.shard_map(
        local_steps,
        mesh=mesh,
        in_specs=(P("row", None, "col"), P("row", None, None), P(), P("col", None, None)),
        out_specs=(P(), P(), P("row", None, "col")),
        check_vma=False,
    )
```
